128 devices in a mesh: tok: 32 (over y_lo, z, x), voc: 4 (over y_hi, core).
Axes of the slice: x: 4, y: 4 (y_hi: 2, y_lo: 2; y = y_hi * 2 + y_lo), z: 4, core: 2. Of those that a mesh axis runs over, the one named last changes fastest.
Arguments:
- hidden: bfloat16 [1024, 3584], P('tok'), may hold values from -700 to 700
- teacher_logits: bfloat16 [1024, 81920], P(None, ('tok', 'voc')), may hold values from -300 to 300
- sampled_ids: int32 [1024], P('tok'), may hold values from 0 to 81919
- loss_mask: int32 [1024], P('tok'), may hold values from 0 to 1, as said below
- student_head: bfloat16 [3584, 81920], P(None, ('tok', 'voc')), may hold values from -0.3125 to 0.3125
Outputs:
- loss: float32 [], replicated
- sampled_ratio: float32 [1024], P(('tok', 'voc'))
- hidden_grad: bfloat16 [1024, 3584], P(('tok', 'voc'))
- head_grad: bfloat16 [3584, 81920], P(None, ('tok', 'voc'))
The draws below stay inside these ranges and needn't reach their ends.
Inputs may be any that keep to these rules, and one draw needn't show every extreme that they name: `loss_mask`: at least one position is valid.
All inputs are finite; a program needn't handle non-finite values.
Results may differ from the reference program's by a relative error of at most 0.02.
Values may be sent and summed in bfloat16 or wider, within the bound.
No kernel may reach another device: no remote copies, remote signals or barrier semaphores. Data moves between devices by JAX's collectives and lax.ppermute only.
A program may use at most 128 MiB of HBM per device.

```python
import jax
import jax.numpy as jnp

D = 3584
VOCAB = 81920
TOKENS = 1024


def scaled_rows(key, row_count, col_count):
    base = jnp.clip(jax.random.normal(jax.random.fold_in(key, 1), (row_count, col_count), jnp.float32), -6.0, 6.0)
    return base


def draw_hidden(key, part):
    return scaled_rows(key, TOKENS, D).astype(jnp.bfloat16)


def draw_teacher_logits(key, part):
    base = 3.0 * jnp.clip(jax.random.normal(jax.random.fold_in(key, 21), (TOKENS, VOCAB), jnp.float32), -6.0, 6.0)
    return base.astype(jnp.bfloat16)


def draw_loss_mask(key, part):
    levels = jax.random.randint(jax.random.fold_in(key, 11), (TOKENS,), 0, 4)
    valid = jnp.where(levels < 3, 1, 0).astype(jnp.int32)
    position = jnp.arange(TOKENS, dtype=jnp.int32)
    return jnp.where(position == 0, 1, valid).astype(jnp.int32)


def plant(result, stream_key, least, high):
    longest = result.shape.index(max(result.shape))
    spots = []
    for shift in (0, 1):
        where = [jax.random.randint(jax.random.fold_in(stream_key, axis), (), 0, length) for axis, length in enumerate(result.shape)]
        where[longest] = (where[longest] + shift) % result.shape[longest]
        spots.append(tuple(where))
    return result.at[spots[0]].set(least).at[spots[1]].set(high)


def shard_levels(rng, dims, pieces, least, high):
    def one(dim, shards_of):
        draws = jax.random.uniform(jax.random.fold_in(jax.random.fold_in(rng, 6), dim), (shards_of,), jnp.float32, least / len(pieces), high / len(pieces))
        return jnp.repeat(jnp.exp(draws), dims[dim] // shards_of).reshape((-1,) + (1,) * (len(dims) - dim - 1))

    factor_of = one(*pieces[0])
    for cut in pieces[1:]:
        factor_of = factor_of * one(*cut)
    return factor_of


def bell_draw(key, shape, width, most, shards=(), kind=jnp.bfloat16):
    array = width * jax.random.normal(key, shape, jnp.float32)
    if shards:
        array = array * shard_levels(key, shape, shards, -0.22, 0.18)
    return jnp.clip(array, -most, most).astype(kind)


def setup_inputs(seed: int = 0) -> dict:
    key_of = jax.random.split(jax.random.key(seed), 6)
    hidden = draw_hidden(jax.random.fold_in(key_of[5], 71), 0)
    teacher_logits = draw_teacher_logits(jax.random.fold_in(key_of[5], 71), 0)
    sampled_ids = plant(jax.random.randint(key_of[2], (TOKENS,), 0, VOCAB), jax.random.fold_in(key_of[2], 1), 0, VOCAB - 1).astype(jnp.int32)
    loss_mask = draw_loss_mask(jax.random.fold_in(key_of[5], 71), 0)
    student_head = bell_draw(key_of[4], (D, VOCAB), (D // 9) ** -0.5, 0.3125, ((1, 128),))
    return {"hidden": hidden, "teacher_logits": teacher_logits, "sampled_ids": sampled_ids, "loss_mask": loss_mask, "student_head": student_head}


def reference(hidden, teacher_logits, sampled_ids, loss_mask, student_head):
    student = jnp.dot(hidden, student_head, preferred_element_type=jnp.float32)
    teacher = teacher_logits.astype(jnp.float32)
    student_log = jax.nn.log_softmax(student, axis=1)
    teacher_log = jax.nn.log_softmax(teacher, axis=1)
    probs = jnp.exp(student_log)
    differ = student_log - teacher_log
    row_kl = jnp.sum(probs * differ, axis=1)
    weight = loss_mask.astype(jnp.float32)
    count = jnp.sum(weight)
    loss = jnp.sum(weight * row_kl) / count
    picked = jnp.take_along_axis(differ, sampled_ids.astype(jnp.int32)[:, None], axis=1)[:, 0]
    dlogits = (weight[:, None] * probs * (differ - row_kl[:, None])).astype(jnp.bfloat16)
    hidden_grad = jnp.dot(dlogits, student_head.T, preferred_element_type=jnp.float32).astype(jnp.bfloat16)
    head_grad = jnp.dot(hidden.T, dlogits, preferred_element_type=jnp.float32).astype(jnp.bfloat16)
    return loss, picked, hidden_grad, head_grad
```

```python
import jax
import jax.numpy as jnp
from jax import lax
from jax.sharding import Mesh
from jax.sharding import PartitionSpec as P

TOK = ("tok_0", "tok_1", "tok_2")
TOK_VOC = ("tok_0", "tok_1", "tok_2", "voc_0", "voc_1")
CORE = "voc_1"
Y_AXES = ("tok_0", "voc_0")
RING = {"x": ("tok_2", "voc_1"), "z": ("tok_1", "voc_1"), "y": ("tok_0", "voc_0", "voc_1")}
DIGITS = 64
EXTRA = 128
XORS = ((1, 3), (3, 1))


def ring_index(ring, place, core):
    if ring == "y":
        return ((place % 2) * 2 + place // 2) * 2 + core
    return place * 2 + core


def swap(value, ring, step):
    pairs = [
        (ring_index(ring, p, c), ring_index(ring, p ^ XORS[c][step], c))
        for p in range(4)
        for c in range(2)
    ]
    return lax.ppermute(value, RING[ring], pairs)


def swap_core(value):
    return lax.ppermute(value, CORE, [(0, 1), (1, 0)])


def gathered(block, first, second):
    for ring in (first, second):
        for step in (0, 1):
            other = swap(block, ring, step)
            if (ring, step) == (second, 1):
                return block, other
            block = jnp.concatenate([block, other], axis=0)


def token_of_rows(core, z, x, rows):
    n = lax.broadcasted_iota(jnp.int32, (rows, 1), 0)
    quarter = rows // 8
    half, part, top = n // (4 * quarter), (n // (2 * quarter)) % 2, (n // quarter) % 2
    high = half * 2 + top
    low = (n // (quarter // 4)) % 4
    mid = (n // 8) % 2
    first = jnp.where(core == 0, XORS[0][0], XORS[1][0])
    second = jnp.where(core == 0, XORS[0][1], XORS[1][1])

    def place(own, k):
        return own ^ ((k % 2) * first) ^ ((k // 2) * second)

    z_at = jnp.where(part == 0, place(z, high), place(z, low))
    x_at = jnp.where(part == 0, place(x, low), place(x, high))
    return ((((part * 4 + z_at) * 4 + x_at) * 2 + mid) * 2 + core) * 8 + n % 8


def one_hot(rows, columns, dtype):
    return (rows == lax.broadcasted_iota(jnp.int32, (1, columns), 1)).astype(dtype)


def combine(a, b):
    smax, tmax = jnp.maximum(a[0], b[0]), jnp.maximum(a[3], b[3])
    fa, fb = jnp.exp(a[0] - smax), jnp.exp(b[0] - smax)
    return jnp.stack([
        smax,
        a[1] * fa + b[1] * fb,
        a[2] * fa + b[2] * fb,
        tmax,
        a[4] * jnp.exp(a[3] - tmax) + b[4] * jnp.exp(b[3] - tmax),
        a[5] + b[5],
        a[6],
        a[7],
    ])


def per_device(hidden, teacher_logits, sampled_ids, loss_mask, student_head):
    f32, bf16 = jnp.float32, jnp.bfloat16
    core, y_low = lax.axis_index(CORE), lax.axis_index("tok_0")
    z, x = lax.axis_index("tok_1"), lax.axis_index("tok_2")
    position = lax.axis_index(TOK_VOC)
    width, columns = student_head.shape
    tokens = teacher_logits.shape[0]
    rows = tokens // 2

    def own(a):
        return lax.dynamic_index_in_dim(a.reshape(2, 2, 8, *a.shape[1:]), core, 1, False).reshape(
            16, *a.shape[1:]
        )

    ids, mask = own(sampled_ids)[:, None], own(loss_mask)[:, None]
    lane = lax.broadcasted_iota(jnp.int32, (1, EXTRA), 1)
    extra = jnp.where(lane == 0, mask, 0)
    for k in range(3):
        extra = jnp.where(lane == k + 1, (ids // DIGITS**k) % DIGITS, extra)
    block = jnp.concatenate([own(hidden), extra.astype(bf16)], axis=1)
    other = swap(block, "y", 0)
    part_a = jnp.where(y_low == 0, block, other)
    part_b = jnp.where(y_low == 0, other, block)
    a_near, a_far = gathered(part_a, "x", "z")
    b_near, b_far = gathered(part_b, "z", "x")

    head = jnp.concatenate([student_head, swap_core(student_head)], axis=1)
    token = token_of_rows(core, z, x, rows)
    token_other = token_of_rows(1 - core, z, x, rows)
    teacher_own = jnp.dot(one_hot(token, tokens, bf16), teacher_logits)
    teacher_send = jnp.dot(one_hot(token_other, tokens, bf16), teacher_logits)
    teacher = jnp.concatenate([teacher_own, swap_core(teacher_send)], axis=1).astype(f32)

    near = jnp.concatenate([a_near, b_near], axis=0)
    far = jnp.concatenate([a_far, b_far], axis=0)
    student = jnp.concatenate(
        [jnp.dot(h[:, :width], head, preferred_element_type=f32) for h in (near, far)], axis=0
    )
    notes = jnp.concatenate([near[:, width:], far[:, width:]], axis=0).astype(f32)
    weight = notes[:, :1]
    row_ids = (notes[:, 1:2] + DIGITS * notes[:, 2:3] + DIGITS**2 * notes[:, 3:4]).astype(jnp.int32)
    lanes = lax.broadcasted_iota(jnp.int32, (1, 2 * columns), 1)
    column = jnp.where(
        lanes < columns, position * columns + lanes, (position ^ 1) * columns + lanes - columns
    )

    smax = jnp.max(student, axis=1, keepdims=True)
    tmax = jnp.max(teacher, axis=1, keepdims=True)
    shifted = jnp.exp(student - smax)
    differ = student - teacher
    local = jnp.concatenate(
        [
            smax,
            jnp.sum(shifted, axis=1, keepdims=True),
            jnp.sum(shifted * differ, axis=1, keepdims=True),
            tmax,
            jnp.sum(jnp.exp(teacher - tmax), axis=1, keepdims=True),
            jnp.sum(jnp.where(row_ids == column, differ, 0.0), axis=1, keepdims=True),
            weight,
            weight,
        ],
        axis=1,
    )
    reorder = one_hot((token // 16) * 8 + token % 8, rows, f32)
    high = lax.Precision.HIGHEST
    stats = lax.dot_general(
        local, reorder, (((0,), (0,)), ((), ())), precision=high, preferred_element_type=f32
    )
    for ring in ("x", "z", "y"):
        for step in (0, 1):
            stats = combine(stats, swap(stats, ring, step))
    log_stot, log_ttot = jnp.log(stats[1]), jnp.log(stats[4])
    student_shift, teacher_shift = stats[0] + log_stot, stats[3] + log_ttot
    row_kl = stats[2] / stats[1] - student_shift + teacher_shift
    ratio = stats[5] - student_shift + teacher_shift
    chip = position // 2
    sampled_ratio = lax.dynamic_slice_in_dim(ratio, chip * 8, 8, 0)
    sums = jnp.stack([jnp.sum(stats[6] * row_kl), jnp.sum(stats[6])])
    sums = sums + swap_core(sums)
    loss = sums[0] / sums[1]

    shifts = jnp.stack([student_shift, student_shift - teacher_shift + row_kl])
    back = lax.dot_general(
        reorder, shifts, (((1,), (1,)), ((), ())), precision=high, preferred_element_type=f32
    )
    dlogits = (weight * jnp.exp(student - back[:, :1]) * (differ - back[:, 1:2])).astype(bf16)

    def partial_of(d):
        return lax.dot_general(
            d, head, (((1,), (1,)), ((), ())), preferred_element_type=f32
        ).astype(bf16)

    quarter = rows // 4
    far_sum = partial_of(dlogits[2 * quarter :])
    a_in, b_in = swap(far_sum[:quarter], "z", 1), swap(far_sum[quarter:], "x", 1)
    near_sum = partial_of(dlogits[: 2 * quarter])
    a_sum, b_sum = near_sum[:quarter] + a_in, near_sum[quarter:] + b_in
    for (ring_a, ring_b), step in ((("z", "x"), 0), (("x", "z"), 1), (("x", "z"), 0)):
        n = a_sum.shape[0] // 2
        a_in, b_in = swap(a_sum[n:], ring_a, step), swap(b_sum[n:], ring_b, step)
        a_sum, b_sum = a_sum[:n] + a_in, b_sum[:n] + b_in
    last = jnp.concatenate([a_sum, b_sum], axis=0).reshape(4, 8, width)
    last = lax.all_to_all(last, Y_AXES, 0, 0, tiled=True)
    hidden_grad = jnp.sum(last.astype(f32), axis=0).astype(bf16)

    mine = jnp.concatenate([near, far], axis=0)[:, :width]
    both_hidden = jnp.concatenate([mine, swap_core(mine)], axis=0)
    both_dlogits = jnp.concatenate([dlogits[:, :columns], swap_core(dlogits[:, columns:])], axis=0)
    head_grad = lax.dot_general(
        both_hidden, both_dlogits, (((0,), (0,)), ((), ())), preferred_element_type=f32
    ).astype(bf16)
    return (loss, sampled_ratio, hidden_grad, head_grad)


def solution(mesh):
    split = Mesh(mesh.devices.reshape(2, 4, 4, 2, 2), TOK_VOC)
    in_specs = (P(TOK, None), P(None, TOK_VOC), P(TOK), P(TOK), P(None, TOK_VOC))
    out_specs = (P(), P(TOK_VOC), P(TOK_VOC, None), P(None, TOK_VOC))
    return jax.shard_map(
        per_device, mesh=split, in_specs=in_specs, out_specs=out_specs, check_vma=False
    )
```

```python
import jax
import jax.numpy as jnp
from jax import lax
from jax.sharding import Mesh
from jax.sharding import PartitionSpec as P

TOK = ("tok_0", "tok_1", "tok_2")
TOK_VOC = ("tok_0", "tok_1", "tok_2", "voc_0", "voc_1")
CORE = "voc_1"
Y_AXES = ("tok_0", "voc_0")
RING = {"x": ("tok_2", "voc_1"), "z": ("tok_1", "voc_1"), "y": ("tok_0", "voc_0", "voc_1")}
DIGITS = 64
EXTRA = 128
XORS = ((1, 3), (3, 1))


def ring_index(ring, place, core):
    if ring == "y":
        return ((place % 2) * 2 + place // 2) * 2 + core
    return place * 2 + core


def swap(value, ring, step):
    pairs = [
        (ring_index(ring, p, c), ring_index(ring, p ^ XORS[c][step], c))
        for p in range(4)
        for c in range(2)
    ]
    return lax.ppermute(value, RING[ring], pairs)


def swap_core(value):
    return lax.ppermute(value, CORE, [(0, 1), (1, 0)])


def together(*values):
    return lax.optimization_barrier(values)


def token_of_rows(core, z, x, rows):
    n = lax.broadcasted_iota(jnp.int32, (rows, 1), 0)
    quarter = rows // 8
    half, part, top = n // (4 * quarter), (n // (2 * quarter)) % 2, (n // quarter) % 2
    high = half * 2 + top
    low = (n // (quarter // 4)) % 4
    mid = (n // 8) % 2
    first = jnp.where(core == 0, XORS[0][0], XORS[1][0])
    second = jnp.where(core == 0, XORS[0][1], XORS[1][1])

    def place(own, k):
        return own ^ ((k % 2) * first) ^ ((k // 2) * second)

    z_at = jnp.where(part == 0, place(z, high), place(z, low))
    x_at = jnp.where(part == 0, place(x, low), place(x, high))
    return ((((part * 4 + z_at) * 4 + x_at) * 2 + mid) * 2 + core) * 8 + n % 8


def one_hot(rows, columns, dtype):
    return (rows == lax.broadcasted_iota(jnp.int32, (1, columns), 1)).astype(dtype)


def combine(a, b):
    smax, tmax = jnp.maximum(a[0], b[0]), jnp.maximum(a[3], b[3])
    fa, fb = jnp.exp(a[0] - smax), jnp.exp(b[0] - smax)
    return jnp.stack([
        smax,
        a[1] * fa + b[1] * fb,
        a[2] * fa + b[2] * fb,
        tmax,
        a[4] * jnp.exp(a[3] - tmax) + b[4] * jnp.exp(b[3] - tmax),
        a[5] + b[5],
        a[6],
        a[7],
    ])


def per_device(hidden, teacher_logits, sampled_ids, loss_mask, student_head):
    f32, bf16 = jnp.float32, jnp.bfloat16
    core, y_low = lax.axis_index(CORE), lax.axis_index("tok_0")
    z, x = lax.axis_index("tok_1"), lax.axis_index("tok_2")
    position = lax.axis_index(TOK_VOC)
    width, columns = student_head.shape
    tokens = teacher_logits.shape[0]
    rows = tokens // 2

    def own(a):
        return lax.dynamic_index_in_dim(a.reshape(2, 2, 8, *a.shape[1:]), core, 1, False).reshape(
            16, *a.shape[1:]
        )

    ids, mask = own(sampled_ids)[:, None], own(loss_mask)[:, None]
    lane = lax.broadcasted_iota(jnp.int32, (1, EXTRA), 1)
    extra = jnp.where(lane == 0, mask, 0)
    for k in range(3):
        extra = jnp.where(lane == k + 1, (ids // DIGITS**k) % DIGITS, extra)
    block = jnp.concatenate([own(hidden), extra.astype(bf16)], axis=1)
    head_in = swap_core(student_head)
    token = token_of_rows(core, z, x, rows)
    token_other = token_of_rows(1 - core, z, x, rows)
    other = swap(block, "y", 0)
    teacher_send = jnp.dot(one_hot(token_other, tokens, bf16), teacher_logits)
    other, teacher_send = together(other, teacher_send)
    teacher_in = swap_core(teacher_send)
    near_a = jnp.where(y_low == 0, block, other)
    near_b = jnp.where(y_low == 0, other, block)

    far_a, far_b = swap(near_a, "x", 0), swap(near_b, "z", 0)
    teacher_own = jnp.dot(one_hot(token, tokens, bf16), teacher_logits)
    far_a, far_b, teacher_own = together(far_a, far_b, teacher_own)
    near_a, near_b = jnp.concatenate([near_a, far_a]), jnp.concatenate([near_b, far_b])

    far_a, far_b = swap(near_a, "x", 1), swap(near_b, "z", 1)
    teacher = jnp.concatenate([teacher_own, teacher_in], axis=1)
    far_a, far_b, teacher = together(far_a, far_b, teacher)
    teacher = teacher.astype(f32)
    near_a, near_b = jnp.concatenate([near_a, far_a]), jnp.concatenate([near_b, far_b])

    far_a, far_b = swap(near_a, "z", 0), swap(near_b, "x", 0)
    head = jnp.concatenate([student_head, head_in], axis=1)
    far_a, far_b, head = together(far_a, far_b, head)
    near_a, near_b = jnp.concatenate([near_a, far_a]), jnp.concatenate([near_b, far_b])

    far_a, far_b = swap(near_a, "z", 1), swap(near_b, "x", 1)
    near = jnp.concatenate([near_a, near_b])
    student_near = jnp.dot(near[:, :width], head, preferred_element_type=f32)
    far_a, far_b, student_near = together(far_a, far_b, student_near)
    far = jnp.concatenate([far_a, far_b])
    student_far = jnp.dot(far[:, :width], head, preferred_element_type=f32)
    student = jnp.concatenate([student_near, student_far])
    notes = jnp.concatenate([near[:, width:], far[:, width:]], axis=0).astype(f32)
    weight = notes[:, :1]
    row_ids = (notes[:, 1:2] + DIGITS * notes[:, 2:3] + DIGITS**2 * notes[:, 3:4]).astype(jnp.int32)
    lanes = lax.broadcasted_iota(jnp.int32, (1, 2 * columns), 1)
    column = jnp.where(
        lanes < columns, position * columns + lanes, (position ^ 1) * columns + lanes - columns
    )

    smax = jnp.max(student, axis=1, keepdims=True)
    tmax = jnp.max(teacher, axis=1, keepdims=True)
    shifted = jnp.exp(student - smax)
    differ = student - teacher
    local = jnp.concatenate(
        [
            smax,
            jnp.sum(shifted, axis=1, keepdims=True),
            jnp.sum(shifted * differ, axis=1, keepdims=True),
            tmax,
            jnp.sum(jnp.exp(teacher - tmax), axis=1, keepdims=True),
            jnp.sum(jnp.where(row_ids == column, differ, 0.0), axis=1, keepdims=True),
            weight,
            weight,
        ],
        axis=1,
    )
    reorder = one_hot((token // 16) * 8 + token % 8, rows, f32)
    high = lax.Precision.HIGHEST
    stats = lax.dot_general(
        local, reorder, (((0,), (0,)), ((), ())), precision=high, preferred_element_type=f32
    )
    mine = jnp.concatenate([near, far])
    theirs = swap_core(mine)
    for ring in ("x", "z", "y"):
        for step in (0, 1):
            stats = combine(stats, swap(stats, ring, step))
    log_stot, log_ttot = jnp.log(stats[1]), jnp.log(stats[4])
    student_shift, teacher_shift = stats[0] + log_stot, stats[3] + log_ttot
    row_kl = stats[2] / stats[1] - student_shift + teacher_shift
    ratio = stats[5] - student_shift + teacher_shift
    chip = position // 2
    sampled_ratio = lax.dynamic_slice_in_dim(ratio, chip * 8, 8, 0)
    sums = jnp.stack([jnp.sum(stats[6] * row_kl), jnp.sum(stats[6])])
    sums = sums + swap_core(sums)
    loss = sums[0] / sums[1]

    shifts = jnp.stack([student_shift, student_shift - teacher_shift + row_kl])
    back = lax.dot_general(
        reorder, shifts, (((1,), (1,)), ((), ())), precision=high, preferred_element_type=f32
    )
    dlogits = (weight * jnp.exp(student - back[:, :1]) * (differ - back[:, 1:2])).astype(bf16)

    def partial_of(d):
        return lax.dot_general(
            d, head, (((1,), (1,)), ((), ())), preferred_element_type=f32
        ).astype(bf16)

    def head_part(h, d):
        return lax.dot_general(
            h[:, :width], d, (((0,), (0,)), ((), ())), preferred_element_type=f32
        )

    quarter = rows // 4
    dlogits_in = swap_core(dlogits[:, columns:])
    far_sum = partial_of(dlogits[2 * quarter :])
    a_in, b_in = swap(far_sum[:quarter], "z", 1), swap(far_sum[quarter:], "x", 1)
    near_sum = partial_of(dlogits[: 2 * quarter])
    head_sum = head_part(mine, dlogits[:, :columns])
    a_in, b_in, near_sum, head_sum = together(a_in, b_in, near_sum, head_sum)
    a_sum, b_sum = near_sum[:quarter] + a_in, near_sum[quarter:] + b_in
    n = quarter // 2
    a_in, b_in = swap(a_sum[n:], "z", 0), swap(b_sum[n:], "x", 0)
    head_grad = (head_sum + head_part(theirs, dlogits_in)).astype(bf16)
    a_in, b_in, head_grad = together(a_in, b_in, head_grad)
    a_sum, b_sum = a_sum[:n] + a_in, b_sum[:n] + b_in
    for step in (1, 0):
        n = n // 2
        a_in, b_in = together(swap(a_sum[n:], "x", step), swap(b_sum[n:], "z", step))
        a_sum, b_sum = a_sum[:n] + a_in, b_sum[:n] + b_in
    last = jnp.concatenate([a_sum, b_sum], axis=0).reshape(4, 8, width)
    last = lax.all_to_all(last, Y_AXES, 0, 0, tiled=True)
    hidden_grad = jnp.sum(last.astype(f32), axis=0).astype(bf16)
    return (loss, sampled_ratio, hidden_grad, head_grad)


def solution(mesh):
    split = Mesh(mesh.devices.reshape(2, 4, 4, 2, 2), TOK_VOC)
    in_specs = (P(TOK, None), P(None, TOK_VOC), P(TOK), P(TOK), P(None, TOK_VOC))
    out_specs = (P(), P(TOK_VOC), P(TOK_VOC, None), P(None, TOK_VOC))
    return jax.shard_map(
        per_device, mesh=split, in_specs=in_specs, out_specs=out_specs, check_vma=False
    )
```

```python
import functools

import jax
import jax.numpy as jnp
from jax import lax
from jax.sharding import Mesh
from jax.sharding import PartitionSpec as P

TOK = ("tok_0", "tok_1", "tok_2")
TOK_VOC = ("tok_0", "tok_1", "tok_2", "voc_0", "voc_1")
CORE = "voc_1"
Y_AXES = ("tok_0", "voc_0")
RING = {"x": ("tok_2", "voc_1"), "z": ("tok_1", "voc_1"), "y": ("tok_0", "voc_0", "voc_1")}
DIGITS = 64
EXTRA = 128
XORS = ((1, 3, 2), (3, 1, 2))


def ring_index(ring, place, core):
    if ring == "y":
        return ((place % 2) * 2 + place // 2) * 2 + core
    return place * 2 + core


def swap(value, ring, step):
    pairs = [
        (ring_index(ring, p, c), ring_index(ring, p ^ XORS[c][step], c))
        for p in range(4)
        for c in range(2)
    ]
    return lax.ppermute(value, RING[ring], pairs)


def swap_core(value):
    return lax.ppermute(value, CORE, [(0, 1), (1, 0)])


def together(*values):
    return lax.optimization_barrier(values)


def token_of_rows(core, z, x, rows):
    n = lax.broadcasted_iota(jnp.int32, (rows, 1), 0)
    quarter = rows // 8
    half, part, top = n // (4 * quarter), (n // (2 * quarter)) % 2, (n // quarter) % 2
    high = half * 2 + top
    low = (n // (quarter // 4)) % 4
    mid = (n // 8) % 2
    first = jnp.where(core == 0, XORS[0][0], XORS[1][0])
    second = jnp.where(core == 0, XORS[0][1], XORS[1][1])

    def place(own, k):
        return own ^ ((k % 2) * first) ^ ((k // 2) * second)

    z_at = jnp.where(part == 0, place(z, high), place(z, low))
    x_at = jnp.where(part == 0, place(x, low), place(x, high))
    return ((((part * 4 + z_at) * 4 + x_at) * 2 + mid) * 2 + core) * 8 + n % 8


def one_hot(rows, columns, dtype):
    return (rows == lax.broadcasted_iota(jnp.int32, (1, columns), 1)).astype(dtype)


def merged(parts):
    row = lax.broadcasted_iota(jnp.int32, (8, 1), 0)
    most = functools.reduce(jnp.maximum, parts)
    total = 0.0
    for part in parts:
        factor = jnp.where(
            row < 3,
            jnp.exp(part[0:1] - most[0:1]),
            jnp.where(row < 5, jnp.exp(part[3:4] - most[3:4]), 1.0),
        )
        total = total + part * factor
    total = jnp.where(row < 6, total, parts[0])
    return jnp.where((row == 0) | (row == 3), most, total)


def per_device(hidden, teacher_logits, sampled_ids, loss_mask, student_head):
    f32, bf16 = jnp.float32, jnp.bfloat16
    core, y_low = lax.axis_index(CORE), lax.axis_index("tok_0")
    z, x = lax.axis_index("tok_1"), lax.axis_index("tok_2")
    position = lax.axis_index(TOK_VOC)
    width, columns = student_head.shape
    tokens = teacher_logits.shape[0]
    rows = tokens // 2

    ids, mask = sampled_ids[:, None], loss_mask[:, None]
    lane = lax.broadcasted_iota(jnp.int32, (1, EXTRA), 1)
    extra = jnp.where(lane == 0, mask, 0)
    for k in range(3):
        extra = jnp.where(lane == k + 1, (ids // DIGITS**k) % DIGITS, extra)
    block = jnp.concatenate([hidden, extra.astype(bf16)], axis=1).reshape(2, 2, 8, width + EXTRA)
    block = jnp.where(core == 0, block[:, 0], block[:, 1]).reshape(16, width + EXTRA)
    head_in = swap_core(student_head)
    token = token_of_rows(core, z, x, rows)
    token_other = token_of_rows(1 - core, z, x, rows)
    other = swap(block, "y", 0)
    teacher_send = jnp.dot(one_hot(token_other, tokens, bf16), teacher_logits)
    other, teacher_send = together(other, teacher_send)
    teacher_in = swap_core(teacher_send)
    near_a = jnp.where(y_low == 0, block, other)
    near_b = jnp.where(y_low == 0, other, block)

    pieces_a, pieces_b = [near_a], [near_b]
    for step in range(3):
        pieces_a.append(swap(near_a, "x", step))
        pieces_b.append(swap(near_b, "z", step))
    teacher_own = jnp.dot(one_hot(token, tokens, bf16), teacher_logits)
    teacher = jnp.concatenate([teacher_own, teacher_in], axis=1)
    *pieces, teacher = together(*pieces_a, *pieces_b, teacher)
    near_a, near_b = jnp.concatenate(pieces[:4]), jnp.concatenate(pieces[4:])

    far_a, far_b = swap(near_a, "z", 0), swap(near_b, "x", 0)
    head = jnp.concatenate([student_head, head_in], axis=1)
    far_a, far_b, head = together(far_a, far_b, head)
    near_a, near_b = jnp.concatenate([near_a, far_a]), jnp.concatenate([near_b, far_b])

    lanes = lax.broadcasted_iota(jnp.int32, (1, 2 * columns), 1)
    column = jnp.where(
        lanes < columns, position * columns + lanes, (position ^ 1) * columns + lanes - columns
    )

    def local_stats(states, teacher):
        student = jnp.dot(states[:, :width], head, preferred_element_type=f32)
        notes = states[:, width : width + 8].astype(f32)
        row_ids = notes[:, 1:2] + DIGITS * notes[:, 2:3] + DIGITS**2 * notes[:, 3:4]
        chosen = row_ids.astype(jnp.int32) == column
        teacher = teacher.astype(f32)
        smax = jnp.max(student, axis=1, keepdims=True)
        tmax = jnp.max(teacher, axis=1, keepdims=True)
        shifted = jnp.exp(student - smax)
        differ = student - teacher
        sums = [
            smax,
            jnp.sum(shifted, axis=1, keepdims=True),
            jnp.sum(shifted * differ, axis=1, keepdims=True),
            tmax,
            jnp.sum(jnp.exp(teacher - tmax), axis=1, keepdims=True),
            jnp.sum(jnp.where(chosen, differ, 0.0), axis=1, keepdims=True),
            notes[:, :1],
            notes[:, :1],
        ]
        return student, jnp.concatenate(sums, axis=1)

    far_a, far_b = swap(near_a, "z", 1), swap(near_b, "x", 1)
    near = jnp.concatenate([near_a, near_b])
    near_other = swap_core(near)
    half = rows // 2
    student_near, local_near = local_stats(near, teacher[:half])
    far_a, far_b, student_near, local_near = together(far_a, far_b, student_near, local_near)
    far = jnp.concatenate([far_a, far_b])
    student_far, local_far = local_stats(far, teacher[half:])
    local = jnp.concatenate([local_near, local_far])
    reorder = one_hot((token // 16) * 8 + token % 8, rows, f32)
    high = lax.Precision.HIGHEST
    stats = lax.dot_general(
        local, reorder, (((0,), (0,)), ((), ())), precision=high, preferred_element_type=f32
    )
    far_other = swap_core(far)
    stats = merged([stats, *(swap(stats, "x", step) for step in range(3))])
    stats = merged([stats, *(swap(stats, "z", step) for step in range(3))])
    arrived = [swap(stats, "y", step) for step in range(3)]
    head_again = together(stats, student_head, head_in)[1:]
    head_again = jnp.concatenate(head_again, axis=1)
    *arrived, head_again = together(*arrived, head_again)
    stats = merged([stats, *arrived])
    log_stot, log_ttot = jnp.log(stats[1]), jnp.log(stats[4])
    student_shift, teacher_shift = stats[0] + log_stot, stats[3] + log_ttot
    row_kl = stats[2] / stats[1] - student_shift + teacher_shift
    ratio = stats[5] - student_shift + teacher_shift
    chip = position // 2
    sampled_ratio = lax.dynamic_slice_in_dim(ratio, chip * 8, 8, 0)
    sums = jnp.stack([jnp.sum(stats[6] * row_kl), jnp.sum(stats[6])])
    sums = sums + swap_core(sums)
    loss = sums[0] / sums[1]

    shifts = jnp.stack([student_shift, student_shift - teacher_shift + row_kl])
    back = lax.dot_general(
        reorder, shifts, (((1,), (1,)), ((), ())), precision=high, preferred_element_type=f32
    )

    def dlogits_of(student, teacher, notes, shift):
        differ = student - teacher.astype(f32)
        probs = jnp.exp(student - shift[:, :1])
        return (notes[:, 6:7] * probs * (differ - shift[:, 1:2])).astype(bf16)

    def partial_of(d):
        return lax.dot_general(
            d, head_again, (((1,), (1,)), ((), ())), preferred_element_type=f32
        ).astype(bf16)

    quarter = rows // 4
    far_d = dlogits_of(student_far, teacher[half:], local_far, back[half:])
    far_sum = partial_of(far_d)
    far_sum, back_near = together(far_sum, back[:half])
    a_in, b_in = swap(far_sum[:quarter], "z", 1), swap(far_sum[quarter:], "x", 1)
    near_d = dlogits_of(student_near, teacher[:half], local_near, back_near)
    both_d = jnp.concatenate([near_d, far_d])
    both_d_other = swap_core(both_d[:, columns:])
    near_sum = partial_of(near_d)
    head_grad = lax.dot_general(
        jnp.concatenate([near, far, near_other, far_other])[:, :width],
        jnp.concatenate([both_d[:, :columns], both_d_other]),
        (((0,), (0,)), ((), ())),
        preferred_element_type=f32,
    ).astype(bf16)
    a_in, b_in, near_sum, head_grad = together(a_in, b_in, near_sum, head_grad)
    a_sum, b_sum = near_sum[:quarter] + a_in, near_sum[quarter:] + b_in
    n = quarter // 2
    a_in, b_in = together(swap(a_sum[n:], "z", 0), swap(b_sum[n:], "x", 0))
    a_sum, b_sum = a_sum[:n] + a_in, b_sum[:n] + b_in
    n = n // 4
    arrived = [
        swap(part[n * (step + 1) : n * (step + 2)], ring, step)
        for step in range(3)
        for part, ring in ((a_sum, "x"), (b_sum, "z"))
    ]
    arrived = together(*arrived)

    def added(own, parts):
        return sum((p.astype(f32) for p in parts), own.astype(f32)).astype(bf16)

    a_sum, b_sum = added(a_sum[:n], arrived[0::2]), added(b_sum[:n], arrived[1::2])
    last = jnp.concatenate([a_sum, b_sum], axis=0).reshape(4, 8, width)
    last = lax.all_to_all(last, Y_AXES, 0, 0, tiled=True)
    hidden_grad = jnp.sum(last.astype(f32), axis=0).astype(bf16)
    return (loss, sampled_ratio, hidden_grad, head_grad)


def solution(mesh):
    split = Mesh(mesh.devices.reshape(2, 4, 4, 2, 2), TOK_VOC)
    in_specs = (P(TOK, None), P(None, TOK_VOC), P(TOK), P(TOK), P(None, TOK_VOC))
    out_specs = (P(), P(TOK_VOC), P(TOK_VOC, None), P(None, TOK_VOC))
    return jax.shard_map(
        per_device, mesh=split, in_specs=in_specs, out_specs=out_specs, check_vma=False
    )
```

```python
import functools

import jax
import jax.numpy as jnp
from jax import lax
from jax.experimental import pallas as pl
from jax.experimental.pallas import tpu as pltpu
from jax.sharding import Mesh
from jax.sharding import PartitionSpec as P

TOK = ("tok_0", "tok_1", "tok_2")
TOK_VOC = ("tok_0", "tok_1", "tok_2", "voc_0", "voc_1")
CORE = "voc_1"
Y_AXES = ("tok_0", "voc_0")
RING = {"x": ("tok_2", "voc_1"), "z": ("tok_1", "voc_1"), "y": ("tok_0", "voc_0", "voc_1")}
DIGIT_BITS = 6
DIGITS = 1 << DIGIT_BITS
EXTRA = 128
INTERPRET = False
XORS = ((1, 3, 2), (3, 1, 2))


def ring_index(ring, place, core):
    if ring == "y":
        return ((place % 2) * 2 + place // 2) * 2 + core
    return place * 2 + core


def swap(value, ring, step):
    pairs = [
        (ring_index(ring, p, c), ring_index(ring, p ^ XORS[c][step], c))
        for p in range(4)
        for c in range(2)
    ]
    return lax.ppermute(value, RING[ring], pairs)


def swap_core(value):
    return lax.ppermute(value, CORE, [(0, 1), (1, 0)])


def together(*values):
    return lax.optimization_barrier(values)


def token_of_rows(core, z, x, rows):
    n = lax.broadcasted_iota(jnp.int32, (rows, 1), 0)
    quarter = rows // 8
    half, part, top = n // (4 * quarter), (n // (2 * quarter)) % 2, (n // quarter) % 2
    high = half * 2 + top
    low = (n // (quarter // 4)) % 4
    mid = (n // 8) % 2
    first = jnp.where(core == 0, XORS[0][0], XORS[1][0])
    second = jnp.where(core == 0, XORS[0][1], XORS[1][1])

    def place(own, k):
        return own ^ ((k % 2) * first) ^ ((k // 2) * second)

    z_at = jnp.where(part == 0, place(z, high), place(z, low))
    x_at = jnp.where(part == 0, place(x, low), place(x, high))
    return ((((part * 4 + z_at) * 4 + x_at) * 2 + mid) * 2 + core) * 8 + n % 8


def one_hot(rows, columns, dtype):
    return (rows == lax.broadcasted_iota(jnp.int32, (1, columns), 1)).astype(dtype)


def merged(parts):
    row = lax.broadcasted_iota(jnp.int32, (8, 1), 0)
    most = functools.reduce(jnp.maximum, parts)
    total = 0.0
    for part in parts:
        factor = jnp.where(
            row < 3,
            jnp.exp(part[0:1] - most[0:1]),
            jnp.where(row < 5, jnp.exp(part[3:4] - most[3:4]), 1.0),
        )
        total = total + part * factor
    total = jnp.where(row < 6, total, parts[0])
    return jnp.where((row == 0) | (row == 3), most, total)


def nearest_block(width):
    return 512 if width % 512 == 0 else 128


def call(kernel, flops, nbytes, **settings):
    return pl.pallas_call(
        kernel,
        cost_estimate=pl.CostEstimate(flops=flops, bytes_accessed=nbytes, transcendentals=0),
        interpret=INTERPRET,
        **settings,
    )


def whole(shape):
    return pl.BlockSpec(shape, lambda *_: (0,) * len(shape))


def entry_block(core, hidden, ids, mask):
    rows, width = hidden.shape

    def kernel(core_ref, hidden_ref, ids_ref, mask_ref, out_ref):
        lane = lax.broadcasted_iota(jnp.int32, (8, EXTRA), 1)
        for k in range(rows // 16):
            at = 8 * (2 * k + core_ref[0])
            out_ref[8 * k : 8 * k + 8, :width] = hidden_ref[pl.ds(pl.multiple_of(at, 8), 8), :]
            row = at + lax.broadcasted_iota(jnp.int32, (8, rows), 0)
            mine = row == lax.broadcasted_iota(jnp.int32, (8, rows), 1)
            one = jnp.sum(jnp.where(mine, ids_ref[...], 0), axis=1, keepdims=True)
            extra = jnp.where(
                lane == 0, jnp.sum(jnp.where(mine, mask_ref[...], 0), axis=1, keepdims=True), 0
            )
            for d in range(3):
                digit = (one >> (DIGIT_BITS * d)) & (DIGITS - 1)
                extra = jnp.where(lane == d + 1, digit, extra)
            out_ref[8 * k : 8 * k + 8, width:] = extra.astype(jnp.float32).astype(jnp.bfloat16)

    return call(
        kernel,
        10**6,
        hidden.size * 3,
        out_shape=jax.ShapeDtypeStruct((rows // 2, width + EXTRA), jnp.bfloat16),
        in_specs=[pl.BlockSpec(memory_space=pltpu.SMEM)]
        + [pl.BlockSpec(memory_space=pltpu.VMEM)] * 3,
        out_specs=pl.BlockSpec(memory_space=pltpu.VMEM),
    )(core[None], hidden, ids[None], mask[None])


def logits_and_stats(bases, a, b, head, head_in, teacher, teacher_in, which):
    f32 = jnp.float32
    width, columns = head.shape
    part, rows = a.shape[0], 2 * a.shape[0]
    step = 128
    steps = columns // step
    chunk = 32

    def kernel(base_ref, a_ref, b_ref, h_ref, g_ref, t_ref, u_ref, out_ref, local_ref, states, notes):
        j = pl.program_id(0)

        @pl.when(j == 0)
        def _():
            states[:part] = a_ref[:, :width]
            states[part:] = b_ref[:, :width]
            notes[:part] = a_ref[:, width:].astype(f32)
            notes[part:] = b_ref[:, width:].astype(f32)

        weights = jnp.concatenate([h_ref[...], g_ref[...]], axis=1)
        student = jnp.dot(states[...], weights, preferred_element_type=f32)
        out_ref[:, pl.ds(pl.multiple_of(j * step, step), step)] = student[:, :step]
        out_ref[:, pl.ds(pl.multiple_of(columns + j * step, step), step)] = student[:, step:]

        @pl.when(j == steps - 1)
        def _():
            lanes = lax.broadcasted_iota(jnp.int32, (1, 2 * columns), 1)
            column = jnp.where(lanes < columns, base_ref[0] + lanes, base_ref[1] + lanes - columns)
            lane = lax.broadcasted_iota(jnp.int32, (1, 8), 1)

            def body(i, carry):
                at = pl.ds(pl.multiple_of(i * chunk, chunk), chunk)
                student, note = out_ref[at, :], notes[at, :]
                teacher = jnp.concatenate([t_ref[at, :], u_ref[at, :]], axis=1).astype(f32)
                ids = note[:, 1:2] + DIGITS * note[:, 2:3] + DIGITS**2 * note[:, 3:4]
                chosen = ids.astype(jnp.int32) == column
                smax = jnp.max(student, axis=1, keepdims=True)
                tmax = jnp.max(teacher, axis=1, keepdims=True)
                shifted = jnp.exp(student - smax)
                differ = student - teacher
                sums = [
                    smax,
                    jnp.sum(shifted, axis=1, keepdims=True),
                    jnp.sum(shifted * differ, axis=1, keepdims=True),
                    tmax,
                    jnp.sum(jnp.exp(teacher - tmax), axis=1, keepdims=True),
                    jnp.sum(jnp.where(chosen, differ, 0.0), axis=1, keepdims=True),
                    note[:, :1],
                    note[:, :1],
                ]
                found = jnp.zeros((chunk, 8), f32)
                for k, value in enumerate(sums):
                    found = jnp.where(lane == k, value, found)
                local_ref[at, :] = found
                return carry

            lax.fori_loop(0, rows // chunk, body, 0)

    extended = whole((part, width + EXTRA))
    heads = pl.BlockSpec((width, step), lambda j: (0, j))
    teachers = pl.BlockSpec((rows, columns), lambda j: (which, 0))
    return call(
        kernel,
        4 * rows * width * columns,
        4 * width * columns,
        grid=(steps,),
        out_shape=[
            jax.ShapeDtypeStruct((rows, 2 * columns), f32),
            jax.ShapeDtypeStruct((rows, 8), f32),
        ],
        in_specs=[
            pl.BlockSpec(memory_space=pltpu.SMEM),
            extended,
            extended,
            heads,
            heads,
            teachers,
            teachers,
        ],
        out_specs=[whole((rows, 2 * columns)), whole((rows, 8))],
        scratch_shapes=[
            pltpu.VMEM((rows, width), jnp.bfloat16),
            pltpu.VMEM((rows, EXTRA), f32),
        ],
    )(bases, a, b, head, head_in, teacher, teacher_in)


def gradients(student, local, shift, head, head_in, teacher, teacher_in, which):
    f32, bf16 = jnp.float32, jnp.bfloat16
    width, columns = head.shape
    rows = student.shape[0]
    part = rows // 2
    block = nearest_block(width)
    chunk = 32

    def kernel(s_ref, l_ref, c_ref, h_ref, g_ref, t_ref, u_ref, a_ref, b_ref, d_ref, e_ref, both):
        @pl.when(pl.program_id(0) == 0)
        def _():
            def body(i, carry):
                at = pl.ds(pl.multiple_of(i * chunk, chunk), chunk)
                student, shift = s_ref[at, :], c_ref[at, :]
                teacher = jnp.concatenate([t_ref[at, :], u_ref[at, :]], axis=1).astype(f32)
                probs = l_ref[at, 6:7] * jnp.exp(student - shift[:, :1])
                found = (probs * (student - teacher - shift[:, 1:2])).astype(bf16)
                both[at, :] = found
                d_ref[at, :] = found[:, :columns]
                e_ref[at, :] = found[:, columns:]
                return carry

            lax.fori_loop(0, rows // chunk, body, 0)

        weights = jnp.concatenate([h_ref[...], g_ref[...]], axis=1)
        product = lax.dot_general(
            both[...], weights, (((1,), (1,)), ((), ())), preferred_element_type=f32
        ).astype(bf16)
        a_ref[...] = product[:part]
        b_ref[...] = product[part:]

    heads = pl.BlockSpec((block, columns), lambda j: (j, 0))
    teachers = pl.BlockSpec((rows, columns), lambda j: (which, 0))
    sums = pl.BlockSpec((part, block), lambda j: (0, j))
    return call(
        kernel,
        4 * rows * width * columns,
        4 * width * columns,
        grid=(width // block,),
        out_shape=[jax.ShapeDtypeStruct((part, width), bf16)] * 2
        + [jax.ShapeDtypeStruct((rows, columns), bf16)] * 2,
        in_specs=[
            whole((rows, 2 * columns)),
            whole((rows, 8)),
            pl.BlockSpec((rows, 8), lambda j: (which, 0)),
            heads,
            heads,
            teachers,
            teachers,
        ],
        out_specs=[sums, sums, whole((rows, columns)), whole((rows, columns))],
        scratch_shapes=[pltpu.VMEM((rows, 2 * columns), bf16)],
    )(student, local, shift, head, head_in, teacher, teacher_in)


def head_gradient(states, dlogits, width):
    bf16 = jnp.bfloat16
    columns = dlogits[0].shape[1]
    block = nearest_block(width)
    tokens = sum(d.shape[0] for d in dlogits)
    n = len(states)

    def kernel(*refs):
        pieces, others, (out_ref, left, right) = refs[:n], refs[n:-3], refs[-3:]

        @pl.when(pl.program_id(0) == 0)
        def _():
            at = 0
            for ref in others:
                right[at : at + ref.shape[0]] = ref[...]
                at += ref.shape[0]

        at = 0
        for ref in pieces:
            left[at : at + ref.shape[0]] = ref[...]
            at += ref.shape[0]
        out_ref[...] = lax.dot_general(
            left[...], right[...], (((0,), (0,)), ((), ())), preferred_element_type=jnp.float32
        ).astype(bf16)

    return call(
        kernel,
        2 * tokens * width * columns,
        2 * width * (tokens + columns),
        grid=(width // block,),
        out_shape=jax.ShapeDtypeStruct((width, columns), bf16),
        in_specs=[pl.BlockSpec((s.shape[0], block), lambda j: (0, j)) for s in states]
        + [whole(d.shape) for d in dlogits],
        out_specs=pl.BlockSpec((block, columns), lambda j: (j, 0)),
        scratch_shapes=[
            pltpu.VMEM((tokens, block), bf16),
            pltpu.VMEM((tokens, columns), bf16),
        ],
    )(*states, *dlogits)


def per_device(hidden, teacher_logits, sampled_ids, loss_mask, student_head):
    f32, bf16 = jnp.float32, jnp.bfloat16
    core, y_low = lax.axis_index(CORE), lax.axis_index("tok_0")
    z, x = lax.axis_index("tok_1"), lax.axis_index("tok_2")
    position = lax.axis_index(TOK_VOC)
    width, columns = student_head.shape
    tokens = teacher_logits.shape[0]
    rows = tokens // 2

    block = entry_block(core, hidden, sampled_ids, loss_mask)
    head_in = swap_core(student_head)
    token = token_of_rows(core, z, x, rows)
    token_other = token_of_rows(1 - core, z, x, rows)
    other = swap(block, "y", 0)
    teacher_send = jnp.dot(one_hot(token_other, tokens, bf16), teacher_logits)
    other, teacher_send = together(other, teacher_send)
    teacher_in = swap_core(teacher_send)
    near_a = jnp.where(y_low == 0, block, other)
    near_b = jnp.where(y_low == 0, other, block)

    pieces_a, pieces_b = [near_a], [near_b]
    for step in range(3):
        pieces_a.append(swap(near_a, "x", step))
        pieces_b.append(swap(near_b, "z", step))
    teacher = jnp.dot(one_hot(token, tokens, bf16), teacher_logits)
    *pieces, teacher = together(*pieces_a, *pieces_b, teacher)
    near_a, near_b = jnp.concatenate(pieces[:4]), jnp.concatenate(pieces[4:])

    far_a, far_b = together(swap(near_a, "z", 0), swap(near_b, "x", 0))
    near_a, near_b = jnp.concatenate([near_a, far_a]), jnp.concatenate([near_b, far_b])

    far_a, far_b = swap(near_a, "z", 1), swap(near_b, "x", 1)
    bases = jnp.stack([position, position ^ 1]) * columns
    shared = (student_head, head_in, teacher, teacher_in)
    near_other = swap_core(near_a), swap_core(near_b)
    student_near, local_near = logits_and_stats(bases, near_a, near_b, *shared, 0)
    far_a, far_b, student_near, local_near = together(far_a, far_b, student_near, local_near)
    student_far, local_far = logits_and_stats(bases, far_a, far_b, *shared, 1)
    local = jnp.concatenate([local_near, local_far])
    reorder = one_hot((token // 16) * 8 + token % 8, rows, f32)
    high = lax.Precision.HIGHEST
    stats = lax.dot_general(
        local, reorder, (((0,), (0,)), ((), ())), precision=high, preferred_element_type=f32
    )
    far_other = swap_core(far_a), swap_core(far_b)
    stats = merged([stats, *(swap(stats, "x", step) for step in range(3))])
    stats = merged([stats, *(swap(stats, "z", step) for step in range(3))])
    stats = merged([stats, *(swap(stats, "y", step) for step in range(3))])
    log_stot, log_ttot = jnp.log(stats[1]), jnp.log(stats[4])
    student_shift, teacher_shift = stats[0] + log_stot, stats[3] + log_ttot
    row_kl = stats[2] / stats[1] - student_shift + teacher_shift
    ratio = stats[5] - student_shift + teacher_shift
    chip = position // 2
    sampled_ratio = lax.dynamic_slice_in_dim(ratio, chip * 8, 8, 0)
    sums = jnp.stack([jnp.sum(stats[6] * row_kl), jnp.sum(stats[6])])
    sums = sums + swap_core(sums)
    loss = sums[0] / sums[1]

    shifts = jnp.stack([student_shift, student_shift - teacher_shift + row_kl] * 4)
    back = lax.dot_general(
        reorder, shifts, (((1,), (1,)), ((), ())), precision=high, preferred_element_type=f32
    )

    far_sum_a, far_sum_b, *far_d = gradients(student_far, local_far, back, *shared, 1)
    far_sum_a, far_sum_b, back = together(far_sum_a, far_sum_b, back)
    a_in, b_in = swap(far_sum_a, "z", 1), swap(far_sum_b, "x", 1)
    far_d_in = swap_core(far_d[1])
    near_sum_a, near_sum_b, *near_d = gradients(student_near, local_near, back, *shared, 0)
    near_d_in = swap_core(near_d[1])
    head_grad = head_gradient(
        (near_a, near_b, far_a, far_b, *near_other, *far_other),
        (near_d[0], far_d[0], near_d_in, far_d_in),
        width,
    )
    a_in, b_in, near_sum_a, near_sum_b, head_grad = together(
        a_in, b_in, near_sum_a, near_sum_b, head_grad
    )
    quarter = rows // 4
    a_sum, b_sum = near_sum_a + a_in, near_sum_b + b_in
    n = quarter // 2
    a_in, b_in = together(swap(a_sum[n:], "z", 0), swap(b_sum[n:], "x", 0))
    a_sum, b_sum = a_sum[:n] + a_in, b_sum[:n] + b_in
    n = n // 4
    arrived = [
        swap(part[n * (step + 1) : n * (step + 2)], ring, step)
        for step in range(3)
        for part, ring in ((a_sum, "x"), (b_sum, "z"))
    ]
    arrived = together(*arrived)

    def added(own, parts):
        return sum((p.astype(f32) for p in parts), own.astype(f32)).astype(bf16)

    a_sum, b_sum = added(a_sum[:n], arrived[0::2]), added(b_sum[:n], arrived[1::2])
    last = jnp.concatenate([a_sum, b_sum], axis=0).reshape(4, 8, width)
    last = lax.all_to_all(last, Y_AXES, 0, 0, tiled=True)
    hidden_grad = jnp.sum(last.astype(f32), axis=0).astype(bf16)
    return (loss, sampled_ratio, hidden_grad, head_grad)


def solution(mesh):
    split = Mesh(mesh.devices.reshape(2, 4, 4, 2, 2), TOK_VOC)
    in_specs = (P(TOK, None), P(None, TOK_VOC), P(TOK), P(TOK), P(None, TOK_VOC))
    out_specs = (P(), P(TOK_VOC), P(TOK_VOC, None), P(None, TOK_VOC))
    return jax.shard_map(
        per_device, mesh=split, in_specs=in_specs, out_specs=out_specs, check_vma=False
    )
```

```python
import functools

import jax
import jax.numpy as jnp
from jax import lax
from jax.experimental import pallas as pl
from jax.experimental.pallas import tpu as pltpu
from jax.sharding import Mesh
from jax.sharding import PartitionSpec as P

TOK = ("tok_0", "tok_1", "tok_2")
TOK_VOC = ("tok_0", "tok_1", "tok_2", "voc_0", "voc_1")
CORE = "voc_1"
Y_AXES = ("tok_0", "voc_0")
RING = {"x": ("tok_2", "voc_1"), "z": ("tok_1", "voc_1"), "y": ("tok_0", "voc_0", "voc_1")}
DIGIT_BITS = 6
DIGITS = 1 << DIGIT_BITS
EXTRA = 128
INTERPRET = False
XORS = ((1, 3, 2), (3, 1, 2))


def ring_index(ring, place, core):
    if ring == "y":
        return ((place % 2) * 2 + place // 2) * 2 + core
    return place * 2 + core


def swap(value, ring, step):
    pairs = [
        (ring_index(ring, p, c), ring_index(ring, p ^ XORS[c][step], c))
        for p in range(4)
        for c in range(2)
    ]
    return lax.ppermute(value, RING[ring], pairs)


def swap_core(value):
    return lax.ppermute(value, CORE, [(0, 1), (1, 0)])


def together(*values):
    return lax.optimization_barrier(values)


def token_of_rows(core, z, x, rows):
    n = lax.broadcasted_iota(jnp.int32, (rows, 1), 0)
    quarter = rows // 8
    half, part, top = n // (4 * quarter), (n // (2 * quarter)) % 2, (n // quarter) % 2
    high = half * 2 + top
    low = (n // (quarter // 4)) % 4
    mid = (n // 8) % 2
    first = jnp.where(core == 0, XORS[0][0], XORS[1][0])
    second = jnp.where(core == 0, XORS[0][1], XORS[1][1])

    def place(own, k):
        return own ^ ((k % 2) * first) ^ ((k // 2) * second)

    z_at = jnp.where(part == 0, place(z, high), place(z, low))
    x_at = jnp.where(part == 0, place(x, low), place(x, high))
    return ((((part * 4 + z_at) * 4 + x_at) * 2 + mid) * 2 + core) * 8 + n % 8


def one_hot(rows, columns, dtype):
    return (rows == lax.broadcasted_iota(jnp.int32, (1, columns), 1)).astype(dtype)


VMEM = pl.BlockSpec(memory_space=pltpu.VMEM)
SMEM = pl.BlockSpec(memory_space=pltpu.SMEM)
ANY = pl.BlockSpec(memory_space=pl.ANY)


def near(value):
    return value if INTERPRET else pltpu.with_memory_space_constraint(value, pltpu.VMEM)


def far(value):
    return value if INTERPRET else pltpu.with_memory_space_constraint(value, pltpu.HBM)


def call(kernel, operands, outs, in_specs=None, out_specs=None, flops=10**6, scratch=(), mib=16):
    in_specs = in_specs or [VMEM] * len(operands)
    out_specs = out_specs or [VMEM] * len(outs)
    shapes = [
        pltpu.VMEM(shape, dtype)
        if spec is VMEM and not INTERPRET
        else jax.ShapeDtypeStruct(shape, dtype)
        for (shape, dtype), spec in zip(outs, out_specs)
    ]
    operands = [near(v) if spec is VMEM else v for v, spec in zip(operands, in_specs)]
    return pl.pallas_call(
        kernel,
        out_shape=shapes,
        in_specs=in_specs,
        out_specs=out_specs,
        scratch_shapes=scratch,
        compiler_params=pltpu.CompilerParams(vmem_limit_bytes=mib << 20),
        cost_estimate=pl.CostEstimate(flops=flops, bytes_accessed=10**6, transcendentals=0),
        interpret=INTERPRET,
    )(*operands)


def entry_block(core, hidden, ids, mask):
    rows, width = hidden.shape

    def kernel(core_ref, hidden_ref, ids_ref, mask_ref, out_ref):
        lane = lax.broadcasted_iota(jnp.int32, (8, EXTRA), 1)
        for k in range(rows // 16):
            at = 8 * (2 * k + core_ref[0])
            out_ref[8 * k : 8 * k + 8, :width] = hidden_ref[pl.ds(pl.multiple_of(at, 8), 8), :]
            row = at + lax.broadcasted_iota(jnp.int32, (8, rows), 0)
            mine = row == lax.broadcasted_iota(jnp.int32, (8, rows), 1)
            one = jnp.sum(jnp.where(mine, ids_ref[...], 0), axis=1, keepdims=True)
            extra = jnp.where(
                lane == 0, jnp.sum(jnp.where(mine, mask_ref[...], 0), axis=1, keepdims=True), 0
            )
            for d in range(3):
                digit = (one >> (DIGIT_BITS * d)) & (DIGITS - 1)
                extra = jnp.where(lane == d + 1, digit, extra)
            out_ref[8 * k : 8 * k + 8, width:] = extra.astype(jnp.float32).astype(jnp.bfloat16)

    return call(
        kernel,
        (core[None], hidden, ids[None], mask[None]),
        [((rows // 2, width + EXTRA), jnp.bfloat16)],
        in_specs=[SMEM, VMEM, VMEM, VMEM],
    )[0]


def joined(*groups):
    sizes = [len(g) for g in groups]
    pieces = [p for g in groups for p in g]

    def kernel(*refs):
        ins, outs = list(refs[: len(pieces)]), refs[len(pieces) :]
        for out_ref, size in zip(outs, sizes):
            at = 0
            for _ in range(size):
                ref = ins.pop(0)
                out_ref[at : at + ref.shape[0]] = ref[...]
                at += ref.shape[0]

    outs = [((sum(p.shape[0] for p in g), g[0].shape[1]), g[0].dtype) for g in groups]
    return call(kernel, pieces, outs)


def added(groups, blocks):
    sizes = [len(g) for g in groups]
    parts = [p for g in groups for p in g]

    def kernel(*refs):
        ins, outs = list(refs[: len(parts)]), list(refs[len(parts) :])
        for size in sizes:
            terms = [ins.pop(0) for _ in range(size)]
            cut = terms[0].shape[0] // blocks
            for k in range(blocks):
                at = slice(k * cut, (k + 1) * cut)
                total = sum(t[at].astype(jnp.float32) for t in terms[1:])
                outs.pop(0)[...] = (total + terms[0][at].astype(jnp.float32)).astype(jnp.bfloat16)

    outs = [
        ((g[0].shape[0] // blocks, g[0].shape[1]), jnp.bfloat16) for g in groups for _ in range(blocks)
    ]
    return call(kernel, parts, outs)


def combined(parts, final=False):
    shape = parts[0].shape

    def kernel(*refs):
        ins, out_ref = refs[:-1], refs[-1]
        smax = functools.reduce(jnp.maximum, [r[0:1] for r in ins])
        tmax = functools.reduce(jnp.maximum, [r[3:4] for r in ins])
        stot = cross = ttot = pick = 0.0
        for r in ins:
            factor = jnp.exp(r[0:1] - smax)
            stot, cross = stot + r[1:2] * factor, cross + r[2:3] * factor
            ttot = ttot + r[4:5] * jnp.exp(r[3:4] - tmax)
            pick = pick + r[5:6]
        mask = ins[0][6:7]
        rows = [smax, stot, cross, tmax, ttot, pick, mask, mask]
        if final:
            student_shift, teacher_shift = smax + jnp.log(stot), tmax + jnp.log(ttot)
            apart = student_shift - teacher_shift
            row_kl = cross / stot - apart
            rows = [student_shift, apart + row_kl, row_kl, pick - apart] + [mask] * 4
        for k, row in enumerate(rows):
            out_ref[k : k + 1] = row

    return call(kernel, parts, [(shape, jnp.float32)])[0]


def side_by_side(head, head_in):
    width, columns = head.shape
    cuts = 4

    def kernel(h_ref, g_ref, out_ref, sems):
        copies = []
        for k in range(cuts):
            at = pl.ds(k * width // cuts, width // cuts)
            for ref, column in ((h_ref, 0), (g_ref, columns)):
                copies.append(
                    pltpu.make_async_copy(
                        ref.at[at], out_ref.at[at, pl.ds(column, columns)], sems.at[len(copies)]
                    )
                )
        for copy in copies:
            copy.start()
        for copy in copies:
            copy.wait()

    return call(
        kernel,
        (far(head), far(head_in)),
        [((width, 2 * columns), head.dtype)],
        in_specs=[ANY, ANY],
        scratch=[pltpu.SemaphoreType.DMA((2 * cuts,))],
        flops=4 * 10**9,
        mib=4,
    )[0]


def logits_and_stats(bases, a, b, heads, teacher, teacher_in, places, which, before=None):
    f32 = jnp.float32
    width, both = heads.shape
    columns = both // 2
    part, rows, tokens = a.shape[0], 2 * a.shape[0], places.shape[0]
    chunk = 32

    def kernel(base_ref, a_ref, b_ref, h_ref, t_ref, u_ref, p_ref, *rest):
        out_ref, stats_ref, states = rest[-3:]
        states[:part] = a_ref[:, :width]
        states[part:] = b_ref[:, :width]
        out_ref[...] = jnp.dot(states[...], h_ref[...], preferred_element_type=f32)
        lanes = lax.broadcasted_iota(jnp.int32, (1, both), 1)
        column = jnp.where(lanes < columns, base_ref[0] + lanes, base_ref[1] + lanes - columns)
        spots = lax.broadcasted_iota(jnp.int32, (1, tokens), 1)
        stats_ref[...] = jnp.zeros(stats_ref.shape, f32) if before is None else rest[0][...]
        for k in range(rows // chunk):
            ref, at = (a_ref, k * chunk) if k * chunk < part else (b_ref, k * chunk - part)
            here = slice(k * chunk, (k + 1) * chunk)
            there = slice(which * rows + k * chunk, which * rows + (k + 1) * chunk)
            student, note = out_ref[here, :], ref[at : at + chunk, width:].astype(f32)
            teacher = jnp.concatenate([t_ref[there, :], u_ref[there, :]], axis=1).astype(f32)
            ids = note[:, 1:2] + DIGITS * note[:, 2:3] + DIGITS**2 * note[:, 3:4]
            chosen = ids.astype(jnp.int32) == column
            smax = jnp.max(student, axis=1, keepdims=True)
            tmax = jnp.max(teacher, axis=1, keepdims=True)
            shifted = jnp.exp(student - smax)
            differ = student - teacher
            sums = [
                smax,
                jnp.sum(shifted, axis=1, keepdims=True),
                jnp.sum(shifted * differ, axis=1, keepdims=True),
                tmax,
                jnp.sum(jnp.exp(teacher - tmax), axis=1, keepdims=True),
                jnp.sum(jnp.where(chosen, differ, 0.0), axis=1, keepdims=True),
                note[:, :1],
            ]
            spot = p_ref[there, :] == spots
            for r, value in enumerate(sums):
                stats_ref[r : r + 1] += jnp.sum(jnp.where(spot, value, 0.0), axis=0, keepdims=True)

    operands = [bases, a, b, heads, teacher, teacher_in, places]
    if before is not None:
        operands.append(before)
    return call(
        kernel,
        operands,
        [((rows, both), f32), ((8, tokens), f32)],
        in_specs=[SMEM] + [VMEM] * (len(operands) - 1),
        scratch=[pltpu.VMEM((rows, width), jnp.bfloat16)],
        flops=2 * rows * width * both,
    )


def gradients(student, shifts, heads, teacher, teacher_in, places, which):
    f32, bf16 = jnp.float32, jnp.bfloat16
    width, both = heads.shape
    columns = both // 2
    rows, tokens = student.shape[0], places.shape[0]
    part = rows // 2
    chunk, cuts = 32, 7

    def kernel(s_ref, c_ref, h_ref, t_ref, u_ref, p_ref, a_ref, b_ref, d_ref, e_ref, all_d):
        spots = lax.broadcasted_iota(jnp.int32, (1, tokens), 1)
        for k in range(rows // chunk):
            here = slice(k * chunk, (k + 1) * chunk)
            there = slice(which * rows + k * chunk, which * rows + (k + 1) * chunk)
            spot = p_ref[there, :] == spots

            def of_row(r):
                return jnp.sum(jnp.where(spot, c_ref[r : r + 1], 0.0), axis=1, keepdims=True)

            student = s_ref[here, :]
            teacher = jnp.concatenate([t_ref[there, :], u_ref[there, :]], axis=1).astype(f32)
            probs = of_row(4) * jnp.exp(student - of_row(0))
            found = (probs * (student - teacher - of_row(1))).astype(bf16)
            all_d[here, :] = found
            d_ref[here, :] = found[:, :columns]
            e_ref[here, :] = found[:, columns:]
        for k in range(cuts):
            at = slice(k * width // cuts, (k + 1) * width // cuts)
            product = lax.dot_general(
                all_d[...], h_ref[at, :], (((1,), (1,)), ((), ())), preferred_element_type=f32
            ).astype(bf16)
            a_ref[:, at] = product[:part]
            b_ref[:, at] = product[part:]

    return call(
        kernel,
        [student, shifts, heads, teacher, teacher_in, places],
        [((part, width), bf16)] * 2 + [((rows, columns), bf16)] * 2,
        scratch=[pltpu.VMEM((rows, both), bf16)],
        flops=2 * rows * width * both,
    )


def head_gradient(states, dlogits, width):
    bf16 = jnp.bfloat16
    columns = dlogits[0].shape[1]
    block = 512
    tokens = sum(d.shape[0] for d in dlogits)
    n = len(states)

    def kernel(*refs):
        pieces, others = refs[:n], refs[n:-5]
        out_ref, left, right, found, sems = refs[-5:]
        at = 0
        for ref in others:
            right[at : at + ref.shape[0]] = ref[...]
            at += ref.shape[0]
        copies = []
        for k in range(width // block):
            at = 0
            for ref in pieces:
                left[at : at + ref.shape[0]] = ref[:, k * block : (k + 1) * block]
                at += ref.shape[0]
            product = lax.dot_general(
                left[...], right[...], (((0,), (0,)), ((), ())), preferred_element_type=jnp.float32
            ).astype(bf16)
            slot = k % 2
            if k >= 2:
                copies[k - 2].wait()
            found[slot] = product
            copies.append(
                pltpu.make_async_copy(
                    found.at[slot], out_ref.at[pl.ds(k * block, block)], sems.at[slot]
                )
            )
            copies[k].start()
        copies[-2].wait()
        copies[-1].wait()

    return call(
        kernel,
        [*states, *dlogits],
        [((width, columns), bf16)],
        out_specs=[ANY],
        scratch=[
            pltpu.VMEM((tokens, block), bf16),
            pltpu.VMEM((tokens, columns), bf16),
            pltpu.VMEM((2, block, columns), bf16),
            pltpu.SemaphoreType.DMA((2,)),
        ],
        flops=2 * tokens * width * columns,
    )[0]


def per_device(hidden, teacher_logits, sampled_ids, loss_mask, student_head):
    f32, bf16 = jnp.float32, jnp.bfloat16
    core, y_low = lax.axis_index(CORE), lax.axis_index("tok_0")
    z, x = lax.axis_index("tok_1"), lax.axis_index("tok_2")
    position = lax.axis_index(TOK_VOC)
    width, columns = student_head.shape
    tokens = teacher_logits.shape[0]
    rows = tokens // 2

    block = entry_block(core, hidden, sampled_ids, loss_mask)
    head_in = swap_core(student_head)
    token = token_of_rows(core, z, x, rows)
    token_other = token_of_rows(1 - core, z, x, rows)
    places = (token // 16) * 8 + token % 8
    other = swap(block, "y", 0)
    teacher_send = jnp.dot(one_hot(token_other, tokens, bf16), teacher_logits)
    other, teacher_send = together(other, teacher_send)
    teacher_in = swap_core(teacher_send)
    near_a = jnp.where(y_low == 0, block, other)
    near_b = jnp.where(y_low == 0, other, block)

    pieces_a, pieces_b = [near_a], [near_b]
    for step in range(3):
        pieces_a.append(swap(near_a, "x", step))
        pieces_b.append(swap(near_b, "z", step))
    teacher = jnp.dot(one_hot(token, tokens, bf16), teacher_logits)
    *pieces, teacher = together(*pieces_a, *pieces_b, teacher)
    near_a, near_b = joined(pieces[:4], pieces[4:])

    far_a, far_b = swap(near_a, "z", 0), swap(near_b, "x", 0)
    heads = side_by_side(student_head, head_in)
    far_a, far_b, heads = together(far_a, far_b, heads)
    near_a, near_b = joined((near_a, far_a), (near_b, far_b))

    far_a, far_b = swap(near_a, "z", 1), swap(near_b, "x", 1)
    bases = jnp.stack([position, position ^ 1]) * columns
    shared = (heads, teacher, teacher_in, places)
    near_other = swap_core(near_a), swap_core(near_b)
    student_near, stats = logits_and_stats(bases, near_a, near_b, *shared, 0)
    far_a, far_b, student_near, stats = together(far_a, far_b, student_near, stats)
    student_far, stats = logits_and_stats(bases, far_a, far_b, *shared, 1, stats)
    far_other = swap_core(far_a), swap_core(far_b)
    for ring in ("x", "z", "y"):
        parts = [stats, *(swap(stats, ring, step) for step in range(3))]
        stats = combined(parts, ring == "y")

    far_sum_a, far_sum_b, *far_d = gradients(student_far, stats, *shared, 1)
    far_sum_a, far_sum_b, stats_later = together(far_sum_a, far_sum_b, stats)
    a_in, b_in = swap(far_sum_a, "z", 1), swap(far_sum_b, "x", 1)
    far_d_in = swap_core(far_d[1])
    near_sum_a, near_sum_b, *near_d = gradients(student_near, stats_later, *shared, 0)
    near_d_in = swap_core(near_d[1])
    head_grad = head_gradient(
        (near_a, near_b, far_a, far_b, *near_other, *far_other),
        (near_d[0], far_d[0], near_d_in, far_d_in),
        width,
    )
    a_in, b_in, near_sum_a, near_sum_b, head_grad = together(
        a_in, b_in, near_sum_a, near_sum_b, head_grad
    )
    keep_a, send_a, keep_b, send_b = added(((near_sum_a, a_in), (near_sum_b, b_in)), 2)
    a_in, b_in = together(swap(send_a, "z", 0), swap(send_b, "x", 0))
    keep_a, *send_a, keep_b, s0, s1, s2 = added(((keep_a, a_in), (keep_b, b_in)), 4)
    arrived = [
        swap(part, ring, step)
        for step in range(3)
        for part, ring in ((send_a[step], "x"), ((s0, s1, s2)[step], "z"))
    ]
    chip = position // 2
    sampled_ratio = lax.dynamic_slice(stats_later, (3, chip * 8), (1, 8))[0]
    sums = jnp.stack([jnp.sum(stats_later[4] * stats_later[2]), jnp.sum(stats_later[4])])
    sums = sums + swap_core(sums)
    loss = sums[0] / sums[1]
    arrived = together(*arrived)
    a_sum, b_sum = added(((keep_a, *arrived[0::2]), (keep_b, *arrived[1::2])), 1)
    last = jnp.concatenate([a_sum, b_sum], axis=0).reshape(4, 8, width)
    last = lax.all_to_all(last, Y_AXES, 0, 0, tiled=True)
    hidden_grad = jnp.sum(last.astype(f32), axis=0).astype(bf16)
    return (loss, sampled_ratio, hidden_grad, head_grad)


def solution(mesh):
    split = Mesh(mesh.devices.reshape(2, 4, 4, 2, 2), TOK_VOC)
    in_specs = (P(TOK, None), P(None, TOK_VOC), P(TOK), P(TOK), P(None, TOK_VOC))
    out_specs = (P(), P(TOK_VOC), P(TOK_VOC, None), P(None, TOK_VOC))
    return jax.shard_map(
        per_device, mesh=split, in_specs=in_specs, out_specs=out_specs, check_vma=False
    )
```

```python
import functools
import itertools

import jax
import jax.numpy as jnp
from jax import lax
from jax.experimental import pallas as pl
from jax.experimental.pallas import tpu as pltpu
from jax.sharding import Mesh
from jax.sharding import PartitionSpec as P

TOK = ("tok_0", "tok_1", "tok_2")
TOK_VOC = ("tok_0", "tok_1", "tok_2", "voc_0", "voc_1")
CORE = "voc_1"
Y_AXES = ("tok_0", "voc_0")
RING = {"x": ("tok_2", "voc_1"), "z": ("tok_1", "voc_1"), "y": ("tok_0", "voc_0", "voc_1")}
DIGIT_BITS = 6
DIGITS = 1 << DIGIT_BITS
EXTRA = 128
INTERPRET = False
XORS = ((1, 3, 2), (3, 1, 2))


def ring_index(ring, place, core):
    if ring == "y":
        return ((place % 2) * 2 + place // 2) * 2 + core
    return place * 2 + core


def swap(value, ring, step):
    pairs = [
        (ring_index(ring, p, c), ring_index(ring, p ^ XORS[c][step], c))
        for p in range(4)
        for c in range(2)
    ]
    return lax.ppermute(value, RING[ring], pairs)


def swap_core(value):
    return lax.ppermute(value, CORE, [(0, 1), (1, 0)])


def spread(value, k, across):
    pairs = []
    for y, z, x, c in itertools.product(range(4), range(4), range(4), range(2)):
        step = (0, *XORS[c])[k]
        to_z, to_x = (z, x ^ step) if y % 2 == 0 else (z ^ step, x)
        to_y = y ^ XORS[c][0] if across else y
        pairs.append(
            tuple(
                ((((v % 2) * 4 + w) * 4 + u) * 2 + v // 2) * 2 + c
                for v, w, u in ((y, z, x), (to_y, to_z, to_x))
            )
        )
    return lax.ppermute(value, TOK_VOC, pairs)


def together(*values):
    return lax.optimization_barrier(values)


def token_of_rows(core, z, x, rows):
    n = lax.broadcasted_iota(jnp.int32, (rows, 1), 0)
    quarter = rows // 8
    half, part, top = n // (4 * quarter), (n // (2 * quarter)) % 2, (n // quarter) % 2
    high = half * 2 + top
    low = (n // (quarter // 4)) % 4
    mid = (n // 8) % 2
    first = jnp.where(core == 0, XORS[0][0], XORS[1][0])
    second = jnp.where(core == 0, XORS[0][1], XORS[1][1])

    def place(own, k):
        return own ^ ((k % 2) * first) ^ ((k // 2) * second)

    z_at = jnp.where(part == 0, place(z, high), place(z, low))
    x_at = jnp.where(part == 0, place(x, low), place(x, high))
    return ((((part * 4 + z_at) * 4 + x_at) * 2 + mid) * 2 + core) * 8 + n % 8


def one_hot(rows, columns, dtype):
    return (rows == lax.broadcasted_iota(jnp.int32, (1, columns), 1)).astype(dtype)


VMEM = pl.BlockSpec(memory_space=pltpu.VMEM)
SMEM = pl.BlockSpec(memory_space=pltpu.SMEM)
ANY = pl.BlockSpec(memory_space=pl.ANY)


def near(value):
    return value if INTERPRET else pltpu.with_memory_space_constraint(value, pltpu.VMEM)


def far(value):
    return value if INTERPRET else pltpu.with_memory_space_constraint(value, pltpu.HBM)


def call(kernel, operands, outs, in_specs=None, out_specs=None, flops=10**6, scratch=(), mib=16, aliases={}):
    in_specs = in_specs or [VMEM] * len(operands)
    out_specs = out_specs or [VMEM] * len(outs)
    shapes = [
        pltpu.VMEM(shape, dtype)
        if spec is VMEM and not INTERPRET
        else jax.ShapeDtypeStruct(shape, dtype)
        for (shape, dtype), spec in zip(outs, out_specs)
    ]
    operands = [near(v) if spec is VMEM else v for v, spec in zip(operands, in_specs)]
    return pl.pallas_call(
        kernel,
        out_shape=shapes,
        in_specs=in_specs,
        out_specs=out_specs,
        scratch_shapes=scratch,
        input_output_aliases=aliases,
        compiler_params=pltpu.CompilerParams(vmem_limit_bytes=mib << 20),
        cost_estimate=pl.CostEstimate(flops=flops, bytes_accessed=10**6, transcendentals=0),
        interpret=INTERPRET,
    )(*operands)


def entry_block(core, hidden, ids, mask):
    rows, width = hidden.shape

    def kernel(core_ref, hidden_ref, ids_ref, mask_ref, out_ref, ints, sems):
        starts = [8 * (2 * k + core_ref[0]) for k in range(rows // 16)]
        copies = [
            pltpu.make_async_copy(ids_ref, ints.at[pl.ds(0, 1)], sems.at[0]),
            pltpu.make_async_copy(mask_ref, ints.at[pl.ds(8, 1)], sems.at[1]),
        ]
        for k, at in enumerate(starts):
            copies.append(
                pltpu.make_async_copy(
                    hidden_ref.at[pl.ds(pl.multiple_of(at, 8), 8)],
                    out_ref.at[pl.ds(8 * k, 8), pl.ds(0, width)],
                    sems.at[2 + k],
                )
            )
        for copy in copies:
            copy.start()
        copies[0].wait()
        copies[1].wait()
        lane = lax.broadcasted_iota(jnp.int32, (8, EXTRA), 1)
        for k, at in enumerate(starts):
            row = at + lax.broadcasted_iota(jnp.int32, (8, rows), 0)
            mine = row == lax.broadcasted_iota(jnp.int32, (8, rows), 1)
            one = jnp.sum(jnp.where(mine, ints[0:1], 0), axis=1, keepdims=True)
            extra = jnp.where(
                lane == 0, jnp.sum(jnp.where(mine, ints[8:9], 0), axis=1, keepdims=True), 0
            )
            for d in range(3):
                digit = (one >> (DIGIT_BITS * d)) & (DIGITS - 1)
                extra = jnp.where(lane == d + 1, digit, extra)
            out_ref[8 * k : 8 * k + 8, width:] = extra.astype(jnp.float32).astype(jnp.bfloat16)
        for copy in copies[2:]:
            copy.wait()

    return call(
        kernel,
        (core[None], hidden, ids[None], mask[None]),
        [((rows // 2, width + EXTRA), jnp.bfloat16)],
        in_specs=[SMEM, ANY, ANY, ANY],
        scratch=[pltpu.VMEM((16, rows), jnp.int32), pltpu.SemaphoreType.DMA((2 + rows // 16,))],
        mib=2,
    )[0]


def joined(first, second, swapped=None, after=None):
    n = len(first)
    height = first[0].shape[0]

    def kernel(*refs):
        ins, (first_ref, second_ref) = refs[: 2 * n], refs[-2:]

        def put(one, two):
            for k in range(n):
                one[k * height : (k + 1) * height] = ins[k][...]
                two[k * height : (k + 1) * height] = ins[n + k][...]

        if swapped is None:
            put(first_ref, second_ref)
        else:
            pl.when(refs[2 * n][0] == 0)(lambda: put(first_ref, second_ref))
            pl.when(refs[2 * n][0] != 0)(lambda: put(second_ref, first_ref))

    operands = [*first, *second]
    specs = [VMEM] * (2 * n)
    if swapped is not None:
        operands, specs = [*operands, swapped[None]], [*specs, SMEM]
    if after is not None:
        operands, specs = [*operands, after], [*specs, VMEM]
    out = ((n * height, first[0].shape[1]), first[0].dtype)
    return call(kernel, operands, [out, out], in_specs=specs, mib=4)


def added(groups, blocks):
    sizes = [len(g) for g in groups]
    parts = [p for g in groups for p in g]

    def kernel(*refs):
        ins, outs = list(refs[: len(parts)]), list(refs[len(parts) :])
        for size in sizes:
            terms = [ins.pop(0) for _ in range(size)]
            cut = terms[0].shape[0] // blocks
            for k in range(blocks):
                at = slice(k * cut, (k + 1) * cut)
                total = sum(t[at].astype(jnp.float32) for t in terms[1:])
                outs.pop(0)[...] = (total + terms[0][at].astype(jnp.float32)).astype(jnp.bfloat16)

    outs = [
        ((g[0].shape[0] // blocks, g[0].shape[1]), jnp.bfloat16) for g in groups for _ in range(blocks)
    ]
    return call(kernel, parts, outs, mib=4)


def added_by_place(groups, order):
    sizes = [len(g) for g in groups]
    parts = [p for g in groups for p in g]
    rows, width = parts[0].shape

    def kernel(order_ref, *refs):
        ins, outs, sums = list(refs[: len(parts)]), refs[len(parts) : -1], refs[-1]
        for k, size in enumerate(sizes):
            terms = [ins.pop(0) for _ in range(size)]
            sums[k * rows : (k + 1) * rows] = sum(t[...].astype(jnp.float32) for t in terms)
        for k, out_ref in enumerate(outs):
            at = pl.multiple_of(order_ref[k] * 8, 8)
            out_ref[...] = sums[pl.ds(at, 8), :].astype(jnp.bfloat16)

    blocks = len(groups) * rows // 8
    return call(
        kernel,
        [order, *parts],
        [((8, width), jnp.bfloat16)] * blocks,
        in_specs=[SMEM] + [VMEM] * len(parts),
        scratch=[pltpu.VMEM((len(groups) * rows, width), jnp.float32)],
        mib=4,
    )


def combined(parts, final=False):
    shape = parts[0].shape

    def kernel(*refs):
        ins, out_ref = refs[:-1], refs[-1]
        smax = functools.reduce(jnp.maximum, [r[0:1] for r in ins])
        tmax = functools.reduce(jnp.maximum, [r[3:4] for r in ins])
        stot = cross = ttot = pick = 0.0
        for r in ins:
            factor = jnp.exp(r[0:1] - smax)
            stot, cross = stot + r[1:2] * factor, cross + r[2:3] * factor
            ttot = ttot + r[4:5] * jnp.exp(r[3:4] - tmax)
            pick = pick + r[5:6]
        mask = ins[0][6:7]
        rows = [smax, stot, cross, tmax, ttot, pick, mask, mask]
        if final:
            student_shift, teacher_shift = smax + jnp.log(stot), tmax + jnp.log(ttot)
            apart = student_shift - teacher_shift
            row_kl = cross / stot - apart
            rows = [student_shift, apart + row_kl, row_kl, pick - apart] + [mask] * 4
        for k, row in enumerate(rows):
            out_ref[k : k + 1] = row

    return call(kernel, parts, [(shape, jnp.float32)], mib=2)[0]


def side_by_side(head, head_in):
    width, columns = head.shape
    cuts = 4

    def kernel(h_ref, g_ref, out_ref, mark_ref, sems):
        mark_ref[...] = jnp.zeros(mark_ref.shape, jnp.float32)
        copies = []
        for k in range(cuts):
            at = pl.ds(k * width // cuts, width // cuts)
            for ref, column in ((h_ref, 0), (g_ref, columns)):
                copies.append(
                    pltpu.make_async_copy(
                        ref.at[at], out_ref.at[at, pl.ds(column, columns)], sems.at[len(copies)]
                    )
                )
        for copy in copies:
            copy.start()
        for copy in copies:
            copy.wait()

    return call(
        kernel,
        (far(head), far(head_in)),
        [((width, 2 * columns), head.dtype), ((8, 128), jnp.float32)],
        in_specs=[ANY, ANY],
        scratch=[pltpu.SemaphoreType.DMA((2 * cuts,))],
        flops=4 * 10**9,
        mib=2,
    )


def logits_and_stats(bases, a, b, heads, teacher, teacher_in, places, which, before=None):
    f32 = jnp.float32
    width, both = heads.shape
    columns = both // 2
    part, rows, tokens = a.shape[0], 2 * a.shape[0], places.shape[0]
    chunk = 32

    def kernel(base_ref, a_ref, b_ref, h_ref, t_ref, u_ref, p_ref, *rest):
        out_ref, stats_ref, states, placed = rest[-4:]
        states[:part] = a_ref[:, :width]
        states[part:] = b_ref[:, :width]
        out_ref[...] = jnp.dot(states[...], h_ref[...], preferred_element_type=f32)
        lanes = lax.broadcasted_iota(jnp.int32, (1, both), 1)
        column = jnp.where(lanes < columns, base_ref[0] + lanes, base_ref[1] + lanes - columns)
        spots = lax.broadcasted_iota(jnp.int32, (1, tokens), 1)
        placed[...] = jnp.zeros(placed.shape, f32)
        for k in range(rows // chunk):
            ref, at = (a_ref, k * chunk) if k * chunk < part else (b_ref, k * chunk - part)
            here = slice(k * chunk, (k + 1) * chunk)
            there = slice(which * rows + k * chunk, which * rows + (k + 1) * chunk)
            student, note = out_ref[here, :], ref[at : at + chunk, width:].astype(f32)
            teacher = jnp.concatenate([t_ref[there, :], u_ref[there, :]], axis=1).astype(f32)
            ids = note[:, 1:2] + DIGITS * note[:, 2:3] + DIGITS**2 * note[:, 3:4]
            chosen = ids.astype(jnp.int32) == column
            smax = jnp.max(student, axis=1, keepdims=True)
            tmax = jnp.max(teacher, axis=1, keepdims=True)
            shifted = jnp.exp(student - smax)
            differ = student - teacher
            sums = [
                smax,
                jnp.sum(shifted, axis=1, keepdims=True),
                jnp.sum(shifted * differ, axis=1, keepdims=True),
                tmax,
                jnp.sum(jnp.exp(teacher - tmax), axis=1, keepdims=True),
                jnp.sum(jnp.where(chosen, differ, 0.0), axis=1, keepdims=True),
                note[:, :1],
            ]
            spot = p_ref[there, :] == spots
            for r, value in enumerate(sums):
                found = jnp.where(spot, value, 0.0).reshape(chunk // 8, 8, tokens)
                placed[r] += jnp.sum(found, axis=0)
        for r in range(8):
            row = jnp.sum(placed[r], axis=0, keepdims=True)
            stats_ref[r : r + 1] = row if before is None else row + rest[0][r : r + 1]

    operands = [bases, a, b, heads, teacher, teacher_in, places]
    if before is not None:
        operands.append(before)
    return call(
        kernel,
        operands,
        [((rows, both), f32), ((8, tokens), f32)],
        in_specs=[SMEM] + [VMEM] * (len(operands) - 1),
        scratch=[pltpu.VMEM((rows, width), jnp.bfloat16), pltpu.VMEM((8, 8, tokens), f32)],
        flops=2 * rows * width * both,
    )


def gradients(student, shifts, heads, teacher, teacher_in, places, which):
    f32, bf16 = jnp.float32, jnp.bfloat16
    width, both = heads.shape
    columns = both // 2
    rows, tokens = student.shape[0], places.shape[0]
    part = rows // 2
    chunk, cuts = 32, 7

    def kernel(s_ref, c_ref, h_ref, t_ref, u_ref, p_ref, a_ref, b_ref, d_ref, e_ref, all_d):
        spots = lax.broadcasted_iota(jnp.int32, (1, tokens), 1)
        for k in range(rows // chunk):
            here = slice(k * chunk, (k + 1) * chunk)
            there = slice(which * rows + k * chunk, which * rows + (k + 1) * chunk)
            spot = p_ref[there, :] == spots

            def of_row(r):
                return jnp.sum(jnp.where(spot, c_ref[r : r + 1], 0.0), axis=1, keepdims=True)

            student = s_ref[here, :]
            teacher = jnp.concatenate([t_ref[there, :], u_ref[there, :]], axis=1).astype(f32)
            probs = of_row(4) * jnp.exp(student - of_row(0))
            found = (probs * (student - teacher - of_row(1))).astype(bf16)
            all_d[here, :] = found
            d_ref[here, :] = found[:, :columns]
            e_ref[here, :] = found[:, columns:]
        for k in range(cuts):
            at = slice(k * width // cuts, (k + 1) * width // cuts)
            product = lax.dot_general(
                all_d[...], h_ref[at, :], (((1,), (1,)), ((), ())), preferred_element_type=f32
            ).astype(bf16)
            a_ref[:, at] = product[:part]
            b_ref[:, at] = product[part:]

    return call(
        kernel,
        [student, shifts, heads, teacher, teacher_in, places],
        [((part, width), bf16)] * 2 + [((rows, columns), bf16)] * 2,
        scratch=[pltpu.VMEM((rows, both), bf16)],
        flops=2 * rows * width * both,
    )


def head_gradient(states, dlogits, width, blocks, before=None):
    bf16 = jnp.bfloat16
    columns = dlogits[0].shape[1]
    block = 512
    tokens = sum(d.shape[0] for d in dlogits)
    n = len(states)
    m = n + len(dlogits)

    def kernel(*refs):
        pieces, others = refs[:n], refs[n:m]
        out_ref, left, right, found, sems = refs[-5:]
        at = 0
        for ref in others:
            right[at : at + ref.shape[0]] = ref[...]
            at += ref.shape[0]
        copies = []
        for j, k in enumerate(blocks):
            at = 0
            for ref in pieces:
                left[at : at + ref.shape[0]] = ref[:, k * block : (k + 1) * block]
                at += ref.shape[0]
            product = lax.dot_general(
                left[...], right[...], (((0,), (0,)), ((), ())), preferred_element_type=jnp.float32
            ).astype(bf16)
            slot = j % 2
            if j >= 2:
                copies[j - 2].wait()
            found[slot] = product
            copies.append(
                pltpu.make_async_copy(
                    found.at[slot], out_ref.at[pl.ds(k * block, block)], sems.at[slot]
                )
            )
            copies[j].start()
        copies[-2].wait()
        copies[-1].wait()

    operands, specs = [*states, *dlogits], [VMEM] * m
    if before is not None:
        operands, specs = [*operands, before], [*specs, ANY]
    return call(
        kernel,
        operands,
        [((width, columns), bf16)],
        in_specs=specs,
        out_specs=[ANY],
        scratch=[
            pltpu.VMEM((tokens, block), bf16),
            pltpu.VMEM((tokens, columns), bf16),
            pltpu.VMEM((2, block, columns), bf16),
            pltpu.SemaphoreType.DMA((2,)),
        ],
        flops=2 * tokens * len(blocks) * block * columns,
        aliases={} if before is None else {m: 0},
    )[0]


def per_device(hidden, teacher_logits, sampled_ids, loss_mask, student_head):
    f32, bf16 = jnp.float32, jnp.bfloat16
    core, y_low = lax.axis_index(CORE), lax.axis_index("tok_0")
    z, x = lax.axis_index("tok_1"), lax.axis_index("tok_2")
    position = lax.axis_index(TOK_VOC)
    width, columns = student_head.shape
    tokens = teacher_logits.shape[0]
    rows = tokens // 2

    block = entry_block(core, hidden, sampled_ids, loss_mask)
    head_in = swap_core(student_head)
    token = token_of_rows(core, z, x, rows)
    token_other = token_of_rows(1 - core, z, x, rows)
    places = (token // 16) * 8 + token % 8
    pieces = [block, *(spread(block, k, False) for k in range(1, 4))]
    pieces += [spread(block, k, True) for k in range(4)]
    teacher_send = jnp.dot(one_hot(token_other, tokens, bf16), teacher_logits)
    teacher_in = swap_core(teacher_send)
    teacher = jnp.dot(one_hot(token, tokens, bf16), teacher_logits)
    *pieces, teacher, places = together(*pieces, teacher, places)
    near_a, near_b = joined(pieces[:4], pieces[4:], y_low)

    far_a, far_b = swap(near_a, "z", 0), swap(near_b, "x", 0)
    heads, mark = side_by_side(student_head, head_in)
    near_a, near_b = joined((near_a, far_a), (near_b, far_b), after=mark)

    far_a, far_b = swap(near_a, "z", 1), swap(near_b, "x", 1)
    bases = jnp.stack([position, position ^ 1]) * columns
    shared = (heads, teacher, teacher_in, places)
    near_other = swap_core(near_a), swap_core(near_b)
    student_near, stats = logits_and_stats(bases, near_a, near_b, *shared, 0)
    far_a, far_b, student_near, stats = together(far_a, far_b, student_near, stats)
    student_far, stats = logits_and_stats(bases, far_a, far_b, *shared, 1, stats)
    far_other = swap_core(far_a), swap_core(far_b)
    for ring in ("x", "z", "y"):
        parts = [stats, *(swap(stats, ring, step) for step in range(3))]
        stats = combined(parts, ring == "y")

    far_sum_a, far_sum_b, *far_d = gradients(student_far, stats, *shared, 1)
    far_sum_a, far_sum_b, stats_later = together(far_sum_a, far_sum_b, stats)
    a_in, b_in = swap(far_sum_a, "z", 1), swap(far_sum_b, "x", 1)
    far_d_in = swap_core(far_d[1])
    near_sum_a, near_sum_b, *near_d = gradients(student_near, stats_later, *shared, 0)
    near_d_in = swap_core(near_d[1])
    states = (near_a, near_b, far_a, far_b, *near_other, *far_other)
    all_d = (near_d[0], far_d[0], near_d_in, far_d_in)
    head_grad = head_gradient(states, all_d, width, range(4))
    a_in, b_in, near_sum_a, near_sum_b, head_grad = together(
        a_in, b_in, near_sum_a, near_sum_b, head_grad
    )
    keep_a, send_a, keep_b, send_b = added(((near_sum_a, a_in), (near_sum_b, b_in)), 2)
    a_in, b_in = swap(send_a, "z", 0), swap(send_b, "x", 0)
    chip = position // 2
    sampled_ratio = lax.dynamic_slice(stats_later, (3, chip * 8), (1, 8))[0]
    sums = jnp.stack([jnp.sum(stats_later[4] * stats_later[2]), jnp.sum(stats_later[4])])
    sums = sums + swap_core(sums)
    loss = sums[0] / sums[1]
    head_grad = head_gradient(states, all_d, width, range(4, width // 512), head_grad)
    a_in, b_in, head_grad, loss, sampled_ratio = together(a_in, b_in, head_grad, loss, sampled_ratio)
    keep_a, *send_a, keep_b, s0, s1, s2 = added(((keep_a, a_in), (keep_b, b_in)), 4)
    arrived = [
        swap(part, ring, step)
        for step in range(3)
        for part, ring in ((send_a[step], "x"), ((s0, s1, s2)[step], "z"))
    ]
    arrived = together(*arrived)
    y = lax.axis_index("voc_0") * 2 + y_low
    xors = [0] + [jnp.where(core == 0, XORS[0][k], XORS[1][k]) for k in range(3)]
    order = jnp.stack([((y ^ k) % 2) * 2 + (y ^ k) // 2 for k in xors])
    keep, *send = added_by_place(((keep_a, *arrived[0::2]), (keep_b, *arrived[1::2])), order)
    arrived = [swap(part, "y", step) for step, part in enumerate(send)]
    hidden_grad = sum((p.astype(f32) for p in arrived), keep.astype(f32)).astype(bf16)
    return (loss, sampled_ratio, hidden_grad, head_grad)


def solution(mesh):
    split = Mesh(mesh.devices.reshape(2, 4, 4, 2, 2), TOK_VOC)
    in_specs = (P(TOK, None), P(None, TOK_VOC), P(TOK), P(TOK), P(None, TOK_VOC))
    out_specs = (P(), P(TOK_VOC), P(TOK_VOC, None), P(None, TOK_VOC))
    return jax.shard_map(
        per_device, mesh=split, in_specs=in_specs, out_specs=out_specs, check_vma=False
    )
```

```python
import functools

import jax
import jax.numpy as jnp
from jax import lax
from jax.experimental import pallas as pl
from jax.experimental.pallas import tpu as pltpu
from jax.sharding import Mesh
from jax.sharding import PartitionSpec as P

TOK = ("tok_0", "tok_1", "tok_2")
TOK_VOC = ("tok_0", "tok_1", "tok_2", "voc_0", "voc_1")
CORE = "voc_1"
Y_AXES = ("tok_0", "voc_0")
RING = {"x": ("tok_2", "voc_1"), "z": ("tok_1", "voc_1"), "y": ("tok_0", "voc_0", "voc_1")}
DIGIT_BITS = 6
DIGITS = 1 << DIGIT_BITS
EXTRA = 128
INTERPRET = False
XORS = ((1, 3, 2), (3, 1, 2))


def ring_index(ring, place, core):
    if ring == "y":
        return ((place % 2) * 2 + place // 2) * 2 + core
    return place * 2 + core


def swap(value, ring, step):
    pairs = [
        (ring_index(ring, p, c), ring_index(ring, p ^ XORS[c][step], c))
        for p in range(4)
        for c in range(2)
    ]
    return lax.ppermute(value, RING[ring], pairs)


def swap_core(value):
    return lax.ppermute(value, CORE, [(0, 1), (1, 0)])


def together(*values):
    return lax.optimization_barrier(values)


def token_of_rows(core, z, x, rows):
    n = lax.broadcasted_iota(jnp.int32, (rows, 1), 0)
    quarter = rows // 8
    half, part, top = n // (4 * quarter), (n // (2 * quarter)) % 2, (n // quarter) % 2
    high = half * 2 + top
    low = (n // (quarter // 4)) % 4
    mid = (n // 8) % 2
    first = jnp.where(core == 0, XORS[0][0], XORS[1][0])
    second = jnp.where(core == 0, XORS[0][1], XORS[1][1])

    def place(own, k):
        return own ^ ((k % 2) * first) ^ ((k // 2) * second)

    z_at = jnp.where(part == 0, place(z, high), place(z, low))
    x_at = jnp.where(part == 0, place(x, low), place(x, high))
    return ((((part * 4 + z_at) * 4 + x_at) * 2 + mid) * 2 + core) * 8 + n % 8


def one_hot(rows, columns, dtype):
    return (rows == lax.broadcasted_iota(jnp.int32, (1, columns), 1)).astype(dtype)


VMEM = pl.BlockSpec(memory_space=pltpu.VMEM)
SMEM = pl.BlockSpec(memory_space=pltpu.SMEM)
ANY = pl.BlockSpec(memory_space=pl.ANY)


def near(value):
    return value if INTERPRET else pltpu.with_memory_space_constraint(value, pltpu.VMEM)


def far(value):
    return value if INTERPRET else pltpu.with_memory_space_constraint(value, pltpu.HBM)


def call(kernel, operands, outs, in_specs=None, out_specs=None, flops=10**6, scratch=(), mib=16):
    in_specs = in_specs or [VMEM] * len(operands)
    out_specs = out_specs or [VMEM] * len(outs)
    shapes = [
        pltpu.VMEM(shape, dtype)
        if spec is VMEM and not INTERPRET
        else jax.ShapeDtypeStruct(shape, dtype)
        for (shape, dtype), spec in zip(outs, out_specs)
    ]
    operands = [near(v) if spec is VMEM else v for v, spec in zip(operands, in_specs)]
    return pl.pallas_call(
        kernel,
        out_shape=shapes,
        in_specs=in_specs,
        out_specs=out_specs,
        scratch_shapes=scratch,
        compiler_params=pltpu.CompilerParams(vmem_limit_bytes=mib << 20),
        cost_estimate=pl.CostEstimate(flops=flops, bytes_accessed=10**6, transcendentals=0),
        interpret=INTERPRET,
    )(*operands)


def entry_block(core, hidden, ids, mask):
    rows, width = hidden.shape

    def kernel(core_ref, hidden_ref, ids_ref, mask_ref, out_ref, ints, sems):
        starts = [8 * (2 * k + core_ref[0]) for k in range(rows // 16)]
        copies = [
            pltpu.make_async_copy(ids_ref, ints.at[pl.ds(0, 1)], sems.at[0]),
            pltpu.make_async_copy(mask_ref, ints.at[pl.ds(8, 1)], sems.at[1]),
        ]
        for k, at in enumerate(starts):
            copies.append(
                pltpu.make_async_copy(
                    hidden_ref.at[pl.ds(pl.multiple_of(at, 8), 8)],
                    out_ref.at[pl.ds(8 * k, 8), pl.ds(0, width)],
                    sems.at[2 + k],
                )
            )
        for copy in copies:
            copy.start()
        copies[0].wait()
        copies[1].wait()
        lane = lax.broadcasted_iota(jnp.int32, (8, EXTRA), 1)
        for k, at in enumerate(starts):
            row = at + lax.broadcasted_iota(jnp.int32, (8, rows), 0)
            mine = row == lax.broadcasted_iota(jnp.int32, (8, rows), 1)
            one = jnp.sum(jnp.where(mine, ints[0:1], 0), axis=1, keepdims=True)
            extra = jnp.where(
                lane == 0, jnp.sum(jnp.where(mine, ints[8:9], 0), axis=1, keepdims=True), 0
            )
            for d in range(3):
                digit = (one >> (DIGIT_BITS * d)) & (DIGITS - 1)
                extra = jnp.where(lane == d + 1, digit, extra)
            out_ref[8 * k : 8 * k + 8, width:] = extra.astype(jnp.float32).astype(jnp.bfloat16)
        for copy in copies[2:]:
            copy.wait()

    return call(
        kernel,
        (core[None], far(hidden), far(ids[None]), far(mask[None])),
        [((rows // 2, width + EXTRA), jnp.bfloat16)],
        in_specs=[SMEM, ANY, ANY, ANY],
        scratch=[pltpu.VMEM((16, rows), jnp.int32), pltpu.SemaphoreType.DMA((2 + rows // 16,))],
        mib=2,
    )[0]


def joined(*groups, after=()):
    sizes = [len(g) for g in groups]
    pieces = [p for g in groups for p in g]

    def kernel(*refs):
        ins, outs = list(refs[: len(pieces)]), refs[len(refs) - len(groups) :]
        for out_ref, size in zip(outs, sizes):
            at = 0
            for _ in range(size):
                ref = ins.pop(0)
                out_ref[at : at + ref.shape[0]] = ref[...]
                at += ref.shape[0]

    outs = [((sum(p.shape[0] for p in g), g[0].shape[1]), g[0].dtype) for g in groups]
    return call(kernel, [*pieces, *after], outs, mib=4)


def turned(a, b, width):
    rows = a.shape[0]
    cuts = 7

    def kernel(a_ref, b_ref, out_ref):
        for k in range(cuts):
            at = slice(k * width // cuts, (k + 1) * width // cuts)
            out_ref[at, :rows] = a_ref[:, at].T
            out_ref[at, rows:] = b_ref[:, at].T

    return call(kernel, [a, b], [((width, 2 * rows), a.dtype)], flops=10**9)[0]


def added(groups, blocks):
    sizes = [len(g) for g in groups]
    parts = [p for g in groups for p in g]

    def kernel(*refs):
        ins, outs = list(refs[: len(parts)]), list(refs[len(parts) :])
        for size in sizes:
            terms = [ins.pop(0) for _ in range(size)]
            cut = terms[0].shape[0] // blocks
            for k in range(blocks):
                at = slice(k * cut, (k + 1) * cut)
                total = sum(t[at].astype(jnp.float32) for t in terms[1:])
                outs.pop(0)[...] = (total + terms[0][at].astype(jnp.float32)).astype(jnp.bfloat16)

    outs = [
        ((g[0].shape[0] // blocks, g[0].shape[1]), jnp.bfloat16) for g in groups for _ in range(blocks)
    ]
    return call(kernel, parts, outs, mib=4)


def added_by_place(groups, spot):
    sizes = [len(g) for g in groups]
    parts = [p for g in groups for p in g]
    rows, width = parts[0].shape

    def kernel(spot_ref, *refs):
        ins, outs, sums = list(refs[: len(parts)]), refs[len(parts) : -1], refs[-1]
        for k, size in enumerate(sizes):
            terms = [ins.pop(0) for _ in range(size)]
            sums[k * rows : (k + 1) * rows] = sum(t[...].astype(jnp.float32) for t in terms)
        for k, out_ref in enumerate(outs):
            step = 0 if k == 0 else jnp.where(spot_ref[0] == 0, XORS[0][k - 1], XORS[1][k - 1])
            y = (spot_ref[2] * 2 + spot_ref[1]) ^ step
            at = pl.multiple_of(((y & 1) * 2 + (y >> 1)) * 8, 8)
            out_ref[...] = sums[pl.ds(at, 8), :].astype(jnp.bfloat16)

    blocks = len(groups) * rows // 8
    return call(
        kernel,
        [spot, *parts],
        [((8, width), jnp.bfloat16)] * blocks,
        in_specs=[SMEM] + [VMEM] * len(parts),
        scratch=[pltpu.VMEM((len(groups) * rows, width), jnp.float32)],
        mib=4,
    )


def combined(parts, spot=None):
    shape = parts[0].shape
    n = len(parts)

    def kernel(*refs):
        ins, outs = refs[:n], refs[n:]
        smax = functools.reduce(jnp.maximum, [r[0:1] for r in ins])
        tmax = functools.reduce(jnp.maximum, [r[3:4] for r in ins])
        stot = cross = ttot = pick = 0.0
        for r in ins:
            factor = jnp.exp(r[0:1] - smax)
            stot, cross = stot + r[1:2] * factor, cross + r[2:3] * factor
            ttot = ttot + r[4:5] * jnp.exp(r[3:4] - tmax)
            pick = pick + r[5:6]
        mask = ins[0][6:7]
        rows = [smax, stot, cross, tmax, ttot, pick, mask, mask]
        if spot is not None:
            spot_ref, *outs = outs
            student_shift, teacher_shift = smax + jnp.log(stot), tmax + jnp.log(ttot)
            apart = student_shift - teacher_shift
            row_kl = cross / stot - apart
            rows = [student_shift, apart + row_kl] + [mask] * 6
            lane = lax.broadcasted_iota(jnp.int32, (8, 128), 1)
            total = jnp.sum(mask * row_kl, axis=1, keepdims=True)
            count = jnp.sum(mask, axis=1, keepdims=True)
            outs[1][...] = jnp.where(lane == 0, total, count)
            row = (spot_ref[3] >> 1) * 8 + lax.broadcasted_iota(jnp.int32, (8, shape[1]), 0)
            mine = row == lax.broadcasted_iota(jnp.int32, (8, shape[1]), 1)
            ratio = jnp.sum(jnp.where(mine, pick - apart, 0.0), axis=1, keepdims=True)
            here = lane == lax.broadcasted_iota(jnp.int32, (8, 128), 0)
            ratio = jnp.sum(jnp.where(here, ratio, 0.0), axis=0, keepdims=True)
            outs[2][...] = jnp.broadcast_to(ratio, (8, 128))
        for k, row in enumerate(rows):
            outs[0][k : k + 1] = row

    out = (shape, jnp.float32)
    if spot is None:
        return call(kernel, parts, [out], mib=2)[0]
    outs = [out, ((8, 128), jnp.float32), ((8, 128), jnp.float32)]
    return call(kernel, [*parts, spot], outs, in_specs=[VMEM] * n + [SMEM], mib=2)


def side_by_side(head, head_in):
    width, columns = head.shape
    cuts = 4

    def kernel(h_ref, g_ref, out_ref, mark_ref, sems):
        mark_ref[...] = jnp.zeros(mark_ref.shape, jnp.float32)
        copies = []
        for k in range(cuts):
            at = pl.ds(k * width // cuts, width // cuts)
            for ref, column in ((h_ref, 0), (g_ref, columns)):
                copies.append(
                    pltpu.make_async_copy(
                        ref.at[at], out_ref.at[at, pl.ds(column, columns)], sems.at[len(copies)]
                    )
                )
        for copy in copies:
            copy.start()
        for copy in copies:
            copy.wait()

    return call(
        kernel,
        (far(head), far(head_in)),
        [((width, 2 * columns), head.dtype), ((8, 128), jnp.float32)],
        in_specs=[ANY, ANY],
        scratch=[pltpu.SemaphoreType.DMA((2 * cuts,))],
        flops=4 * 10**9,
        mib=2,
    )


def logits_and_stats(spot, a, b, heads, teacher, teacher_in, places, which, before=None):
    f32 = jnp.float32
    width, both = heads.shape
    columns = both // 2
    part, rows, tokens = a.shape[0], 2 * a.shape[0], places.shape[0]
    chunk = 32

    def kernel(spot_ref, a_ref, b_ref, h_ref, t_ref, u_ref, p_ref, *rest):
        out_ref, stats_ref, states, placed = rest[-4:]
        states[:part] = a_ref[:, :width]
        states[part:] = b_ref[:, :width]
        out_ref[...] = jnp.dot(states[...], h_ref[...], preferred_element_type=f32)
        lanes = lax.broadcasted_iota(jnp.int32, (1, both), 1)
        base, other_base = spot_ref[3] * columns, (spot_ref[3] ^ 1) * columns
        column = jnp.where(lanes < columns, base + lanes, other_base + lanes - columns)
        spots = lax.broadcasted_iota(jnp.int32, (1, tokens), 1)
        placed[...] = jnp.zeros(placed.shape, f32)
        for k in range(rows // chunk):
            ref, at = (a_ref, k * chunk) if k * chunk < part else (b_ref, k * chunk - part)
            here = slice(k * chunk, (k + 1) * chunk)
            there = slice(which * rows + k * chunk, which * rows + (k + 1) * chunk)
            student, note = out_ref[here, :], ref[at : at + chunk, width:].astype(f32)
            teacher = jnp.concatenate([t_ref[there, :], u_ref[there, :]], axis=1).astype(f32)
            ids = note[:, 1:2] + DIGITS * note[:, 2:3] + DIGITS**2 * note[:, 3:4]
            chosen = ids.astype(jnp.int32) == column
            smax = jnp.max(student, axis=1, keepdims=True)
            tmax = jnp.max(teacher, axis=1, keepdims=True)
            shifted = jnp.exp(student - smax)
            differ = student - teacher
            sums = [
                smax,
                jnp.sum(shifted, axis=1, keepdims=True),
                jnp.sum(shifted * differ, axis=1, keepdims=True),
                tmax,
                jnp.sum(jnp.exp(teacher - tmax), axis=1, keepdims=True),
                jnp.sum(jnp.where(chosen, differ, 0.0), axis=1, keepdims=True),
                note[:, :1],
            ]
            mine = p_ref[there, :] == spots
            for r, value in enumerate(sums):
                found = jnp.where(mine, value, 0.0).reshape(chunk // 8, 8, tokens)
                placed[r] += jnp.sum(found, axis=0)
        for r in range(8):
            row = jnp.sum(placed[r], axis=0, keepdims=True)
            stats_ref[r : r + 1] = row if before is None else row + rest[0][r : r + 1]

    operands = [spot, a, b, heads, teacher, teacher_in, places]
    if before is not None:
        operands.append(before)
    return call(
        kernel,
        operands,
        [((rows, both), f32), ((8, tokens), f32)],
        in_specs=[SMEM] + [VMEM] * (len(operands) - 1),
        scratch=[pltpu.VMEM((rows, width), jnp.bfloat16), pltpu.VMEM((8, 8, tokens), f32)],
        flops=2 * rows * width * both,
    )


def gradients(student, shifts, heads, teacher, teacher_in, places, which):
    f32, bf16 = jnp.float32, jnp.bfloat16
    width, both = heads.shape
    columns = both // 2
    rows, tokens = student.shape[0], places.shape[0]
    part = rows // 2
    chunk, cuts = 32, 7

    def kernel(s_ref, c_ref, h_ref, t_ref, u_ref, p_ref, a_ref, b_ref, d_ref, e_ref, all_d):
        spots = lax.broadcasted_iota(jnp.int32, (1, tokens), 1)
        for k in range(rows // chunk):
            here = slice(k * chunk, (k + 1) * chunk)
            there = slice(which * rows + k * chunk, which * rows + (k + 1) * chunk)
            mine = p_ref[there, :] == spots

            def of_row(r):
                return jnp.sum(jnp.where(mine, c_ref[r : r + 1], 0.0), axis=1, keepdims=True)

            student = s_ref[here, :]
            teacher = jnp.concatenate([t_ref[there, :], u_ref[there, :]], axis=1).astype(f32)
            probs = of_row(2) * jnp.exp(student - of_row(0))
            found = (probs * (student - teacher - of_row(1))).astype(bf16)
            all_d[here, :] = found
            d_ref[here, :] = found[:, :columns]
            e_ref[here, :] = found[:, columns:]
        for k in range(cuts):
            at = slice(k * width // cuts, (k + 1) * width // cuts)
            product = lax.dot_general(
                all_d[...], h_ref[at, :], (((1,), (1,)), ((), ())), preferred_element_type=f32
            ).astype(bf16)
            a_ref[:, at] = product[:part]
            b_ref[:, at] = product[part:]

    return call(
        kernel,
        [student, shifts, heads, teacher, teacher_in, places],
        [((part, width), bf16)] * 2 + [((rows, columns), bf16)] * 2,
        scratch=[pltpu.VMEM((rows, both), bf16)],
        flops=2 * rows * width * both,
    )


def head_gradient(states, dlogits):
    bf16 = jnp.bfloat16
    width, columns = states[0].shape[0], dlogits[0].shape[1]
    block = 512
    tokens = sum(d.shape[0] for d in dlogits)
    n = len(states)

    def kernel(*refs):
        pieces, others = refs[:n], refs[n:-4]
        out_ref, right, found, sems = refs[-4:]
        at = 0
        for ref in others:
            right[at : at + ref.shape[0]] = ref[...]
            at += ref.shape[0]
        copies = []
        for k in range(width // block):
            left = jnp.concatenate([r[k * block : (k + 1) * block, :] for r in pieces], axis=1)
            product = jnp.dot(left, right[...], preferred_element_type=jnp.float32).astype(bf16)
            slot = k % 2
            if k >= 2:
                copies[k - 2].wait()
            found[slot] = product
            copies.append(
                pltpu.make_async_copy(
                    found.at[slot], out_ref.at[pl.ds(k * block, block)], sems.at[slot]
                )
            )
            copies[k].start()
        copies[-2].wait()
        copies[-1].wait()

    return call(
        kernel,
        [*states, *dlogits],
        [((width, columns), bf16)],
        out_specs=[ANY],
        scratch=[
            pltpu.VMEM((tokens, columns), bf16),
            pltpu.VMEM((2, block, columns), bf16),
            pltpu.SemaphoreType.DMA((2,)),
        ],
        flops=2 * tokens * width * columns,
    )[0]


def per_device(hidden, teacher_logits, sampled_ids, loss_mask, student_head):
    f32, bf16 = jnp.float32, jnp.bfloat16
    core, y_low = lax.axis_index(CORE), lax.axis_index("tok_0")
    z, x = lax.axis_index("tok_1"), lax.axis_index("tok_2")
    position = lax.axis_index(TOK_VOC)
    width, columns = student_head.shape
    tokens = teacher_logits.shape[0]
    rows = tokens // 2

    block = entry_block(core, hidden, sampled_ids, loss_mask)
    head_in = swap_core(student_head)
    token = token_of_rows(core, z, x, rows)
    token_other = token_of_rows(1 - core, z, x, rows)
    places = (token // 16) * 8 + token % 8
    spot = jnp.stack([core, y_low, lax.axis_index("voc_0"), position])
    other = swap(block, "y", 0)
    teacher_send = jnp.dot(one_hot(token_other, tokens, bf16), teacher_logits)
    other, teacher_send, spot, places = together(other, teacher_send, spot, places)
    teacher_in = swap_core(teacher_send)
    near_a = jnp.where(y_low == 0, block, other)
    near_b = jnp.where(y_low == 0, other, block)

    far_a, far_b = together(swap(near_a, "x", 0), swap(near_b, "z", 0))
    near_a, near_b = joined((near_a, far_a), (near_b, far_b))
    far_a, far_b = swap(near_a, "x", 1), swap(near_b, "z", 1)
    teacher = jnp.dot(one_hot(token, tokens, bf16), teacher_logits)
    far_a, far_b, teacher = together(far_a, far_b, teacher)
    near_a, near_b = joined((near_a, far_a), (near_b, far_b))

    far_a, far_b = swap(near_a, "z", 0), swap(near_b, "x", 0)
    heads, mark = side_by_side(student_head, head_in)
    near_a, near_b = joined((near_a, far_a), (near_b, far_b), after=(mark,))

    far_a, far_b = swap(near_a, "z", 1), swap(near_b, "x", 1)
    shared = (heads, teacher, teacher_in, places)
    near_other = swap_core(near_a), swap_core(near_b)
    student_near, stats = logits_and_stats(spot, near_a, near_b, *shared, 0)
    states = [turned(near_a, near_b, width)]
    far_a, far_b, student_near, stats, states[0] = together(
        far_a, far_b, student_near, stats, states[0]
    )
    student_far, stats = logits_and_stats(spot, far_a, far_b, *shared, 1, stats)
    far_other = swap_core(far_a), swap_core(far_b)
    for ring, pair in (("x", (far_a, far_b)), ("z", near_other), ("y", far_other)):
        parts = [stats, *(swap(stats, ring, step) for step in range(3))]
        *parts, state = together(*parts, turned(*pair, width))
        states.append(state)
        stats = combined(parts, spot if ring == "y" else None)
    stats, sums, ratios = stats
    sampled_ratio = ratios[0, :8]

    far_sum_a, far_sum_b, *far_d = gradients(student_far, stats, *shared, 1)
    far_sum_a, far_sum_b, stats_later = together(far_sum_a, far_sum_b, stats)
    a_in, b_in = swap(far_sum_a, "z", 1), swap(far_sum_b, "x", 1)
    far_d_in = swap_core(far_d[1])
    near_sum_a, near_sum_b, *near_d = gradients(student_near, stats_later, *shared, 0)
    near_d_in = swap_core(near_d[1])
    head_grad = head_gradient(states, (near_d[0], far_d[0], near_d_in, far_d_in))
    a_in, b_in, near_sum_a, near_sum_b, head_grad = together(
        a_in, b_in, near_sum_a, near_sum_b, head_grad
    )
    keep_a, send_a, keep_b, send_b = added(((near_sum_a, a_in), (near_sum_b, b_in)), 2)
    a_in, b_in = swap(send_a, "z", 0), swap(send_b, "x", 0)
    sums = sums + swap_core(sums)
    loss = sums[0, 0] / sums[0, 1]
    a_in, b_in, loss, sampled_ratio = together(a_in, b_in, loss, sampled_ratio)
    keep_a, send_a, keep_b, send_b = added(((keep_a, a_in), (keep_b, b_in)), 2)
    a_in, b_in = together(swap(send_a, "x", 1), swap(send_b, "z", 1))
    keep_a, send_a, keep_b, send_b = added(((keep_a, a_in), (keep_b, b_in)), 2)
    a_in, b_in = together(swap(send_a, "x", 0), swap(send_b, "z", 0))
    keep, *send = added_by_place(((keep_a, a_in), (keep_b, b_in)), spot)
    arrived = [swap(part, "y", step) for step, part in enumerate(send)]
    hidden_grad = sum((p.astype(f32) for p in arrived), keep.astype(f32)).astype(bf16)
    return (loss, sampled_ratio, hidden_grad, head_grad)


def solution(mesh):
    split = Mesh(mesh.devices.reshape(2, 4, 4, 2, 2), TOK_VOC)
    in_specs = (P(TOK, None), P(None, TOK_VOC), P(TOK), P(TOK), P(None, TOK_VOC))
    out_specs = (P(), P(TOK_VOC), P(TOK_VOC, None), P(None, TOK_VOC))
    return jax.shard_map(
        per_device, mesh=split, in_specs=in_specs, out_specs=out_specs, check_vma=False
    )
```

```python
import functools
import itertools

import jax
import jax.numpy as jnp
from jax import lax
from jax.experimental import pallas as pl
from jax.experimental.pallas import tpu as pltpu
from jax.sharding import Mesh
from jax.sharding import PartitionSpec as P

TOK = ("tok_0", "tok_1", "tok_2")
TOK_VOC = ("tok_0", "tok_1", "tok_2", "voc_0", "voc_1")
CORE = "voc_1"
DIGIT_BITS = 6
DIGITS = 1 << DIGIT_BITS
EXTRA = 128
INTERPRET = False
XORS = ((1, 3, 2), (3, 1, 2))


def group_of(core, y, z, x):
    return core ^ ((x ^ y ^ z) & 1)


def moved(value, target):
    pairs = []
    for y, z, x, c in itertools.product(range(4), range(4), range(4), range(2)):
        pairs.append(
            tuple(
                ((((v % 2) * 4 + w) * 4 + u) * 2 + v // 2) * 2 + d
                for v, w, u, d in ((y, z, x, c), target(y, z, x, c))
            )
        )
    return lax.ppermute(value, TOK_VOC, pairs)


def swap(value, ring, step):
    def target(y, z, x, c):
        group = group_of(c, y, z, x)
        xor = XORS[group][step]
        at = {"y": y, "z": z, "x": x}
        at[ring] ^= xor
        return at["y"], at["z"], at["x"], group_of(group, at["y"], at["z"], at["x"])

    return moved(value, target)


def to_owner(value, step=None):
    def target(y, z, x, c):
        group = group_of(c, y, z, x)
        return y if step is None else y ^ XORS[group][step], z, x, group

    return moved(value, target)


def swap_core(value):
    return lax.ppermute(value, CORE, [(0, 1), (1, 0)])


def together(*values):
    return lax.optimization_barrier(values)


def token_of_rows(group, z, x, rows):
    n = lax.broadcasted_iota(jnp.int32, (rows, 1), 0)
    quarter = rows // 8
    half, part, top = n // (4 * quarter), (n // (2 * quarter)) % 2, (n // quarter) % 2
    high = half * 2 + top
    low = (n // (quarter // 4)) % 4
    mid = (n // 8) % 2
    first = jnp.where(group == 0, XORS[0][0], XORS[1][0])
    second = jnp.where(group == 0, XORS[0][1], XORS[1][1])

    def place(own, k):
        return own ^ ((k % 2) * first) ^ ((k // 2) * second)

    z_at = jnp.where(part == 0, place(z, high), place(z, low))
    x_at = jnp.where(part == 0, place(x, low), place(x, high))
    return ((((part * 4 + z_at) * 4 + x_at) * 2 + mid) * 2 + group) * 8 + n % 8


def one_hot(rows, columns, dtype):
    return (rows == lax.broadcasted_iota(jnp.int32, (1, columns), 1)).astype(dtype)


VMEM = pl.BlockSpec(memory_space=pltpu.VMEM)
SMEM = pl.BlockSpec(memory_space=pltpu.SMEM)
ANY = pl.BlockSpec(memory_space=pl.ANY)


def near(value):
    return value if INTERPRET else pltpu.with_memory_space_constraint(value, pltpu.VMEM)


def far(value):
    return value if INTERPRET else pltpu.with_memory_space_constraint(value, pltpu.HBM)


def call(kernel, operands, outs, in_specs=None, out_specs=None, flops=10**6, scratch=(), mib=16, aliases={}):
    in_specs = in_specs or [VMEM] * len(operands)
    out_specs = out_specs or [VMEM] * len(outs)
    shapes = [
        pltpu.VMEM(shape, dtype)
        if spec is VMEM and not INTERPRET
        else jax.ShapeDtypeStruct(shape, dtype)
        for (shape, dtype), spec in zip(outs, out_specs)
    ]
    operands = [near(v) if spec is VMEM else v for v, spec in zip(operands, in_specs)]
    return pl.pallas_call(
        kernel,
        out_shape=shapes,
        in_specs=in_specs,
        out_specs=out_specs,
        scratch_shapes=scratch,
        input_output_aliases=aliases,
        compiler_params=pltpu.CompilerParams(vmem_limit_bytes=mib << 20),
        cost_estimate=pl.CostEstimate(flops=flops, bytes_accessed=10**6, transcendentals=0),
        interpret=INTERPRET,
    )(*operands)


def entry_block(group, hidden, ids, mask):
    rows, width = hidden.shape

    def kernel(group_ref, hidden_ref, ids_ref, mask_ref, out_ref, ints, sems):
        starts = [8 * (2 * k + group_ref[0]) for k in range(rows // 16)]
        copies = [
            pltpu.make_async_copy(ids_ref, ints.at[pl.ds(0, 1)], sems.at[0]),
            pltpu.make_async_copy(mask_ref, ints.at[pl.ds(8, 1)], sems.at[1]),
        ]
        for k, at in enumerate(starts):
            copies.append(
                pltpu.make_async_copy(
                    hidden_ref.at[pl.ds(pl.multiple_of(at, 8), 8)],
                    out_ref.at[pl.ds(8 * k, 8), pl.ds(0, width)],
                    sems.at[2 + k],
                )
            )
        for copy in copies:
            copy.start()
        copies[0].wait()
        copies[1].wait()
        lane = lax.broadcasted_iota(jnp.int32, (8, EXTRA), 1)
        for k, at in enumerate(starts):
            row = at + lax.broadcasted_iota(jnp.int32, (8, rows), 0)
            mine = row == lax.broadcasted_iota(jnp.int32, (8, rows), 1)
            one = jnp.sum(jnp.where(mine, ints[0:1], 0), axis=1, keepdims=True)
            extra = jnp.where(
                lane == 0, jnp.sum(jnp.where(mine, ints[8:9], 0), axis=1, keepdims=True), 0
            )
            for d in range(3):
                digit = (one >> (DIGIT_BITS * d)) & (DIGITS - 1)
                extra = jnp.where(lane == d + 1, digit, extra)
            out_ref[8 * k : 8 * k + 8, width:] = extra.astype(jnp.float32).astype(jnp.bfloat16)
        for copy in copies[2:]:
            copy.wait()

    return call(
        kernel,
        (group[None], far(hidden), far(ids[None]), far(mask[None])),
        [((rows // 2, width + EXTRA), jnp.bfloat16)],
        in_specs=[SMEM, ANY, ANY, ANY],
        scratch=[pltpu.VMEM((16, rows), jnp.int32), pltpu.SemaphoreType.DMA((2 + rows // 16,))],
        mib=2,
    )[0]


def joined(*groups, after=()):
    sizes = [len(g) for g in groups]
    pieces = [p for g in groups for p in g]

    def kernel(*refs):
        ins, outs = list(refs[: len(pieces)]), refs[len(refs) - len(groups) :]
        for out_ref, size in zip(outs, sizes):
            at = 0
            for _ in range(size):
                ref = ins.pop(0)
                out_ref[at : at + ref.shape[0]] = ref[...]
                at += ref.shape[0]

    outs = [((sum(p.shape[0] for p in g), g[0].shape[1]), g[0].dtype) for g in groups]
    return call(kernel, [*pieces, *after], outs, mib=4)


def turned(a, b, width):
    rows = a.shape[0]
    cuts = 7

    def kernel(a_ref, b_ref, out_ref):
        for k in range(cuts):
            at = slice(k * width // cuts, (k + 1) * width // cuts)
            out_ref[at, :rows] = a_ref[:, at].T
            out_ref[at, rows:] = b_ref[:, at].T

    return call(kernel, [a, b], [((width, 2 * rows), a.dtype)], flops=10**9)[0]


def added(groups, blocks):
    sizes = [len(g) for g in groups]
    parts = [p for g in groups for p in g]

    def kernel(*refs):
        ins, outs = list(refs[: len(parts)]), list(refs[len(parts) :])
        for size in sizes:
            terms = [ins.pop(0) for _ in range(size)]
            cut = terms[0].shape[0] // blocks
            for k in range(blocks):
                at = slice(k * cut, (k + 1) * cut)
                total = sum(t[at].astype(jnp.float32) for t in terms[1:])
                outs.pop(0)[...] = (total + terms[0][at].astype(jnp.float32)).astype(jnp.bfloat16)

    outs = [
        ((g[0].shape[0] // blocks, g[0].shape[1]), jnp.bfloat16) for g in groups for _ in range(blocks)
    ]
    return call(kernel, parts, outs, mib=4)


def added_by_place(groups, spot):
    sizes = [len(g) for g in groups]
    parts = [p for g in groups for p in g]
    rows, width = parts[0].shape

    def kernel(spot_ref, *refs):
        ins, outs, sums = list(refs[: len(parts)]), refs[len(parts) : -1], refs[-1]
        for k, size in enumerate(sizes):
            terms = [ins.pop(0) for _ in range(size)]
            sums[k * rows : (k + 1) * rows] = sum(t[...].astype(jnp.float32) for t in terms)
        for k, out_ref in enumerate(outs):
            step = 0 if k == 0 else jnp.where(spot_ref[0] == 0, XORS[0][k - 1], XORS[1][k - 1])
            y = (spot_ref[2] * 2 + spot_ref[1]) ^ step
            at = pl.multiple_of(((y & 1) * 2 + (y >> 1)) * 8, 8)
            out_ref[...] = sums[pl.ds(at, 8), :].astype(jnp.bfloat16)

    blocks = len(groups) * rows // 8
    return call(
        kernel,
        [spot, *parts],
        [((8, width), jnp.bfloat16)] * blocks,
        in_specs=[SMEM] + [VMEM] * len(parts),
        scratch=[pltpu.VMEM((len(groups) * rows, width), jnp.float32)],
        mib=4,
    )


def combined(parts, spot=None):
    shape = parts[0].shape
    n = len(parts)

    def kernel(*refs):
        ins, outs = refs[:n], refs[n:]
        smax = functools.reduce(jnp.maximum, [r[0:1] for r in ins])
        tmax = functools.reduce(jnp.maximum, [r[3:4] for r in ins])
        stot = cross = ttot = pick = 0.0
        for r in ins:
            factor = jnp.exp(r[0:1] - smax)
            stot, cross = stot + r[1:2] * factor, cross + r[2:3] * factor
            ttot = ttot + r[4:5] * jnp.exp(r[3:4] - tmax)
            pick = pick + r[5:6]
        mask = ins[0][6:7]
        rows = [smax, stot, cross, tmax, ttot, pick, mask, mask]
        if spot is not None:
            spot_ref, *outs = outs
            student_shift, teacher_shift = smax + jnp.log(stot), tmax + jnp.log(ttot)
            apart = student_shift - teacher_shift
            row_kl = cross / stot - apart
            rows = [student_shift, apart + row_kl] + [mask] * 6
            lane = lax.broadcasted_iota(jnp.int32, (8, 128), 1)
            total = jnp.sum(mask * row_kl, axis=1, keepdims=True)
            count = jnp.sum(mask, axis=1, keepdims=True)
            row = (spot_ref[3] >> 1) * 8 + lax.broadcasted_iota(jnp.int32, (8, shape[1]), 0)
            mine = row == lax.broadcasted_iota(jnp.int32, (8, shape[1]), 1)
            ratio = jnp.sum(jnp.where(mine, pick - apart, 0.0), axis=1, keepdims=True)
            here = lane == lax.broadcasted_iota(jnp.int32, (8, 128), 0)
            ratio = jnp.sum(jnp.where(here, ratio, 0.0), axis=0, keepdims=True)
            line = lax.broadcasted_iota(jnp.int32, (8, 128), 0)
            outs[1][...] = jnp.where(line == 0, total, jnp.where(line == 1, count, ratio))
        for k, row in enumerate(rows):
            outs[0][k : k + 1] = row

    out = (shape, jnp.float32)
    if spot is None:
        return call(kernel, parts, [out], mib=2)[0]
    outs = [out, ((8, 128), jnp.float32)]
    return call(kernel, [*parts, spot], outs, in_specs=[VMEM] * n + [SMEM], mib=2)


def side_by_side(head, head_in):
    width, columns = head.shape
    cuts = 4

    def kernel(h_ref, g_ref, out_ref, mark_ref, sems):
        mark_ref[...] = jnp.zeros(mark_ref.shape, jnp.float32)
        copies = []
        for k in range(cuts):
            at = pl.ds(k * width // cuts, width // cuts)
            for ref, column in ((h_ref, 0), (g_ref, columns)):
                copies.append(
                    pltpu.make_async_copy(
                        ref.at[at], out_ref.at[at, pl.ds(column, columns)], sems.at[len(copies)]
                    )
                )
        for copy in copies:
            copy.start()
        for copy in copies:
            copy.wait()

    return call(
        kernel,
        (far(head), far(head_in)),
        [((width, 2 * columns), head.dtype), ((8, 128), jnp.float32)],
        in_specs=[ANY, ANY],
        scratch=[pltpu.SemaphoreType.DMA((2 * cuts,))],
        flops=4 * 10**9,
        mib=2,
    )


def logits_and_stats(spot, a, b, heads, teacher, teacher_in, places, which, before=None):
    f32 = jnp.float32
    width, both = heads.shape
    columns = both // 2
    part, rows, tokens = a.shape[0], 2 * a.shape[0], places.shape[0]
    chunk = 32

    def kernel(spot_ref, a_ref, b_ref, h_ref, t_ref, u_ref, p_ref, *rest):
        out_ref, stats_ref, states, placed = rest[-4:]
        states[:part] = a_ref[:, :width]
        states[part:] = b_ref[:, :width]
        out_ref[...] = jnp.dot(states[...], h_ref[...], preferred_element_type=f32)
        lanes = lax.broadcasted_iota(jnp.int32, (1, both), 1)
        base, other_base = spot_ref[3] * columns, (spot_ref[3] ^ 1) * columns
        column = jnp.where(lanes < columns, base + lanes, other_base + lanes - columns)
        spots = lax.broadcasted_iota(jnp.int32, (1, tokens), 1)
        placed[...] = jnp.zeros(placed.shape, f32)
        for k in range(rows // chunk):
            ref, at = (a_ref, k * chunk) if k * chunk < part else (b_ref, k * chunk - part)
            here = slice(k * chunk, (k + 1) * chunk)
            there = slice(which * rows + k * chunk, which * rows + (k + 1) * chunk)
            student, note = out_ref[here, :], ref[at : at + chunk, width:].astype(f32)
            teacher = jnp.concatenate([t_ref[there, :], u_ref[there, :]], axis=1).astype(f32)
            ids = note[:, 1:2] + DIGITS * note[:, 2:3] + DIGITS**2 * note[:, 3:4]
            chosen = ids.astype(jnp.int32) == column
            smax = jnp.max(student, axis=1, keepdims=True)
            tmax = jnp.max(teacher, axis=1, keepdims=True)
            shifted = jnp.exp(student - smax)
            differ = student - teacher
            sums = [
                smax,
                jnp.sum(shifted, axis=1, keepdims=True),
                jnp.sum(shifted * differ, axis=1, keepdims=True),
                tmax,
                jnp.sum(jnp.exp(teacher - tmax), axis=1, keepdims=True),
                jnp.sum(jnp.where(chosen, differ, 0.0), axis=1, keepdims=True),
                note[:, :1],
            ]
            mine = p_ref[there, :] == spots
            for r, value in enumerate(sums):
                found = jnp.where(mine, value, 0.0).reshape(chunk // 8, 8, tokens)
                placed[r] += jnp.sum(found, axis=0)
        for r in range(8):
            row = jnp.sum(placed[r], axis=0, keepdims=True)
            stats_ref[r : r + 1] = row if before is None else row + rest[0][r : r + 1]

    operands = [spot, a, b, heads, teacher, teacher_in, places]
    if before is not None:
        operands.append(before)
    return call(
        kernel,
        operands,
        [((rows, both), f32), ((8, tokens), f32)],
        in_specs=[SMEM] + [VMEM] * (len(operands) - 1),
        scratch=[pltpu.VMEM((rows, width), jnp.bfloat16), pltpu.VMEM((8, 8, tokens), f32)],
        flops=2 * rows * width * both,
    )


def gradients(student, shifts, heads, teacher, teacher_in, places, which):
    f32, bf16 = jnp.float32, jnp.bfloat16
    width, both = heads.shape
    columns = both // 2
    rows, tokens = student.shape[0], places.shape[0]
    part = rows // 2
    chunk, cuts = 32, 7

    def kernel(s_ref, c_ref, h_ref, t_ref, u_ref, p_ref, a_ref, b_ref, d_ref, e_ref, all_d):
        spots = lax.broadcasted_iota(jnp.int32, (1, tokens), 1)
        for k in range(rows // chunk):
            here = slice(k * chunk, (k + 1) * chunk)
            there = slice(which * rows + k * chunk, which * rows + (k + 1) * chunk)
            mine = p_ref[there, :] == spots

            def of_row(r):
                return jnp.sum(jnp.where(mine, c_ref[r : r + 1], 0.0), axis=1, keepdims=True)

            student = s_ref[here, :]
            teacher = jnp.concatenate([t_ref[there, :], u_ref[there, :]], axis=1).astype(f32)
            probs = of_row(2) * jnp.exp(student - of_row(0))
            found = (probs * (student - teacher - of_row(1))).astype(bf16)
            all_d[here, :] = found
            d_ref[here, :] = found[:, :columns]
            e_ref[here, :] = found[:, columns:]
        for k in range(cuts):
            at = slice(k * width // cuts, (k + 1) * width // cuts)
            product = lax.dot_general(
                all_d[...], h_ref[at, :], (((1,), (1,)), ((), ())), preferred_element_type=f32
            ).astype(bf16)
            a_ref[:, at] = product[:part]
            b_ref[:, at] = product[part:]

    return call(
        kernel,
        [student, shifts, heads, teacher, teacher_in, places],
        [((part, width), bf16)] * 2 + [((rows, columns), bf16)] * 2,
        scratch=[pltpu.VMEM((rows, both), bf16)],
        flops=2 * rows * width * both,
    )


def head_gradient(states, dlogits, blocks, before=None):
    bf16 = jnp.bfloat16
    width, columns = states[0].shape[0], dlogits[0].shape[1]
    block = 512
    tokens = sum(d.shape[0] for d in dlogits)
    n, m = len(states), len(states) + len(dlogits)

    def kernel(*refs):
        pieces, others = refs[:n], refs[n:m]
        out_ref, right, found, sems = refs[-4:]
        at = 0
        for ref in others:
            right[at : at + ref.shape[0]] = ref[...]
            at += ref.shape[0]
        copies = []
        for j, k in enumerate(blocks):
            left = jnp.concatenate([r[k * block : (k + 1) * block, :] for r in pieces], axis=1)
            product = jnp.dot(left, right[...], preferred_element_type=jnp.float32).astype(bf16)
            slot = j % 2
            if j >= 2:
                copies[j - 2].wait()
            found[slot] = product
            copies.append(
                pltpu.make_async_copy(
                    found.at[slot], out_ref.at[pl.ds(k * block, block)], sems.at[slot]
                )
            )
            copies[j].start()
        copies[-2].wait()
        copies[-1].wait()

    operands, specs = [*states, *dlogits], [VMEM] * m
    if before is not None:
        operands, specs = [*operands, before], [*specs, ANY]
    return call(
        kernel,
        operands,
        [((width, columns), bf16)],
        in_specs=specs,
        out_specs=[ANY],
        scratch=[
            pltpu.VMEM((tokens, columns), bf16),
            pltpu.VMEM((2, block, columns), bf16),
            pltpu.SemaphoreType.DMA((2,)),
        ],
        flops=2 * tokens * len(blocks) * block * columns,
        aliases={} if before is None else {m: 0},
    )[0]


def per_device(hidden, teacher_logits, sampled_ids, loss_mask, student_head):
    f32, bf16 = jnp.float32, jnp.bfloat16
    core, y_low = lax.axis_index(CORE), lax.axis_index("tok_0")
    z, x = lax.axis_index("tok_1"), lax.axis_index("tok_2")
    position = lax.axis_index(TOK_VOC)
    group = group_of(core, y_low, z, x)
    width, columns = student_head.shape
    tokens = teacher_logits.shape[0]
    rows = tokens // 2

    block = entry_block(group, hidden, sampled_ids, loss_mask)
    head_in = swap_core(student_head)
    token = token_of_rows(group, z, x, rows)
    token_other = token_of_rows(1 - group, z, x, rows)
    places = (token // 16) * 8 + token % 8
    spot = jnp.stack([group, y_low, lax.axis_index("voc_0"), position])
    other = swap(block, "y", 0)
    teacher_send = jnp.dot(one_hot(token_other, tokens, bf16), teacher_logits)
    own_group = jnp.broadcast_to(group == core, (8,))
    other, teacher_send, spot, places, own_group = together(
        other, teacher_send, spot, places, own_group
    )
    teacher_in = swap_core(teacher_send)
    near_a = jnp.where(y_low == 0, block, other)
    near_b = jnp.where(y_low == 0, other, block)

    far_a, far_b = together(swap(near_a, "x", 0), swap(near_b, "z", 0))
    near_a, near_b = joined((near_a, far_a), (near_b, far_b))
    far_a, far_b = swap(near_a, "x", 1), swap(near_b, "z", 1)
    teacher = jnp.dot(one_hot(token, tokens, bf16), teacher_logits)
    far_a, far_b, teacher = together(far_a, far_b, teacher)
    near_a, near_b = joined((near_a, far_a), (near_b, far_b))

    far_a, far_b = swap(near_a, "z", 0), swap(near_b, "x", 0)
    heads, mark = side_by_side(student_head, head_in)
    near_a, near_b = joined((near_a, far_a), (near_b, far_b), after=(mark,))

    far_a, far_b = swap(near_a, "z", 1), swap(near_b, "x", 1)
    shared = (heads, teacher, teacher_in, places)
    near_other = swap_core(near_a), swap_core(near_b)
    student_near, stats = logits_and_stats(spot, near_a, near_b, *shared, 0)
    states = [turned(near_a, near_b, width)]
    far_a, far_b, student_near, stats, states[0] = together(
        far_a, far_b, student_near, stats, states[0]
    )
    student_far, stats = logits_and_stats(spot, far_a, far_b, *shared, 1, stats)
    far_other = swap_core(far_a), swap_core(far_b)
    for ring, pair in (("x", (far_a, far_b)), ("z", near_other), ("y", far_other)):
        parts = [stats, *(swap(stats, ring, step) for step in range(3))]
        *parts, state = together(*parts, turned(*pair, width))
        states.append(state)
        stats = combined(parts, spot if ring == "y" else None)
    stats, sums = stats

    far_sum_a, far_sum_b, *far_d = gradients(student_far, stats, *shared, 1)
    far_sum_a, far_sum_b, stats_later = together(far_sum_a, far_sum_b, stats)
    a_in, b_in = swap(far_sum_a, "z", 1), swap(far_sum_b, "x", 1)
    far_d_in = swap_core(far_d[1])
    near_sum_a, near_sum_b, *near_d = gradients(student_near, stats_later, *shared, 0)
    near_d_in = swap_core(near_d[1])
    all_d = (near_d[0], far_d[0], near_d_in, far_d_in)
    head_grad = head_gradient(states, all_d, range(4))
    a_in, b_in, near_sum_a, near_sum_b, head_grad = together(
        a_in, b_in, near_sum_a, near_sum_b, head_grad
    )
    keep_a, send_a, keep_b, send_b = added(((near_sum_a, a_in), (near_sum_b, b_in)), 2)
    a_in, b_in = swap(send_a, "z", 0), swap(send_b, "x", 0)
    other_sums = swap_core(sums)
    loss = (sums[0, 0] + other_sums[0, 0]) / (sums[1, 0] + other_sums[1, 0])
    sampled_ratio = jnp.where(own_group, sums[2, :8], other_sums[2, :8])
    head_grad = head_gradient(states, all_d, range(4, width // 512), head_grad)
    a_in, b_in, loss, sampled_ratio, head_grad = together(
        a_in, b_in, loss, sampled_ratio, head_grad
    )
    keep_a, send_a, keep_b, send_b = added(((keep_a, a_in), (keep_b, b_in)), 2)
    a_in, b_in = together(swap(send_a, "x", 1), swap(send_b, "z", 1))
    keep_a, send_a, keep_b, send_b = added(((keep_a, a_in), (keep_b, b_in)), 2)
    a_in, b_in = together(swap(send_a, "x", 0), swap(send_b, "z", 0))
    keep, *send = added_by_place(((keep_a, a_in), (keep_b, b_in)), spot)
    arrived = [to_owner(part, step) for step, part in enumerate(send)]
    parts = [to_owner(keep), *arrived]
    hidden_grad = sum(p.astype(f32) for p in parts).astype(bf16)
    return (loss, sampled_ratio, hidden_grad, head_grad)


def solution(mesh):
    split = Mesh(mesh.devices.reshape(2, 4, 4, 2, 2), TOK_VOC)
    in_specs = (P(TOK, None), P(None, TOK_VOC), P(TOK), P(TOK), P(None, TOK_VOC))
    out_specs = (P(), P(TOK_VOC), P(TOK_VOC, None), P(None, TOK_VOC))
    return jax.shard_map(
        per_device, mesh=split, in_specs=in_specs, out_specs=out_specs, check_vma=False
    )
```

```python
import functools
import itertools

import jax
import jax.numpy as jnp
from jax import lax
from jax.experimental import pallas as pl
from jax.experimental.pallas import tpu as pltpu
from jax.sharding import Mesh
from jax.sharding import PartitionSpec as P

TOK = ("tok_0", "tok_1", "tok_2")
TOK_VOC = ("tok_0", "tok_1", "tok_2", "voc_0", "voc_1")
CORE = "voc_1"
DIGIT_BITS = 6
DIGITS = 1 << DIGIT_BITS
EXTRA = 128
INTERPRET = False
XORS = ((1, 3, 2), (3, 1, 2))


def group_of(core, y, z, x):
    return core ^ ((x ^ y ^ z) & 1)


def moved(value, target):
    pairs = []
    for y, z, x, c in itertools.product(range(4), range(4), range(4), range(2)):
        pairs.append(
            tuple(
                ((((v % 2) * 4 + w) * 4 + u) * 2 + v // 2) * 2 + d
                for v, w, u, d in ((y, z, x, c), target(y, z, x, c))
            )
        )
    return lax.ppermute(value, TOK_VOC, pairs)


def swap(value, ring, step):
    def target(y, z, x, c):
        group = group_of(c, y, z, x)
        xor = XORS[group][step]
        at = {"y": y, "z": z, "x": x}
        at[ring] ^= xor
        return at["y"], at["z"], at["x"], group_of(group, at["y"], at["z"], at["x"])

    return moved(value, target)


def to_owner(value, step=None):
    def target(y, z, x, c):
        group = group_of(c, y, z, x)
        return y if step is None else y ^ XORS[group][step], z, x, group

    return moved(value, target)


def swap_core(value):
    return lax.ppermute(value, CORE, [(0, 1), (1, 0)])


def together(*values):
    return lax.optimization_barrier(values)


def token_of_rows(group, z, x, rows):
    n = lax.broadcasted_iota(jnp.int32, (rows, 1), 0)
    quarter = rows // 8
    half, part, top = n // (4 * quarter), (n // (2 * quarter)) % 2, (n // quarter) % 2
    high = half * 2 + top
    low = (n // (quarter // 4)) % 4
    mid = (n // 8) % 2
    first = jnp.where(group == 0, XORS[0][0], XORS[1][0])
    second = jnp.where(group == 0, XORS[0][1], XORS[1][1])

    def place(own, k):
        return own ^ ((k % 2) * first) ^ ((k // 2) * second)

    z_at = jnp.where(part == 0, place(z, high), place(z, low))
    x_at = jnp.where(part == 0, place(x, low), place(x, high))
    return ((((part * 4 + z_at) * 4 + x_at) * 2 + mid) * 2 + group) * 8 + n % 8


def one_hot(rows, columns, dtype):
    return (rows == lax.broadcasted_iota(jnp.int32, (1, columns), 1)).astype(dtype)


VMEM = pl.BlockSpec(memory_space=pltpu.VMEM)
SMEM = pl.BlockSpec(memory_space=pltpu.SMEM)
ANY = pl.BlockSpec(memory_space=pl.ANY)


def near(value):
    return value if INTERPRET else pltpu.with_memory_space_constraint(value, pltpu.VMEM)


def far(value):
    return value if INTERPRET else pltpu.with_memory_space_constraint(value, pltpu.HBM)


def call(kernel, operands, outs, in_specs=None, out_specs=None, flops=10**6, scratch=(), mib=16, aliases={}):
    in_specs = in_specs or [VMEM] * len(operands)
    out_specs = out_specs or [VMEM] * len(outs)
    shapes = [
        pltpu.VMEM(shape, dtype)
        if spec is VMEM and not INTERPRET
        else jax.ShapeDtypeStruct(shape, dtype)
        for (shape, dtype), spec in zip(outs, out_specs)
    ]
    operands = [near(v) if spec is VMEM else v for v, spec in zip(operands, in_specs)]
    return pl.pallas_call(
        kernel,
        out_shape=shapes,
        in_specs=in_specs,
        out_specs=out_specs,
        scratch_shapes=scratch,
        input_output_aliases=aliases,
        compiler_params=pltpu.CompilerParams(vmem_limit_bytes=mib << 20),
        cost_estimate=pl.CostEstimate(flops=flops, bytes_accessed=10**6, transcendentals=0),
        interpret=INTERPRET,
    )(*operands)


def entry_block(group, hidden, ids, mask):
    rows, width = hidden.shape

    def kernel(group_ref, hidden_ref, ids_ref, mask_ref, out_ref, ints, sems):
        starts = [8 * (2 * k + group_ref[0]) for k in range(rows // 16)]
        copies = [
            pltpu.make_async_copy(ids_ref, ints.at[pl.ds(0, 1)], sems.at[0]),
            pltpu.make_async_copy(mask_ref, ints.at[pl.ds(8, 1)], sems.at[1]),
        ]
        for k, at in enumerate(starts):
            copies.append(
                pltpu.make_async_copy(
                    hidden_ref.at[pl.ds(pl.multiple_of(at, 8), 8)],
                    out_ref.at[pl.ds(8 * k, 8), pl.ds(0, width)],
                    sems.at[2 + k],
                )
            )
        for copy in copies:
            copy.start()
        copies[0].wait()
        copies[1].wait()
        lane = lax.broadcasted_iota(jnp.int32, (8, EXTRA), 1)
        for k, at in enumerate(starts):
            row = at + lax.broadcasted_iota(jnp.int32, (8, rows), 0)
            mine = row == lax.broadcasted_iota(jnp.int32, (8, rows), 1)
            one = jnp.sum(jnp.where(mine, ints[0:1], 0), axis=1, keepdims=True)
            extra = jnp.where(
                lane == 0, jnp.sum(jnp.where(mine, ints[8:9], 0), axis=1, keepdims=True), 0
            )
            for d in range(3):
                digit = (one >> (DIGIT_BITS * d)) & (DIGITS - 1)
                extra = jnp.where(lane == d + 1, digit, extra)
            out_ref[8 * k : 8 * k + 8, width:] = extra.astype(jnp.float32).astype(jnp.bfloat16)
        for copy in copies[2:]:
            copy.wait()

    return call(
        kernel,
        (group[None], far(hidden), far(ids[None]), far(mask[None])),
        [((rows // 2, width + EXTRA), jnp.bfloat16)],
        in_specs=[SMEM, ANY, ANY, ANY],
        scratch=[pltpu.VMEM((16, rows), jnp.int32), pltpu.SemaphoreType.DMA((2 + rows // 16,))],
        mib=2,
    )[0]


def joined(*groups, after=()):
    sizes = [len(g) for g in groups]
    pieces = [p for g in groups for p in g]

    def kernel(*refs):
        ins, outs = list(refs[: len(pieces)]), refs[len(refs) - len(groups) :]
        for out_ref, size in zip(outs, sizes):
            at = 0
            for _ in range(size):
                ref = ins.pop(0)
                out_ref[at : at + ref.shape[0]] = ref[...]
                at += ref.shape[0]

    outs = [((sum(p.shape[0] for p in g), g[0].shape[1]), g[0].dtype) for g in groups]
    return call(kernel, [*pieces, *after], outs, mib=4)


def turned(a, b, width):
    rows = a.shape[0]
    cuts = 7

    def kernel(a_ref, b_ref, out_ref):
        for k in range(cuts):
            at = slice(k * width // cuts, (k + 1) * width // cuts)
            out_ref[at, :rows] = a_ref[:, at].T
            out_ref[at, rows:] = b_ref[:, at].T

    return call(kernel, [a, b], [((width, 2 * rows), a.dtype)], flops=10**9)[0]


def added(groups, blocks):
    sizes = [len(g) for g in groups]
    parts = [p for g in groups for p in g]

    def kernel(*refs):
        ins, outs = list(refs[: len(parts)]), list(refs[len(parts) :])
        for size in sizes:
            terms = [ins.pop(0) for _ in range(size)]
            cut = terms[0].shape[0] // blocks
            for k in range(blocks):
                at = slice(k * cut, (k + 1) * cut)
                total = sum(t[at].astype(jnp.float32) for t in terms[1:])
                outs.pop(0)[...] = (total + terms[0][at].astype(jnp.float32)).astype(jnp.bfloat16)

    outs = [
        ((g[0].shape[0] // blocks, g[0].shape[1]), jnp.bfloat16) for g in groups for _ in range(blocks)
    ]
    return call(kernel, parts, outs, mib=4)


def added_by_place(groups, spot):
    sizes = [len(g) for g in groups]
    parts = [p for g in groups for p in g]
    rows, width = parts[0].shape

    def kernel(spot_ref, *refs):
        ins, outs, sums = list(refs[: len(parts)]), refs[len(parts) : -1], refs[-1]
        for k, size in enumerate(sizes):
            terms = [ins.pop(0) for _ in range(size)]
            sums[k * rows : (k + 1) * rows] = sum(t[...].astype(jnp.float32) for t in terms)
        for k, out_ref in enumerate(outs):
            step = 0 if k == 0 else jnp.where(spot_ref[0] == 0, XORS[0][k - 1], XORS[1][k - 1])
            y = (spot_ref[2] * 2 + spot_ref[1]) ^ step
            at = pl.multiple_of(((y & 1) * 2 + (y >> 1)) * 8, 8)
            out_ref[...] = sums[pl.ds(at, 8), :].astype(jnp.bfloat16)

    blocks = len(groups) * rows // 8
    return call(
        kernel,
        [spot, *parts],
        [((8, width), jnp.bfloat16)] * blocks,
        in_specs=[SMEM] + [VMEM] * len(parts),
        scratch=[pltpu.VMEM((len(groups) * rows, width), jnp.float32)],
        mib=4,
    )


def combined(parts, spot=None):
    shape = parts[0].shape
    n = len(parts)

    def kernel(*refs):
        ins, outs = refs[:n], refs[n:]
        smax = functools.reduce(jnp.maximum, [r[0:1] for r in ins])
        tmax = functools.reduce(jnp.maximum, [r[3:4] for r in ins])
        stot = cross = ttot = pick = 0.0
        for r in ins:
            factor = jnp.exp(r[0:1] - smax)
            stot, cross = stot + r[1:2] * factor, cross + r[2:3] * factor
            ttot = ttot + r[4:5] * jnp.exp(r[3:4] - tmax)
            pick = pick + r[5:6]
        mask = ins[0][6:7]
        rows = [smax, stot, cross, tmax, ttot, pick, mask, mask]
        if spot is not None:
            spot_ref, *outs = outs
            student_shift, teacher_shift = smax + jnp.log(stot), tmax + jnp.log(ttot)
            apart = student_shift - teacher_shift
            row_kl = cross / stot - apart
            rows = [student_shift, apart + row_kl] + [mask] * 6
            lane = lax.broadcasted_iota(jnp.int32, (8, 128), 1)
            total = jnp.sum(mask * row_kl, axis=1, keepdims=True)
            count = jnp.sum(mask, axis=1, keepdims=True)
            row = (spot_ref[3] >> 1) * 8 + lax.broadcasted_iota(jnp.int32, (8, shape[1]), 0)
            mine = row == lax.broadcasted_iota(jnp.int32, (8, shape[1]), 1)
            ratio = jnp.sum(jnp.where(mine, pick - apart, 0.0), axis=1, keepdims=True)
            here = lane == lax.broadcasted_iota(jnp.int32, (8, 128), 0)
            ratio = jnp.sum(jnp.where(here, ratio, 0.0), axis=0, keepdims=True)
            line = lax.broadcasted_iota(jnp.int32, (8, 128), 0)
            outs[1][...] = jnp.where(line == 0, total, jnp.where(line == 1, count, ratio))
        for k, row in enumerate(rows):
            outs[0][k : k + 1] = row

    out = (shape, jnp.float32)
    if spot is None:
        return call(kernel, parts, [out], mib=2)[0]
    outs = [out, ((8, 128), jnp.float32)]
    return call(kernel, [*parts, spot], outs, in_specs=[VMEM] * n + [SMEM], mib=2)


def side_by_side(head, head_in):
    width, columns = head.shape
    cuts = 4

    def kernel(h_ref, g_ref, out_ref, mark_ref, sems):
        mark_ref[...] = jnp.zeros(mark_ref.shape, jnp.float32)
        copies = []
        for k in range(cuts):
            at = pl.ds(k * width // cuts, width // cuts)
            for ref, column in ((h_ref, 0), (g_ref, columns)):
                copies.append(
                    pltpu.make_async_copy(
                        ref.at[at], out_ref.at[at, pl.ds(column, columns)], sems.at[len(copies)]
                    )
                )
        for copy in copies:
            copy.start()
        for copy in copies:
            copy.wait()

    return call(
        kernel,
        (far(head), far(head_in)),
        [((width, 2 * columns), head.dtype), ((8, 128), jnp.float32)],
        in_specs=[ANY, ANY],
        scratch=[pltpu.SemaphoreType.DMA((2 * cuts,))],
        flops=4 * 10**9,
        mib=2,
    )


def logits_and_stats(spot, a, b, heads, teacher, teacher_in, places, which, before=None):
    f32 = jnp.float32
    width, both = heads.shape
    columns = both // 2
    part, rows, tokens = a.shape[0], 2 * a.shape[0], places.shape[0]
    chunk = 32

    def kernel(spot_ref, a_ref, b_ref, h_ref, t_ref, u_ref, p_ref, *rest):
        out_ref, stats_ref, states, placed = rest[-4:]
        states[:part] = a_ref[:, :width]
        states[part:] = b_ref[:, :width]
        out_ref[...] = jnp.dot(states[...], h_ref[...], preferred_element_type=f32)
        lanes = lax.broadcasted_iota(jnp.int32, (1, both), 1)
        base, other_base = spot_ref[3] * columns, (spot_ref[3] ^ 1) * columns
        column = jnp.where(lanes < columns, base + lanes, other_base + lanes - columns)
        spots = lax.broadcasted_iota(jnp.int32, (1, tokens), 1)
        placed[...] = jnp.zeros(placed.shape, f32)
        for k in range(rows // chunk):
            ref, at = (a_ref, k * chunk) if k * chunk < part else (b_ref, k * chunk - part)
            here = slice(k * chunk, (k + 1) * chunk)
            there = slice(which * rows + k * chunk, which * rows + (k + 1) * chunk)
            student, note = out_ref[here, :], ref[at : at + chunk, width:].astype(f32)
            teacher = jnp.concatenate([t_ref[there, :], u_ref[there, :]], axis=1).astype(f32)
            ids = note[:, 1:2] + DIGITS * note[:, 2:3] + DIGITS**2 * note[:, 3:4]
            chosen = ids.astype(jnp.int32) == column
            smax = jnp.max(student, axis=1, keepdims=True)
            tmax = jnp.max(teacher, axis=1, keepdims=True)
            shifted = jnp.exp(student - smax)
            differ = student - teacher
            sums = [
                smax,
                jnp.sum(shifted, axis=1, keepdims=True),
                jnp.sum(shifted * differ, axis=1, keepdims=True),
                tmax,
                jnp.sum(jnp.exp(teacher - tmax), axis=1, keepdims=True),
                jnp.sum(jnp.where(chosen, differ, 0.0), axis=1, keepdims=True),
                note[:, :1],
            ]
            mine = p_ref[there, :] == spots
            for r, value in enumerate(sums):
                found = jnp.where(mine, value, 0.0).reshape(chunk // 8, 8, tokens)
                placed[r] += jnp.sum(found, axis=0)
        for r in range(8):
            row = jnp.sum(placed[r], axis=0, keepdims=True)
            stats_ref[r : r + 1] = row if before is None else row + rest[0][r : r + 1]

    operands = [spot, a, b, heads, teacher, teacher_in, places]
    if before is not None:
        operands.append(before)
    return call(
        kernel,
        operands,
        [((rows, both), f32), ((8, tokens), f32)],
        in_specs=[SMEM] + [VMEM] * (len(operands) - 1),
        scratch=[pltpu.VMEM((rows, width), jnp.bfloat16), pltpu.VMEM((8, 8, tokens), f32)],
        flops=2 * rows * width * both,
    )


def gradients(student, shifts, heads, teacher, teacher_in, places, which):
    f32, bf16 = jnp.float32, jnp.bfloat16
    width, both = heads.shape
    columns = both // 2
    rows, tokens = student.shape[0], places.shape[0]
    part = rows // 2
    chunk, cuts = 32, 7

    def kernel(s_ref, c_ref, h_ref, t_ref, u_ref, p_ref, a_ref, b_ref, d_ref, e_ref, all_d):
        spots = lax.broadcasted_iota(jnp.int32, (1, tokens), 1)
        for k in range(rows // chunk):
            here = slice(k * chunk, (k + 1) * chunk)
            there = slice(which * rows + k * chunk, which * rows + (k + 1) * chunk)
            mine = p_ref[there, :] == spots

            def of_row(r):
                return jnp.sum(jnp.where(mine, c_ref[r : r + 1], 0.0), axis=1, keepdims=True)

            student = s_ref[here, :]
            teacher = jnp.concatenate([t_ref[there, :], u_ref[there, :]], axis=1).astype(f32)
            probs = of_row(2) * jnp.exp(student - of_row(0))
            found = (probs * (student - teacher - of_row(1))).astype(bf16)
            all_d[here, :] = found
            d_ref[here, :] = found[:, :columns]
            e_ref[here, :] = found[:, columns:]
        for k in range(cuts):
            at = slice(k * width // cuts, (k + 1) * width // cuts)
            product = lax.dot_general(
                all_d[...], h_ref[at, :], (((1,), (1,)), ((), ())), preferred_element_type=f32
            ).astype(bf16)
            a_ref[:, at] = product[:part]
            b_ref[:, at] = product[part:]

    return call(
        kernel,
        [student, shifts, heads, teacher, teacher_in, places],
        [((part, width), bf16)] * 2 + [((rows, columns), bf16)] * 2,
        scratch=[pltpu.VMEM((rows, both), bf16)],
        flops=2 * rows * width * both,
    )


def head_gradient(states, dlogits, blocks, before=None):
    bf16 = jnp.bfloat16
    width, columns = states[0].shape[0], dlogits[0].shape[1]
    block = 512
    tokens = sum(d.shape[0] for d in dlogits)
    n, m = len(states), len(states) + len(dlogits)

    def kernel(*refs):
        pieces, others = refs[:n], refs[n:m]
        out_ref, right, found, sems = refs[-4:]
        at = 0
        for ref in others:
            right[at : at + ref.shape[0]] = ref[...]
            at += ref.shape[0]
        copies = []
        for j, k in enumerate(blocks):
            left = jnp.concatenate([r[k * block : (k + 1) * block, :] for r in pieces], axis=1)
            product = jnp.dot(left, right[...], preferred_element_type=jnp.float32).astype(bf16)
            slot = j % 2
            if j >= 2:
                copies[j - 2].wait()
            found[slot] = product
            copies.append(
                pltpu.make_async_copy(
                    found.at[slot], out_ref.at[pl.ds(k * block, block)], sems.at[slot]
                )
            )
            copies[j].start()
        copies[-2].wait()
        copies[-1].wait()

    operands, specs = [*states, *dlogits], [VMEM] * m
    if before is not None:
        operands, specs = [*operands, before], [*specs, ANY]
    return call(
        kernel,
        operands,
        [((width, columns), bf16)],
        in_specs=specs,
        out_specs=[ANY],
        scratch=[
            pltpu.VMEM((tokens, columns), bf16),
            pltpu.VMEM((2, block, columns), bf16),
            pltpu.SemaphoreType.DMA((2,)),
        ],
        flops=2 * tokens * len(blocks) * block * columns,
        aliases={} if before is None else {m: 0},
    )[0]


def per_device(hidden, teacher_logits, sampled_ids, loss_mask, student_head):
    f32, bf16 = jnp.float32, jnp.bfloat16
    core, y_low = lax.axis_index(CORE), lax.axis_index("tok_0")
    z, x = lax.axis_index("tok_1"), lax.axis_index("tok_2")
    position = lax.axis_index(TOK_VOC)
    group = group_of(core, y_low, z, x)
    width, _ = student_head.shape
    tokens = teacher_logits.shape[0]
    rows = tokens // 2

    block = entry_block(group, hidden, sampled_ids, loss_mask)
    token = token_of_rows(group, z, x, rows)
    token_other = token_of_rows(1 - group, z, x, rows)
    places = (token // 16) * 8 + token % 8
    spot = jnp.stack([group, y_low, lax.axis_index("voc_0"), position])
    other = swap(block, "y", 0)
    head_in = swap_core(student_head)
    teacher_send = jnp.dot(one_hot(token_other, tokens, bf16), teacher_logits)
    own_group = jnp.broadcast_to(group == core, (8,))
    other, teacher_send, spot, places, own_group = together(
        other, teacher_send, spot, places, own_group
    )
    teacher_in = swap_core(teacher_send)
    near_a = jnp.where(y_low == 0, block, other)
    near_b = jnp.where(y_low == 0, other, block)

    pieces_a, pieces_b = [near_a], [near_b]
    for step in range(3):
        pieces_a.append(swap(near_a, "x", step))
        pieces_b.append(swap(near_b, "z", step))
    teacher = jnp.dot(one_hot(token, tokens, bf16), teacher_logits)
    *pieces, teacher = together(*pieces_a, *pieces_b, teacher)
    near_a, near_b = joined(pieces[:4], pieces[4:])

    far_a, far_b = swap(near_a, "z", 0), swap(near_b, "x", 0)
    heads, mark = side_by_side(student_head, head_in)
    near_a, near_b = joined((near_a, far_a), (near_b, far_b), after=(mark,))

    far_a, far_b = swap(near_a, "z", 1), swap(near_b, "x", 1)
    shared = (heads, teacher, teacher_in, places)
    near_other = swap_core(near_a), swap_core(near_b)
    student_near, stats = logits_and_stats(spot, near_a, near_b, *shared, 0)
    states = [turned(near_a, near_b, width)]
    far_a, far_b, student_near, stats, states[0] = together(
        far_a, far_b, student_near, stats, states[0]
    )
    student_far, stats = logits_and_stats(spot, far_a, far_b, *shared, 1, stats)
    pair = (far_a, far_b)
    for ring in ("x", "z", "y"):
        parts = [stats]
        for step in range(3):
            parts.append(swap(stats, ring, step))
        state = turned(*pair, width)
        states.append(state)
        if ring == "z":
            far_a, far_b, parts[0] = together(far_a, far_b, parts[0])
            pair = swap_core(far_a), swap_core(far_b)
        *parts, states[-1] = together(*parts, state)
        stats = combined(parts, spot if ring == "y" else None)
        if ring == "x":
            *pair, stats = together(*near_other, stats)
    stats, sums = stats

    far_sum_a, far_sum_b, *far_d = gradients(student_far, stats, *shared, 1)
    far_sum_a, far_sum_b, stats_later = together(far_sum_a, far_sum_b, stats)
    a_in, b_in = swap(far_sum_a, "z", 1), swap(far_sum_b, "x", 1)
    far_d_in = swap_core(far_d[1])
    near_sum_a, near_sum_b, *near_d = gradients(student_near, stats_later, *shared, 0)
    near_d_in = swap_core(near_d[1])
    all_d = (near_d[0], far_d[0], near_d_in, far_d_in)
    head_grad = head_gradient(states, all_d, range(4))
    a_in, b_in, near_sum_a, near_sum_b, head_grad, other_sums = together(
        a_in, b_in, near_sum_a, near_sum_b, head_grad, swap_core(sums)
    )
    keep_a, send_a, keep_b, send_b = added(((near_sum_a, a_in), (near_sum_b, b_in)), 2)
    a_in, b_in = swap(send_a, "z", 0), swap(send_b, "x", 0)
    head_grad = head_gradient(states, all_d, range(4, width // 512), head_grad)
    a_in, b_in, head_grad = together(a_in, b_in, head_grad)
    keep_a, *send_a, keep_b, to_1, to_2, to_3 = added(((keep_a, a_in), (keep_b, b_in)), 4)
    arrived = [
        swap(part, ring, step)
        for step in range(3)
        for part, ring in ((send_a[step], "x"), ((to_1, to_2, to_3)[step], "z"))
    ]
    loss = (sums[0, 0] + other_sums[0, 0]) / (sums[1, 0] + other_sums[1, 0])
    sampled_ratio = jnp.where(own_group, sums[2, :8], other_sums[2, :8])
    *arrived, loss, sampled_ratio = together(*arrived, loss, sampled_ratio)
    keep, *send = added_by_place(((keep_a, *arrived[0::2]), (keep_b, *arrived[1::2])), spot)
    arrived = [to_owner(part, step) for step, part in enumerate(send)]
    parts = [to_owner(keep), *arrived]
    hidden_grad = sum(p.astype(f32) for p in parts).astype(bf16)
    return (loss, sampled_ratio, hidden_grad, head_grad)


def solution(mesh):
    split = Mesh(mesh.devices.reshape(2, 4, 4, 2, 2), TOK_VOC)
    in_specs = (P(TOK, None), P(None, TOK_VOC), P(TOK), P(TOK), P(None, TOK_VOC))
    out_specs = (P(), P(TOK_VOC), P(TOK_VOC, None), P(None, TOK_VOC))

    return jax.shard_map(
        per_device, mesh=split, in_specs=in_specs, out_specs=out_specs, check_vma=False
    )
```

```python
import functools
import itertools

import jax
import jax.numpy as jnp
from jax import lax
from jax.experimental import pallas as pl
from jax.experimental.pallas import tpu as pltpu
from jax.sharding import Mesh
from jax.sharding import PartitionSpec as P

TOK = ("tok_0", "tok_1", "tok_2")
TOK_VOC = ("tok_0", "tok_1", "tok_2", "voc_0", "voc_1")
CORE = "voc_1"
DIGIT_BITS = 6
DIGITS = 1 << DIGIT_BITS
EXTRA = 128
INTERPRET = False
XORS = ((1, 3, 2), (3, 1, 2))


def group_of(core, y, z, x):
    return core ^ ((x ^ y ^ z) & 1)


def moved(value, target):
    pairs = []
    for y, z, x, c in itertools.product(range(4), range(4), range(4), range(2)):
        pairs.append(
            tuple(
                ((((v % 2) * 4 + w) * 4 + u) * 2 + v // 2) * 2 + d
                for v, w, u, d in ((y, z, x, c), target(y, z, x, c))
            )
        )
    return lax.ppermute(value, TOK_VOC, pairs)


def swap(value, ring, step):
    def target(y, z, x, c):
        group = group_of(c, y, z, x)
        xor = XORS[group][step]
        at = {"y": y, "z": z, "x": x}
        at[ring] ^= xor
        return at["y"], at["z"], at["x"], group_of(group, at["y"], at["z"], at["x"])

    return moved(value, target)


def along(value, own, step):
    def target(y, z, x, c):
        group = group_of(c, y, z, x)
        xor = XORS[group][step]
        even = (y % 2 == 0) == own
        to_z, to_x = (z, x ^ xor) if even else (z ^ xor, x)
        return y, to_z, to_x, group_of(group, y, to_z, to_x)

    return moved(value, target)


def to_owner(value, step=None):
    def target(y, z, x, c):
        group = group_of(c, y, z, x)
        return y if step is None else y ^ XORS[group][step], z, x, group

    return moved(value, target)


def swap_core(value):
    return lax.ppermute(value, CORE, [(0, 1), (1, 0)])


def together(*values):
    return lax.optimization_barrier(values)


def token_of_rows(group, z, x, rows):
    n = lax.broadcasted_iota(jnp.int32, (rows, 1), 0)
    quarter = rows // 8
    half, part, top = n // (4 * quarter), (n // (2 * quarter)) % 2, (n // quarter) % 2
    high = half * 2 + top
    low = (n // (quarter // 4)) % 4
    mid = (n // 8) % 2
    first = jnp.where(group == 0, XORS[0][0], XORS[1][0])
    second = jnp.where(group == 0, XORS[0][1], XORS[1][1])

    def place(own, k):
        return own ^ ((k % 2) * first) ^ ((k // 2) * second)

    z_at = jnp.where(part == 0, place(z, high), place(z, low))
    x_at = jnp.where(part == 0, place(x, low), place(x, high))
    return ((((part * 4 + z_at) * 4 + x_at) * 2 + mid) * 2 + group) * 8 + n % 8


def one_hot(rows, columns, dtype):
    return (rows == lax.broadcasted_iota(jnp.int32, (1, columns), 1)).astype(dtype)


VMEM = pl.BlockSpec(memory_space=pltpu.VMEM)
SMEM = pl.BlockSpec(memory_space=pltpu.SMEM)
ANY = pl.BlockSpec(memory_space=pl.ANY)


def near(value):
    return value if INTERPRET else pltpu.with_memory_space_constraint(value, pltpu.VMEM)


def far(value):
    return value if INTERPRET else pltpu.with_memory_space_constraint(value, pltpu.HBM)


def call(kernel, operands, outs, in_specs=None, out_specs=None, flops=10**6, scratch=(), mib=16, aliases={}):
    in_specs = in_specs or [VMEM] * len(operands)
    out_specs = out_specs or [VMEM] * len(outs)
    shapes = [
        pltpu.VMEM(shape, dtype)
        if spec is VMEM and not INTERPRET
        else jax.ShapeDtypeStruct(shape, dtype)
        for (shape, dtype), spec in zip(outs, out_specs)
    ]
    operands = [near(v) if spec is VMEM else v for v, spec in zip(operands, in_specs)]
    return pl.pallas_call(
        kernel,
        out_shape=shapes,
        in_specs=in_specs,
        out_specs=out_specs,
        scratch_shapes=scratch,
        input_output_aliases=aliases,
        compiler_params=pltpu.CompilerParams(vmem_limit_bytes=mib << 20),
        cost_estimate=pl.CostEstimate(flops=flops, bytes_accessed=10**6, transcendentals=0),
        interpret=INTERPRET,
    )(*operands)


def entry_block(group, hidden, ids, mask):
    rows, width = hidden.shape

    def kernel(group_ref, hidden_ref, ids_ref, mask_ref, out_ref, ints, sems):
        starts = [8 * (2 * k + group_ref[0]) for k in range(rows // 16)]
        copies = [
            pltpu.make_async_copy(ids_ref, ints.at[pl.ds(0, 1)], sems.at[0]),
            pltpu.make_async_copy(mask_ref, ints.at[pl.ds(8, 1)], sems.at[1]),
        ]
        for k, at in enumerate(starts):
            copies.append(
                pltpu.make_async_copy(
                    hidden_ref.at[pl.ds(pl.multiple_of(at, 8), 8)],
                    out_ref.at[pl.ds(8 * k, 8), pl.ds(0, width)],
                    sems.at[2 + k],
                )
            )
        for copy in copies:
            copy.start()
        copies[0].wait()
        copies[1].wait()
        lane = lax.broadcasted_iota(jnp.int32, (8, EXTRA), 1)
        for k, at in enumerate(starts):
            row = at + lax.broadcasted_iota(jnp.int32, (8, rows), 0)
            mine = row == lax.broadcasted_iota(jnp.int32, (8, rows), 1)
            one = jnp.sum(jnp.where(mine, ints[0:1], 0), axis=1, keepdims=True)
            extra = jnp.where(
                lane == 0, jnp.sum(jnp.where(mine, ints[8:9], 0), axis=1, keepdims=True), 0
            )
            for d in range(3):
                digit = (one >> (DIGIT_BITS * d)) & (DIGITS - 1)
                extra = jnp.where(lane == d + 1, digit, extra)
            out_ref[8 * k : 8 * k + 8, width:] = extra.astype(jnp.float32).astype(jnp.bfloat16)
        for copy in copies[2:]:
            copy.wait()

    return call(
        kernel,
        (group[None], far(hidden), far(ids[None]), far(mask[None])),
        [((rows // 2, width + EXTRA), jnp.bfloat16)],
        in_specs=[SMEM, ANY, ANY, ANY],
        scratch=[pltpu.VMEM((16, rows), jnp.int32), pltpu.SemaphoreType.DMA((2 + rows // 16,))],
        mib=2,
    )[0]


def joined(*groups, after=(), parity=None):
    sizes = [len(g) for g in groups]
    pieces = [p for g in groups for p in g]
    n = len(pieces)

    def kernel(*refs):
        outs = refs[len(refs) - len(groups) :]

        def put(outs):
            ins = list(refs[:n])
            for out_ref, size in zip(outs, sizes):
                at = 0
                for _ in range(size):
                    ref = ins.pop(0)
                    out_ref[at : at + ref.shape[0]] = ref[...]
                    at += ref.shape[0]

        if parity is None:
            put(outs)
        else:
            pl.when(refs[n][1] == 0)(lambda: put(outs))
            pl.when(refs[n][1] != 0)(lambda: put(outs[::-1]))

    outs = [((sum(p.shape[0] for p in g), g[0].shape[1]), g[0].dtype) for g in groups]
    operands, specs = [*pieces, *after], [VMEM] * (n + len(after))
    if parity is not None:
        operands, specs = [*operands, parity], [*specs, SMEM]
    return call(kernel, operands, outs, in_specs=specs, mib=4)


def turned(a, b, width):
    rows = a.shape[0]
    cuts = 7

    def kernel(a_ref, b_ref, out_ref):
        for k in range(cuts):
            at = slice(k * width // cuts, (k + 1) * width // cuts)
            out_ref[at, :rows] = a_ref[:, at].T
            out_ref[at, rows:] = b_ref[:, at].T

    return call(kernel, [a, b], [((width, 2 * rows), a.dtype)], flops=10**9)[0]


def added(groups, blocks, parity=None):
    sizes = [len(g) for g in groups]
    parts = [p for g in groups for p in g]
    n = len(parts)

    def kernel(*refs):
        outs = refs[len(refs) - blocks * len(groups) :]

        def put(outs):
            ins, outs = list(refs[:n]), list(outs)
            for size in sizes:
                terms = [ins.pop(0) for _ in range(size)]
                cut = terms[0].shape[0] // blocks
                for k in range(blocks):
                    at = slice(k * cut, (k + 1) * cut)
                    total = sum(t[at].astype(jnp.float32) for t in terms)
                    outs.pop(0)[...] = total.astype(jnp.bfloat16)

        if parity is None:
            put(outs)
        else:
            pl.when(refs[n][1] == 0)(lambda: put(outs))
            pl.when(refs[n][1] != 0)(lambda: put(outs[blocks:] + outs[:blocks]))

    outs = [
        ((g[0].shape[0] // blocks, g[0].shape[1]), jnp.bfloat16) for g in groups for _ in range(blocks)
    ]
    operands, specs = parts, [VMEM] * n
    if parity is not None:
        operands, specs = [*parts, parity], [*specs, SMEM]
    return call(kernel, operands, outs, in_specs=specs, mib=4)


def added_by_place(parts, spot, steps, after=()):
    rows, width = parts[0].shape

    def kernel(spot_ref, *refs):
        ins, outs, sums = refs[: len(parts)], refs[len(parts) + len(after) : -1], refs[-1]
        sums[...] = sum(t[...].astype(jnp.float32) for t in ins)
        for k, out_ref in zip(steps, outs):
            xor = 0 if k is None else jnp.where(spot_ref[0] == 0, XORS[0][k], XORS[1][k])
            at = pl.multiple_of((spot_ref[2] ^ (xor >> 1)) * 8, 8)
            out_ref[...] = sums[pl.ds(at, 8), :].astype(jnp.bfloat16)

    return call(
        kernel,
        [spot, *parts, *after],
        [((8, width), jnp.bfloat16)] * len(steps),
        in_specs=[SMEM] + [VMEM] * (len(parts) + len(after)),
        scratch=[pltpu.VMEM((rows, width), jnp.float32)],
        mib=4,
    )


def combined(parts, spot=None):
    shape = parts[0].shape
    n = len(parts)

    def kernel(*refs):
        ins, outs = refs[:n], refs[n:]
        smax = functools.reduce(jnp.maximum, [r[0:1] for r in ins])
        tmax = functools.reduce(jnp.maximum, [r[3:4] for r in ins])
        stot = cross = ttot = pick = 0.0
        for r in ins:
            factor = jnp.exp(r[0:1] - smax)
            stot, cross = stot + r[1:2] * factor, cross + r[2:3] * factor
            ttot = ttot + r[4:5] * jnp.exp(r[3:4] - tmax)
            pick = pick + r[5:6]
        mask = ins[0][6:7]
        rows = [smax, stot, cross, tmax, ttot, pick, mask, mask]
        if spot is not None:
            spot_ref, *outs = outs
            student_shift, teacher_shift = smax + jnp.log(stot), tmax + jnp.log(ttot)
            apart = student_shift - teacher_shift
            row_kl = cross / stot - apart
            rows = [student_shift, apart + row_kl] + [mask] * 6
            lane = lax.broadcasted_iota(jnp.int32, (8, 128), 1)
            total = jnp.sum(mask * row_kl, axis=1, keepdims=True)
            count = jnp.sum(mask, axis=1, keepdims=True)
            row = (spot_ref[3] >> 1) * 8 + lax.broadcasted_iota(jnp.int32, (8, shape[1]), 0)
            mine = row == lax.broadcasted_iota(jnp.int32, (8, shape[1]), 1)
            ratio = jnp.sum(jnp.where(mine, pick - apart, 0.0), axis=1, keepdims=True)
            here = lane == lax.broadcasted_iota(jnp.int32, (8, 128), 0)
            ratio = jnp.sum(jnp.where(here, ratio, 0.0), axis=0, keepdims=True)
            line = lax.broadcasted_iota(jnp.int32, (8, 128), 0)
            outs[1][...] = jnp.where(line == 0, total, jnp.where(line == 1, count, ratio))
        for k, row in enumerate(rows):
            outs[0][k : k + 1] = row

    out = (shape, jnp.float32)
    if spot is None:
        return call(kernel, parts, [out], mib=2)[0]
    outs = [out, ((8, 128), jnp.float32)]
    return call(kernel, [*parts, spot], outs, in_specs=[VMEM] * n + [SMEM], mib=2)


def side_by_side(head, head_in):
    width, columns = head.shape
    cuts = 4

    def kernel(h_ref, g_ref, out_ref, mark_ref, sems):
        mark_ref[...] = jnp.zeros(mark_ref.shape, jnp.float32)
        copies = []
        for k in range(cuts):
            at = pl.ds(k * width // cuts, width // cuts)
            for ref, column in ((h_ref, 0), (g_ref, columns)):
                copies.append(
                    pltpu.make_async_copy(
                        ref.at[at], out_ref.at[at, pl.ds(column, columns)], sems.at[len(copies)]
                    )
                )
        for copy in copies:
            copy.start()
        for copy in copies:
            copy.wait()

    return call(
        kernel,
        (far(head), far(head_in)),
        [((width, 2 * columns), head.dtype), ((8, 128), jnp.float32)],
        in_specs=[ANY, ANY],
        scratch=[pltpu.SemaphoreType.DMA((2 * cuts,))],
        flops=4 * 10**9,
        mib=2,
    )


def logits_and_stats(spot, a, b, heads, teacher, teacher_in, places, which, before=None):
    f32 = jnp.float32
    width, both = heads.shape
    columns = both // 2
    part, rows, tokens = a.shape[0], 2 * a.shape[0], places.shape[0]
    chunk = 32

    def kernel(spot_ref, a_ref, b_ref, h_ref, t_ref, u_ref, p_ref, *rest):
        out_ref, stats_ref, states, placed = rest[-4:]
        states[:part] = a_ref[:, :width]
        states[part:] = b_ref[:, :width]
        out_ref[...] = jnp.dot(states[...], h_ref[...], preferred_element_type=f32)
        lanes = lax.broadcasted_iota(jnp.int32, (1, both), 1)
        base, other_base = spot_ref[3] * columns, (spot_ref[3] ^ 1) * columns
        column = jnp.where(lanes < columns, base + lanes, other_base + lanes - columns)
        spots = lax.broadcasted_iota(jnp.int32, (1, tokens), 1)
        placed[...] = jnp.zeros(placed.shape, f32)
        for k in range(rows // chunk):
            ref, at = (a_ref, k * chunk) if k * chunk < part else (b_ref, k * chunk - part)
            here = slice(k * chunk, (k + 1) * chunk)
            there = slice(which * rows + k * chunk, which * rows + (k + 1) * chunk)
            student, note = out_ref[here, :], ref[at : at + chunk, width:].astype(f32)
            teacher = jnp.concatenate([t_ref[there, :], u_ref[there, :]], axis=1).astype(f32)
            ids = note[:, 1:2] + DIGITS * note[:, 2:3] + DIGITS**2 * note[:, 3:4]
            chosen = ids.astype(jnp.int32) == column
            smax = jnp.max(student, axis=1, keepdims=True)
            tmax = jnp.max(teacher, axis=1, keepdims=True)
            shifted = jnp.exp(student - smax)
            differ = student - teacher
            sums = [
                smax,
                jnp.sum(shifted, axis=1, keepdims=True),
                jnp.sum(shifted * differ, axis=1, keepdims=True),
                tmax,
                jnp.sum(jnp.exp(teacher - tmax), axis=1, keepdims=True),
                jnp.sum(jnp.where(chosen, differ, 0.0), axis=1, keepdims=True),
                note[:, :1],
            ]
            mine = p_ref[there, :] == spots
            for r, value in enumerate(sums):
                found = jnp.where(mine, value, 0.0).reshape(chunk // 8, 8, tokens)
                placed[r] += jnp.sum(found, axis=0)
        for r in range(8):
            row = jnp.sum(placed[r], axis=0, keepdims=True)
            stats_ref[r : r + 1] = row if before is None else row + rest[0][r : r + 1]

    operands = [spot, a, b, heads, teacher, teacher_in, places]
    if before is not None:
        operands.append(before)
    return call(
        kernel,
        operands,
        [((rows, both), f32), ((8, tokens), f32)],
        in_specs=[SMEM] + [VMEM] * (len(operands) - 1),
        scratch=[pltpu.VMEM((rows, width), jnp.bfloat16), pltpu.VMEM((8, 8, tokens), f32)],
        flops=2 * rows * width * both,
    )


def gradients(student, shifts, heads, teacher, teacher_in, places, which):
    f32, bf16 = jnp.float32, jnp.bfloat16
    width, both = heads.shape
    columns = both // 2
    rows, tokens = student.shape[0], places.shape[0]
    part = rows // 2
    chunk, cuts = 32, 7

    def kernel(s_ref, c_ref, h_ref, t_ref, u_ref, p_ref, a_ref, b_ref, d_ref, e_ref, all_d):
        spots = lax.broadcasted_iota(jnp.int32, (1, tokens), 1)
        for k in range(rows // chunk):
            here = slice(k * chunk, (k + 1) * chunk)
            there = slice(which * rows + k * chunk, which * rows + (k + 1) * chunk)
            mine = p_ref[there, :] == spots

            def of_row(r):
                return jnp.sum(jnp.where(mine, c_ref[r : r + 1], 0.0), axis=1, keepdims=True)

            student = s_ref[here, :]
            teacher = jnp.concatenate([t_ref[there, :], u_ref[there, :]], axis=1).astype(f32)
            probs = of_row(2) * jnp.exp(student - of_row(0))
            found = (probs * (student - teacher - of_row(1))).astype(bf16)
            all_d[here, :] = found
            d_ref[here, :] = found[:, :columns]
            e_ref[here, :] = found[:, columns:]
        for k in range(cuts):
            at = slice(k * width // cuts, (k + 1) * width // cuts)
            product = lax.dot_general(
                all_d[...], h_ref[at, :], (((1,), (1,)), ((), ())), preferred_element_type=f32
            ).astype(bf16)
            a_ref[:, at] = product[:part]
            b_ref[:, at] = product[part:]

    return call(
        kernel,
        [student, shifts, heads, teacher, teacher_in, places],
        [((part, width), bf16)] * 2 + [((rows, columns), bf16)] * 2,
        scratch=[pltpu.VMEM((rows, both), bf16)],
        flops=2 * rows * width * both,
    )


def head_gradient(states, dlogits, blocks, before=None):
    bf16 = jnp.bfloat16
    width, columns = states[0].shape[0], dlogits[0].shape[1]
    block = 512
    tokens = sum(d.shape[0] for d in dlogits)
    n, m = len(states), len(states) + len(dlogits)

    def kernel(*refs):
        pieces, others = refs[:n], refs[n:m]
        out_ref, right, found, sems = refs[-4:]
        at = 0
        for ref in others:
            right[at : at + ref.shape[0]] = ref[...]
            at += ref.shape[0]
        copies = []
        for j, k in enumerate(blocks):
            left = jnp.concatenate([r[k * block : (k + 1) * block, :] for r in pieces], axis=1)
            product = jnp.dot(left, right[...], preferred_element_type=jnp.float32).astype(bf16)
            slot = j % 2
            if j >= 2:
                copies[j - 2].wait()
            found[slot] = product
            copies.append(
                pltpu.make_async_copy(
                    found.at[slot], out_ref.at[pl.ds(k * block, block)], sems.at[slot]
                )
            )
            copies[j].start()
        copies[-2].wait()
        copies[-1].wait()

    operands, specs = [*states, *dlogits], [VMEM] * m
    if before is not None:
        operands, specs = [*operands, before], [*specs, ANY]
    return call(
        kernel,
        operands,
        [((width, columns), bf16)],
        in_specs=specs,
        out_specs=[ANY],
        scratch=[
            pltpu.VMEM((tokens, columns), bf16),
            pltpu.VMEM((2, block, columns), bf16),
            pltpu.SemaphoreType.DMA((2,)),
        ],
        flops=2 * tokens * len(blocks) * block * columns,
        aliases={} if before is None else {m: 0},
    )[0]


def per_device(hidden, teacher_logits, sampled_ids, loss_mask, student_head):
    f32, bf16 = jnp.float32, jnp.bfloat16
    core, y_low = lax.axis_index(CORE), lax.axis_index("tok_0")
    z, x = lax.axis_index("tok_1"), lax.axis_index("tok_2")
    position = lax.axis_index(TOK_VOC)
    group = group_of(core, y_low, z, x)
    width, _ = student_head.shape
    tokens = teacher_logits.shape[0]
    rows = tokens // 2

    block = entry_block(group, hidden, sampled_ids, loss_mask)
    token = token_of_rows(group, z, x, rows)
    token_other = token_of_rows(1 - group, z, x, rows)
    places = (token // 16) * 8 + token % 8
    spot = jnp.stack([group, y_low, lax.axis_index("voc_0"), position])
    other = swap(block, "y", 0)
    head_in = swap_core(student_head)
    teacher_send = jnp.dot(one_hot(token_other, tokens, bf16), teacher_logits)
    own_group = jnp.broadcast_to(group == core, (8,))
    other, teacher_send, spot, places, own_group = together(
        other, teacher_send, spot, places, own_group
    )
    teacher_in = swap_core(teacher_send)
    own, across = [block], [other]
    for step in range(3):
        own.append(along(block, True, step))
    for step in range(3):
        across.append(along(other, False, step))
    teacher = jnp.dot(one_hot(token, tokens, bf16), teacher_logits)
    *pieces, teacher = together(*own, *across, teacher)
    near_a, near_b = joined(pieces[:4], pieces[4:], parity=spot)

    far_a, far_b = swap(near_a, "z", 0), swap(near_b, "x", 0)
    heads, mark = side_by_side(student_head, head_in)
    near_a, near_b = joined((near_a, far_a), (near_b, far_b), after=(mark,))

    far_a, far_b = swap(near_a, "z", 1), swap(near_b, "x", 1)
    shared = (heads, teacher, teacher_in, places)
    near_other = swap_core(near_a), swap_core(near_b)
    student_near, stats = logits_and_stats(spot, near_a, near_b, *shared, 0)
    states = [turned(near_a, near_b, width)]
    far_a, far_b, student_near, stats, states[0] = together(
        far_a, far_b, student_near, stats, states[0]
    )
    student_far, stats = logits_and_stats(spot, far_a, far_b, *shared, 1, stats)
    pair = (far_a, far_b)
    for ring in ("x", "z", "y"):
        parts = [stats]
        for step in range(3):
            parts.append(swap(stats, ring, step))
        state = turned(*pair, width)
        states.append(state)
        if ring == "z":
            far_a, far_b, parts[0] = together(far_a, far_b, parts[0])
            pair = swap_core(far_a), swap_core(far_b)
        *parts, states[-1] = together(*parts, state)
        stats = combined(parts, spot if ring == "y" else None)
        if ring == "x":
            *pair, stats = together(*near_other, stats)
    stats, sums = stats

    far_sum_a, far_sum_b, *far_d = gradients(student_far, stats, *shared, 1)
    far_sum_a, far_sum_b, stats_later = together(far_sum_a, far_sum_b, stats)
    a_in, b_in = swap(far_sum_a, "z", 1), swap(far_sum_b, "x", 1)
    far_d_in = swap_core(far_d[1])
    near_sum_a, near_sum_b, *near_d = gradients(student_near, stats_later, *shared, 0)
    near_d_in = swap_core(near_d[1])
    all_d = (near_d[0], far_d[0], near_d_in, far_d_in)
    head_grad = head_gradient(states, all_d, range(4))
    a_in, b_in, near_sum_a, near_sum_b, head_grad, other_sums = together(
        a_in, b_in, near_sum_a, near_sum_b, head_grad, swap_core(sums)
    )
    keep_a, send_a, keep_b, send_b = added(((near_sum_a, a_in), (near_sum_b, b_in)), 2)
    a_in, b_in = swap(send_a, "z", 0), swap(send_b, "x", 0)
    head_grad = head_gradient(states, all_d, range(4, width // 512), head_grad)
    a_in, b_in, head_grad = together(a_in, b_in, head_grad)
    *own, across, to_1, to_2, to_3 = added(((keep_a, a_in), (keep_b, b_in)), 4, spot)
    across_in = []
    for step, part in enumerate((to_1, to_2, to_3)):
        across_in.append(along(part, False, step))
    own_in = []
    for step in range(3):
        own_in.append(along(own[step + 1], True, step))
    send = added_by_place((across, *across_in), spot, (0, 1))
    arrived = [to_owner(part, step) for step, part in enumerate(send)]
    keep, last = added_by_place((own[0], *own_in), spot, (None, 2), after=(send[0],))
    keep, sums, other_sums = together(keep, sums, other_sums)
    parts = [to_owner(keep), *arrived, to_owner(last, 2)]
    loss = (sums[0, 0] + other_sums[0, 0]) / (sums[1, 0] + other_sums[1, 0])
    sampled_ratio = jnp.where(own_group, sums[2, :8], other_sums[2, :8])
    hidden_grad = sum(p.astype(f32) for p in parts).astype(bf16)
    return (loss, sampled_ratio, hidden_grad, head_grad)


def solution(mesh):
    split = Mesh(mesh.devices.reshape(2, 4, 4, 2, 2), TOK_VOC)
    in_specs = (P(TOK, None), P(None, TOK_VOC), P(TOK), P(TOK), P(None, TOK_VOC))
    out_specs = (P(), P(TOK_VOC), P(TOK_VOC, None), P(None, TOK_VOC))

    return jax.shard_map(
        per_device, mesh=split, in_specs=in_specs, out_specs=out_specs, check_vma=False
    )
```

```python
import functools
import itertools

import jax
import jax.numpy as jnp
from jax import lax
from jax.experimental import pallas as pl
from jax.experimental.pallas import tpu as pltpu
from jax.sharding import Mesh
from jax.sharding import PartitionSpec as P

TOK = ("tok_0", "tok_1", "tok_2")
TOK_VOC = ("tok_0", "tok_1", "tok_2", "voc_0", "voc_1")
CORE = "voc_1"
DIGIT_BITS = 6
DIGITS = 1 << DIGIT_BITS
EXTRA = 128
INTERPRET = False
XORS = ((1, 3, 2), (3, 1, 2))


def group_of(core, y, z, x):
    return core ^ ((x ^ y ^ z) & 1)


def moved(value, target):
    pairs = []
    for y, z, x, c in itertools.product(range(4), range(4), range(4), range(2)):
        pairs.append(
            tuple(
                ((((v % 2) * 4 + w) * 4 + u) * 2 + v // 2) * 2 + d
                for v, w, u, d in ((y, z, x, c), target(y, z, x, c))
            )
        )
    return lax.ppermute(value, TOK_VOC, pairs)


def swap(value, ring, step):
    def target(y, z, x, c):
        group = group_of(c, y, z, x)
        xor = XORS[group][step]
        at = {"y": y, "z": z, "x": x}
        at[ring] ^= xor
        return at["y"], at["z"], at["x"], group_of(group, at["y"], at["z"], at["x"])

    return moved(value, target)


def along(value, own, step):
    def target(y, z, x, c):
        group = group_of(c, y, z, x)
        xor = XORS[group][step]
        even = (y % 2 == 0) == own
        to_z, to_x = (z, x ^ xor) if even else (z ^ xor, x)
        return y, to_z, to_x, group_of(group, y, to_z, to_x)

    return moved(value, target)


def to_owner(value, step=None):
    def target(y, z, x, c):
        group = group_of(c, y, z, x)
        return y if step is None else y ^ XORS[group][step], z, x, group

    return moved(value, target)


def swap_core(value):
    return lax.ppermute(value, CORE, [(0, 1), (1, 0)])


def together(*values):
    return lax.optimization_barrier(values)


def token_of_rows(group, z, x, rows):
    n = lax.broadcasted_iota(jnp.int32, (rows, 1), 0)
    quarter = rows // 8
    half, part, top = n // (4 * quarter), (n // (2 * quarter)) % 2, (n // quarter) % 2
    high = half * 2 + top
    low = (n // (quarter // 4)) % 4
    mid = (n // 8) % 2
    first = jnp.where(group == 0, XORS[0][0], XORS[1][0])
    second = jnp.where(group == 0, XORS[0][1], XORS[1][1])

    def place(own, k):
        return own ^ ((k % 2) * first) ^ ((k // 2) * second)

    z_at = jnp.where(part == 0, place(z, high), place(z, low))
    x_at = jnp.where(part == 0, place(x, low), place(x, high))
    return ((((part * 4 + z_at) * 4 + x_at) * 2 + mid) * 2 + group) * 8 + n % 8


def one_hot(rows, columns, dtype):
    return (rows == lax.broadcasted_iota(jnp.int32, (1, columns), 1)).astype(dtype)


VMEM = pl.BlockSpec(memory_space=pltpu.VMEM)
SMEM = pl.BlockSpec(memory_space=pltpu.SMEM)
ANY = pl.BlockSpec(memory_space=pl.ANY)


def near(value):
    return value if INTERPRET else pltpu.with_memory_space_constraint(value, pltpu.VMEM)


def far(value):
    return value if INTERPRET else pltpu.with_memory_space_constraint(value, pltpu.HBM)


def call(kernel, operands, outs, in_specs=None, out_specs=None, flops=10**6, scratch=(), mib=16, aliases={}):
    in_specs = in_specs or [VMEM] * len(operands)
    out_specs = out_specs or [VMEM] * len(outs)
    shapes = [
        pltpu.VMEM(shape, dtype)
        if spec is VMEM and not INTERPRET
        else jax.ShapeDtypeStruct(shape, dtype)
        for (shape, dtype), spec in zip(outs, out_specs)
    ]
    operands = [near(v) if spec is VMEM else v for v, spec in zip(operands, in_specs)]
    return pl.pallas_call(
        kernel,
        out_shape=shapes,
        in_specs=in_specs,
        out_specs=out_specs,
        scratch_shapes=scratch,
        input_output_aliases=aliases,
        compiler_params=pltpu.CompilerParams(vmem_limit_bytes=mib << 20),
        cost_estimate=pl.CostEstimate(flops=flops, bytes_accessed=10**6, transcendentals=0),
        interpret=INTERPRET,
    )(*operands)


def entry_block(group, hidden, ids, mask):
    rows, width = hidden.shape

    def kernel(group_ref, hidden_ref, ids_ref, mask_ref, out_ref, ints, sems):
        starts = [8 * (2 * k + group_ref[0]) for k in range(rows // 16)]
        copies = [
            pltpu.make_async_copy(ids_ref, ints.at[pl.ds(0, 1)], sems.at[0]),
            pltpu.make_async_copy(mask_ref, ints.at[pl.ds(8, 1)], sems.at[1]),
        ]
        for k, at in enumerate(starts):
            copies.append(
                pltpu.make_async_copy(
                    hidden_ref.at[pl.ds(pl.multiple_of(at, 8), 8)],
                    out_ref.at[pl.ds(8 * k, 8), pl.ds(0, width)],
                    sems.at[2 + k],
                )
            )
        for copy in copies:
            copy.start()
        copies[0].wait()
        copies[1].wait()
        lane = lax.broadcasted_iota(jnp.int32, (8, EXTRA), 1)
        for k, at in enumerate(starts):
            row = at + lax.broadcasted_iota(jnp.int32, (8, rows), 0)
            mine = row == lax.broadcasted_iota(jnp.int32, (8, rows), 1)
            one = jnp.sum(jnp.where(mine, ints[0:1], 0), axis=1, keepdims=True)
            extra = jnp.where(
                lane == 0, jnp.sum(jnp.where(mine, ints[8:9], 0), axis=1, keepdims=True), 0
            )
            for d in range(3):
                digit = (one >> (DIGIT_BITS * d)) & (DIGITS - 1)
                extra = jnp.where(lane == d + 1, digit, extra)
            out_ref[8 * k : 8 * k + 8, width:] = extra.astype(jnp.float32).astype(jnp.bfloat16)
        for copy in copies[2:]:
            copy.wait()

    return call(
        kernel,
        (group[None], far(hidden), far(ids[None]), far(mask[None])),
        [((rows // 2, width + EXTRA), jnp.bfloat16)],
        in_specs=[SMEM, ANY, ANY, ANY],
        scratch=[pltpu.VMEM((16, rows), jnp.int32), pltpu.SemaphoreType.DMA((2 + rows // 16,))],
        mib=2,
    )[0]


def joined(*groups, after=(), parity=None):
    sizes = [len(g) for g in groups]
    pieces = [p for g in groups for p in g]
    n = len(pieces)

    def kernel(*refs):
        outs = refs[len(refs) - len(groups) :]

        def put(outs):
            ins = list(refs[:n])
            for out_ref, size in zip(outs, sizes):
                at = 0
                for _ in range(size):
                    ref = ins.pop(0)
                    out_ref[at : at + ref.shape[0]] = ref[...]
                    at += ref.shape[0]

        if parity is None:
            put(outs)
        else:
            pl.when(refs[n][1] == 0)(lambda: put(outs))
            pl.when(refs[n][1] != 0)(lambda: put(outs[::-1]))

    outs = [((sum(p.shape[0] for p in g), g[0].shape[1]), g[0].dtype) for g in groups]
    operands, specs = [*pieces, *after], [VMEM] * (n + len(after))
    if parity is not None:
        operands, specs = [*operands, parity], [*specs, SMEM]
    return call(kernel, operands, outs, in_specs=specs, mib=4)


def turned(a, b, width):
    rows = a.shape[0]
    cuts = 7

    def kernel(a_ref, b_ref, out_ref):
        for k in range(cuts):
            at = slice(k * width // cuts, (k + 1) * width // cuts)
            out_ref[at, :rows] = a_ref[:, at].T
            out_ref[at, rows:] = b_ref[:, at].T

    return call(kernel, [a, b], [((width, 2 * rows), a.dtype)], flops=10**9)[0]


def added(groups, blocks, parity=None):
    sizes = [len(g) for g in groups]
    parts = [p for g in groups for p in g]
    n = len(parts)

    def kernel(*refs):
        outs = refs[len(refs) - blocks * len(groups) :]

        def put(outs):
            ins, outs = list(refs[:n]), list(outs)
            for size in sizes:
                terms = [ins.pop(0) for _ in range(size)]
                cut = terms[0].shape[0] // blocks
                for k in range(blocks):
                    at = slice(k * cut, (k + 1) * cut)
                    total = sum(t[at].astype(jnp.float32) for t in terms)
                    outs.pop(0)[...] = total.astype(jnp.bfloat16)

        if parity is None:
            put(outs)
        else:
            pl.when(refs[n][1] == 0)(lambda: put(outs))
            pl.when(refs[n][1] != 0)(lambda: put(outs[blocks:] + outs[:blocks]))

    outs = [
        ((g[0].shape[0] // blocks, g[0].shape[1]), jnp.bfloat16) for g in groups for _ in range(blocks)
    ]
    operands, specs = parts, [VMEM] * n
    if parity is not None:
        operands, specs = [*parts, parity], [*specs, SMEM]
    return call(kernel, operands, outs, in_specs=specs, mib=4)


def added_by_place(parts, spot, steps, after=()):
    rows, width = parts[0].shape

    def kernel(spot_ref, *refs):
        ins, outs, sums = refs[: len(parts)], refs[len(parts) + len(after) : -1], refs[-1]
        sums[...] = sum(t[...].astype(jnp.float32) for t in ins)
        for k, out_ref in zip(steps, outs):
            xor = 0 if k is None else jnp.where(spot_ref[0] == 0, XORS[0][k], XORS[1][k])
            at = pl.multiple_of((spot_ref[2] ^ (xor >> 1)) * 8, 8)
            out_ref[...] = sums[pl.ds(at, 8), :].astype(jnp.bfloat16)

    return call(
        kernel,
        [spot, *parts, *after],
        [((8, width), jnp.bfloat16)] * len(steps),
        in_specs=[SMEM] + [VMEM] * (len(parts) + len(after)),
        scratch=[pltpu.VMEM((rows, width), jnp.float32)],
        mib=4,
    )


def combined(parts, spot=None):
    shape = parts[0].shape
    n = len(parts)

    def kernel(*refs):
        ins, outs = refs[:n], refs[n:]
        smax = functools.reduce(jnp.maximum, [r[0:1] for r in ins])
        tmax = functools.reduce(jnp.maximum, [r[3:4] for r in ins])
        stot = cross = ttot = pick = 0.0
        for r in ins:
            factor = jnp.exp(r[0:1] - smax)
            stot, cross = stot + r[1:2] * factor, cross + r[2:3] * factor
            ttot = ttot + r[4:5] * jnp.exp(r[3:4] - tmax)
            pick = pick + r[5:6]
        mask = ins[0][6:7]
        rows = [smax, stot, cross, tmax, ttot, pick, mask, mask]
        if spot is not None:
            spot_ref, *outs = outs
            student_shift, teacher_shift = smax + jnp.log(stot), tmax + jnp.log(ttot)
            apart = student_shift - teacher_shift
            row_kl = cross / stot - apart
            rows = [student_shift, apart + row_kl] + [mask] * 6
            lane = lax.broadcasted_iota(jnp.int32, (8, 128), 1)
            total = jnp.sum(mask * row_kl, axis=1, keepdims=True)
            count = jnp.sum(mask, axis=1, keepdims=True)
            row = (spot_ref[3] >> 1) * 8 + lax.broadcasted_iota(jnp.int32, (8, shape[1]), 0)
            mine = row == lax.broadcasted_iota(jnp.int32, (8, shape[1]), 1)
            ratio = jnp.sum(jnp.where(mine, pick - apart, 0.0), axis=1, keepdims=True)
            here = lane == lax.broadcasted_iota(jnp.int32, (8, 128), 0)
            ratio = jnp.sum(jnp.where(here, ratio, 0.0), axis=0, keepdims=True)
            line = lax.broadcasted_iota(jnp.int32, (8, 128), 0)
            outs[1][...] = jnp.where(line == 0, total, jnp.where(line == 1, count, ratio))
        for k, row in enumerate(rows):
            outs[0][k : k + 1] = row

    out = (shape, jnp.float32)
    if spot is None:
        return call(kernel, parts, [out], mib=2)[0]
    outs = [out, ((8, 128), jnp.float32)]
    return call(kernel, [*parts, spot], outs, in_specs=[VMEM] * n + [SMEM], mib=2)


def side_by_side(head, head_in):
    width, columns = head.shape
    cuts = 4

    def kernel(h_ref, g_ref, out_ref, mark_ref, sems):
        mark_ref[...] = jnp.zeros(mark_ref.shape, jnp.float32)
        copies = []
        for k in range(cuts):
            at = pl.ds(k * width // cuts, width // cuts)
            for ref, column in ((h_ref, 0), (g_ref, columns)):
                copies.append(
                    pltpu.make_async_copy(
                        ref.at[at], out_ref.at[at, pl.ds(column, columns)], sems.at[len(copies)]
                    )
                )
        for copy in copies:
            copy.start()
        for copy in copies:
            copy.wait()

    return call(
        kernel,
        (far(head), far(head_in)),
        [((width, 2 * columns), head.dtype), ((8, 128), jnp.float32)],
        in_specs=[ANY, ANY],
        scratch=[pltpu.SemaphoreType.DMA((2 * cuts,))],
        flops=4 * 10**9,
        mib=2,
    )


def logits_and_stats(spot, a, b, heads, teacher, teacher_in, places, which, before=None):
    f32 = jnp.float32
    width, both = heads.shape
    columns = both // 2
    part, rows, tokens = a.shape[0], 2 * a.shape[0], places.shape[0]
    chunk = 32

    def kernel(spot_ref, a_ref, b_ref, h_ref, t_ref, u_ref, p_ref, *rest):
        out_ref, stats_ref, states, placed = rest[-4:]
        states[:part] = a_ref[:, :width]
        states[part:] = b_ref[:, :width]
        out_ref[...] = jnp.dot(states[...], h_ref[...], preferred_element_type=f32)
        lanes = lax.broadcasted_iota(jnp.int32, (1, both), 1)
        base, other_base = spot_ref[3] * columns, (spot_ref[3] ^ 1) * columns
        column = jnp.where(lanes < columns, base + lanes, other_base + lanes - columns)
        spots = lax.broadcasted_iota(jnp.int32, (1, tokens), 1)
        placed[...] = jnp.zeros(placed.shape, f32)
        for k in range(rows // chunk):
            ref, at = (a_ref, k * chunk) if k * chunk < part else (b_ref, k * chunk - part)
            here = slice(k * chunk, (k + 1) * chunk)
            there = slice(which * rows + k * chunk, which * rows + (k + 1) * chunk)
            student, note = out_ref[here, :], ref[at : at + chunk, width:].astype(f32)
            teacher = jnp.concatenate([t_ref[there, :], u_ref[there, :]], axis=1).astype(f32)
            ids = note[:, 1:2] + DIGITS * note[:, 2:3] + DIGITS**2 * note[:, 3:4]
            chosen = ids.astype(jnp.int32) == column
            smax = jnp.max(student, axis=1, keepdims=True)
            tmax = jnp.max(teacher, axis=1, keepdims=True)
            shifted = jnp.exp(student - smax)
            differ = student - teacher
            sums = [
                smax,
                jnp.sum(shifted, axis=1, keepdims=True),
                jnp.sum(shifted * differ, axis=1, keepdims=True),
                tmax,
                jnp.sum(jnp.exp(teacher - tmax), axis=1, keepdims=True),
                jnp.sum(jnp.where(chosen, differ, 0.0), axis=1, keepdims=True),
                note[:, :1],
            ]
            mine = p_ref[there, :] == spots
            for r, value in enumerate(sums):
                found = jnp.where(mine, value, 0.0).reshape(chunk // 8, 8, tokens)
                placed[r] += jnp.sum(found, axis=0)
        for r in range(8):
            row = jnp.sum(placed[r], axis=0, keepdims=True)
            stats_ref[r : r + 1] = row if before is None else row + rest[0][r : r + 1]

    operands = [spot, a, b, heads, teacher, teacher_in, places]
    if before is not None:
        operands.append(before)
    return call(
        kernel,
        operands,
        [((rows, both), f32), ((8, tokens), f32)],
        in_specs=[SMEM] + [VMEM] * (len(operands) - 1),
        scratch=[pltpu.VMEM((rows, width), jnp.bfloat16), pltpu.VMEM((8, 8, tokens), f32)],
        flops=2 * rows * width * both,
    )


def gradients(student, shifts, heads, teacher, teacher_in, places, which):
    f32, bf16 = jnp.float32, jnp.bfloat16
    width, both = heads.shape
    columns = both // 2
    rows, tokens = student.shape[0], places.shape[0]
    part = rows // 2
    chunk, cuts = 32, 7

    def kernel(s_ref, c_ref, h_ref, t_ref, u_ref, p_ref, a_ref, b_ref, d_ref, e_ref, all_d):
        spots = lax.broadcasted_iota(jnp.int32, (1, tokens), 1)
        for k in range(rows // chunk):
            here = slice(k * chunk, (k + 1) * chunk)
            there = slice(which * rows + k * chunk, which * rows + (k + 1) * chunk)
            mine = p_ref[there, :] == spots

            def of_row(r):
                return jnp.sum(jnp.where(mine, c_ref[r : r + 1], 0.0), axis=1, keepdims=True)

            student = s_ref[here, :]
            teacher = jnp.concatenate([t_ref[there, :], u_ref[there, :]], axis=1).astype(f32)
            probs = of_row(2) * jnp.exp(student - of_row(0))
            found = (probs * (student - teacher - of_row(1))).astype(bf16)
            all_d[here, :] = found
            d_ref[here, :] = found[:, :columns]
            e_ref[here, :] = found[:, columns:]
        for k in range(cuts):
            at = slice(k * width // cuts, (k + 1) * width // cuts)
            product = lax.dot_general(
                all_d[...], h_ref[at, :], (((1,), (1,)), ((), ())), preferred_element_type=f32
            ).astype(bf16)
            a_ref[:, at] = product[:part]
            b_ref[:, at] = product[part:]

    return call(
        kernel,
        [student, shifts, heads, teacher, teacher_in, places],
        [((part, width), bf16)] * 2 + [((rows, columns), bf16)] * 2,
        scratch=[pltpu.VMEM((rows, both), bf16)],
        flops=2 * rows * width * both,
    )


def head_gradient(states, dlogits, blocks, before=None):
    bf16 = jnp.bfloat16
    width, columns = states[0].shape[0], dlogits[0].shape[1]
    block = 512
    tokens = sum(d.shape[0] for d in dlogits)
    n, m = len(states), len(states) + len(dlogits)

    def kernel(*refs):
        pieces, others = refs[:n], refs[n:m]
        out_ref, right, found, sems = refs[-4:]
        at = 0
        for ref in others:
            right[at : at + ref.shape[0]] = ref[...]
            at += ref.shape[0]
        copies = []
        for j, k in enumerate(blocks):
            left = jnp.concatenate([r[k * block : (k + 1) * block, :] for r in pieces], axis=1)
            product = jnp.dot(left, right[...], preferred_element_type=jnp.float32).astype(bf16)
            slot = j % 2
            if j >= 2:
                copies[j - 2].wait()
            found[slot] = product
            copies.append(
                pltpu.make_async_copy(
                    found.at[slot], out_ref.at[pl.ds(k * block, block)], sems.at[slot]
                )
            )
            copies[j].start()
        copies[-2].wait()
        copies[-1].wait()

    operands, specs = [*states, *dlogits], [VMEM] * m
    if before is not None:
        operands, specs = [*operands, before], [*specs, ANY]
    return call(
        kernel,
        operands,
        [((width, columns), bf16)],
        in_specs=specs,
        out_specs=[ANY],
        scratch=[
            pltpu.VMEM((tokens, columns), bf16),
            pltpu.VMEM((2, block, columns), bf16),
            pltpu.SemaphoreType.DMA((2,)),
        ],
        flops=2 * tokens * len(blocks) * block * columns,
        aliases={} if before is None else {m: 0},
    )[0]


def per_device(hidden, teacher_logits, sampled_ids, loss_mask, student_head):
    f32, bf16 = jnp.float32, jnp.bfloat16
    core, y_low = lax.axis_index(CORE), lax.axis_index("tok_0")
    z, x = lax.axis_index("tok_1"), lax.axis_index("tok_2")
    position = lax.axis_index(TOK_VOC)
    group = group_of(core, y_low, z, x)
    width, _ = student_head.shape
    tokens = teacher_logits.shape[0]
    rows = tokens // 2

    block = entry_block(group, hidden, sampled_ids, loss_mask)
    token = token_of_rows(group, z, x, rows)
    token_other = token_of_rows(1 - group, z, x, rows)
    places = (token // 16) * 8 + token % 8
    spot = jnp.stack([group, y_low, lax.axis_index("voc_0"), position])
    other = swap(block, "y", 0)
    head_in = swap_core(student_head)
    teacher_send = jnp.dot(one_hot(token_other, tokens, bf16), teacher_logits)
    own_group = jnp.broadcast_to(group == core, (8,))
    other, teacher_send, spot, places, own_group = together(
        other, teacher_send, spot, places, own_group
    )
    teacher_in = swap_core(teacher_send)
    own_in = along(block, True, 0)
    across_in = along(other, False, 0)
    (own,) = joined((block, own_in))
    own_in = along(own, True, 1)
    (across,) = joined((other, across_in))
    across_in = along(across, False, 1)
    teacher = jnp.dot(one_hot(token, tokens, bf16), teacher_logits)
    own_in, across_in, teacher = together(own_in, across_in, teacher)
    near_a, near_b = joined((own, own_in), (across, across_in), parity=spot)

    far_a, far_b = swap(near_a, "z", 0), swap(near_b, "x", 0)
    heads, mark = side_by_side(student_head, head_in)
    near_a, near_b = joined((near_a, far_a), (near_b, far_b), after=(mark,))

    far_a, far_b = swap(near_a, "z", 1), swap(near_b, "x", 1)
    shared = (heads, teacher, teacher_in, places)
    near_other = swap_core(near_a), swap_core(near_b)
    student_near, stats = logits_and_stats(spot, near_a, near_b, *shared, 0)
    states = [turned(near_a, near_b, width)]
    far_a, far_b, student_near, stats, states[0] = together(
        far_a, far_b, student_near, stats, states[0]
    )
    student_far, stats = logits_and_stats(spot, far_a, far_b, *shared, 1, stats)
    pair = (far_a, far_b)
    for ring in ("x", "z", "y"):
        parts = [stats]
        for step in range(3):
            parts.append(swap(stats, ring, step))
        state = turned(*pair, width)
        states.append(state)
        if ring == "z":
            far_a, far_b, parts[0] = together(far_a, far_b, parts[0])
            pair = swap_core(far_a), swap_core(far_b)
        *parts, states[-1] = together(*parts, state)
        stats = combined(parts, spot if ring == "y" else None)
        if ring == "x":
            *pair, stats = together(*near_other, stats)
    stats, sums = stats

    far_sum_a, far_sum_b, *far_d = gradients(student_far, stats, *shared, 1)
    far_sum_a, far_sum_b, stats_later = together(far_sum_a, far_sum_b, stats)
    a_in, b_in = swap(far_sum_a, "z", 1), swap(far_sum_b, "x", 1)
    far_d_in = swap_core(far_d[1])
    near_sum_a, near_sum_b, *near_d = gradients(student_near, stats_later, *shared, 0)
    near_d_in = swap_core(near_d[1])
    all_d = (near_d[0], far_d[0], near_d_in, far_d_in)
    head_grad = head_gradient(states, all_d, range(4))
    a_in, b_in, near_sum_a, near_sum_b, head_grad, other_sums = together(
        a_in, b_in, near_sum_a, near_sum_b, head_grad, swap_core(sums)
    )
    keep_a, send_a, keep_b, send_b = added(((near_sum_a, a_in), (near_sum_b, b_in)), 2)
    a_in, b_in = swap(send_a, "z", 0), swap(send_b, "x", 0)
    head_grad = head_gradient(states, all_d, range(4, width // 512), head_grad)
    loss = (sums[0, 0] + other_sums[0, 0]) / (sums[1, 0] + other_sums[1, 0])
    sampled_ratio = jnp.where(own_group, sums[2, :8], other_sums[2, :8])
    a_in, b_in, head_grad, loss, sampled_ratio = together(
        a_in, b_in, head_grad, loss, sampled_ratio
    )
    own, own_send, across, across_send = added(((keep_a, a_in), (keep_b, b_in)), 2, spot)
    across_in = along(across_send, False, 1)
    own_in = along(own_send, True, 1)
    across, across_send = added(((across, across_in),), 2)
    across_in = along(across_send, False, 0)
    own, own_send = added(((own, own_in),), 2)
    own_in = along(own_send, True, 0)
    send = added_by_place((across, across_in), spot, (0, 1))
    arrived = [to_owner(part, step) for step, part in enumerate(send)]
    keep, last = added_by_place((own, own_in), spot, (None, 2), after=(send[0],))
    parts = [to_owner(keep), *arrived, to_owner(last, 2)]
    hidden_grad = sum(p.astype(f32) for p in parts).astype(bf16)
    return (loss, sampled_ratio, hidden_grad, head_grad)


def solution(mesh):
    split = Mesh(mesh.devices.reshape(2, 4, 4, 2, 2), TOK_VOC)
    in_specs = (P(TOK, None), P(None, TOK_VOC), P(TOK), P(TOK), P(None, TOK_VOC))
    out_specs = (P(), P(TOK_VOC), P(TOK_VOC, None), P(None, TOK_VOC))

    return jax.shard_map(
        per_device, mesh=split, in_specs=in_specs, out_specs=out_specs, check_vma=False
    )
```
